8 devices in a mesh: replica: 2 (over z, y), stage: 4 (over x, core).
Axes of the slice: x: 2, y: 2, z: 1, core: 2. Of those that a mesh axis runs over, the one named last changes fastest.
Arguments:
- x_dec: bfloat16 [8, 8, 576], P('replica'), parts along dimension 0
- x_pre: bfloat16 [8, 64, 576], P('replica'), parts along dimension 0
- dec_len: int32 [8, 8], P('replica'), parts along dimension 0
- pre_len: int32 [2], P('replica'), parts along dimension 0
- g_attn: bfloat16 [4, 576], P('stage')
- w_q: bfloat16 [4, 576, 576], P('stage')
- w_k: bfloat16 [4, 576, 192], P('stage')
- w_v: bfloat16 [4, 576, 192], P('stage')
- w_o: bfloat16 [4, 576, 576], P('stage')
- g_mlp: bfloat16 [4, 576], P('stage')
- w_gate: bfloat16 [4, 576, 1536], P('stage')
- w_up: bfloat16 [4, 576, 1536], P('stage')
- w_down: bfloat16 [4, 1536, 576], P('stage')
- g_final: bfloat16 [576], replicated
- w_head: bfloat16 [576, 1024], replicated
- k_dec: bfloat16 [4, 8, 8, 512, 3, 64], P('stage', 'replica'), parts along dimension 1
- v_dec: bfloat16 [4, 8, 8, 512, 3, 64], P('stage', 'replica'), parts along dimension 1
- k_pre: bfloat16 [4, 1024, 3, 64], P('stage', 'replica'), parts along dimension 1
- v_pre: bfloat16 [4, 1024, 3, 64], P('stage', 'replica'), parts along dimension 1
Outputs:
- output 1: float32 [8, 9, 1024], P('replica'), parts along dimension 0
- output 2: bfloat16 [4, 8, 8, 512, 3, 64], P('stage', 'replica'), parts along dimension 1
- output 3: bfloat16 [4, 8, 8, 512, 3, 64], P('stage', 'replica'), parts along dimension 1
- output 4: bfloat16 [4, 1024, 3, 64], P('stage', 'replica'), parts along dimension 1
- output 5: bfloat16 [4, 1024, 3, 64], P('stage', 'replica'), parts along dimension 1
There are 2 independent parts. The reference program is written for one: setup_inputs(seed, part) draws one part's arguments, and reference() takes and returns one part's arrays. A program takes and returns all parts, laid end to end along the dimension named above; an argument that names none is the same for every part.
All inputs are finite; a program needn't handle non-finite values.
Results may differ from the reference program's by a relative error of at most 0.0189117.
Values are sent between devices in bfloat16 or wider.
A program may use at most 1 GiB of HBM per device.

```python
import jax
import jax.numpy as jnp
from jax import lax

HIDDEN = 576
Q_HEADS = 9
KV_COUNT = 3
HEAD_DIM = 64
FFN_DIM = 1536
N_LAYERS = 4
N_MICRO = 4
DEC_ROWS = 8
SEG_LEN = 64
CACHE_LEN = 512
VOCAB_SIZE = 1024
NORM_EPS = 1e-6
ROPE_BASE = 10000.0
GROUP_SIZE = Q_HEADS // KV_COUNT
PRE_SPAN = CACHE_LEN - N_MICRO * SEG_LEN


def draw_lengths(base_key):
    key_list = jax.random.split(base_key, 4)
    n_slots = N_MICRO * DEC_ROWS
    min_len = CACHE_LEN // 8
    flat_len = jax.random.randint(key_list[0], (n_slots,), min_len, CACHE_LEN)
    top_at = jax.random.randint(key_list[1], (), 0, n_slots)
    low_at = (top_at + 1 + jax.random.randint(key_list[2], (), 0, n_slots - 1)) % n_slots
    slot_ids = jnp.arange(n_slots)
    flat_len = jnp.where(slot_ids == top_at, CACHE_LEN - 1, flat_len)
    flat_len = jnp.where(slot_ids == low_at, min_len, flat_len)
    pre_len = jax.random.randint(key_list[3], (1,), PRE_SPAN // 4 + 1, PRE_SPAN + 1)
    return flat_len.reshape(N_MICRO, DEC_ROWS).astype(jnp.int32), pre_len.astype(jnp.int32)


def setup_inputs(seed: int = 0, part: int = 0) -> dict:
    base_key = jax.random.key(seed)
    shared_keys = jax.random.split(base_key, 11)
    own_keys = jax.random.split(jax.random.fold_in(base_key, part), 10)
    q_width = Q_HEADS * HEAD_DIM
    kv_width = KV_COUNT * HEAD_DIM

    def weight_of(rng_key, arr_shape, fan_in):
        return (jax.random.normal(rng_key, arr_shape, jnp.float32) * fan_in ** -0.5).astype(jnp.bfloat16)

    def gain_of(rng_key, arr_shape):
        return (1.0 + 0.3 * jax.random.normal(rng_key, arr_shape, jnp.float32)).astype(jnp.bfloat16)

    dec_len, pre_len = draw_lengths(own_keys[2])
    cache_shape = (N_LAYERS, N_MICRO, DEC_ROWS, CACHE_LEN, KV_COUNT, HEAD_DIM)
    mean_shape = (N_LAYERS, N_MICRO, DEC_ROWS, 1, KV_COUNT, HEAD_DIM)
    pre_shape = (N_LAYERS, CACHE_LEN, KV_COUNT, HEAD_DIM)
    return {
        'x_dec': jax.random.normal(own_keys[0], (N_MICRO, DEC_ROWS, HIDDEN), jnp.float32).astype(jnp.bfloat16),
        'x_pre': jax.random.normal(own_keys[1], (N_MICRO, SEG_LEN, HIDDEN), jnp.float32).astype(jnp.bfloat16),
        'dec_len': dec_len,
        'pre_len': pre_len,
        'g_attn': gain_of(shared_keys[0], (N_LAYERS, HIDDEN)),
        'w_q': weight_of(shared_keys[1], (N_LAYERS, HIDDEN, q_width), HIDDEN),
        'w_k': weight_of(shared_keys[2], (N_LAYERS, HIDDEN, kv_width), HIDDEN),
        'w_v': weight_of(shared_keys[3], (N_LAYERS, HIDDEN, kv_width), HIDDEN),
        'w_o': weight_of(shared_keys[4], (N_LAYERS, q_width, HIDDEN), q_width),
        'g_mlp': gain_of(shared_keys[5], (N_LAYERS, HIDDEN)),
        'w_gate': weight_of(shared_keys[6], (N_LAYERS, HIDDEN, FFN_DIM), HIDDEN),
        'w_up': weight_of(shared_keys[7], (N_LAYERS, HIDDEN, FFN_DIM), HIDDEN),
        'w_down': weight_of(shared_keys[8], (N_LAYERS, FFN_DIM, HIDDEN), FFN_DIM),
        'g_final': gain_of(shared_keys[9], (HIDDEN,)),
        'w_head': weight_of(shared_keys[10], (HIDDEN, VOCAB_SIZE), HIDDEN),
        'k_dec': jax.random.normal(own_keys[3], cache_shape, jnp.float32).astype(jnp.bfloat16),
        'v_dec': (jax.random.normal(own_keys[4], cache_shape, jnp.float32) + jax.random.normal(own_keys[5], mean_shape, jnp.float32)).astype(jnp.bfloat16),
        'k_pre': jax.random.normal(own_keys[6], pre_shape, jnp.float32).astype(jnp.bfloat16),
        'v_pre': (jax.random.normal(own_keys[7], pre_shape, jnp.float32) + jax.random.normal(own_keys[8], (N_LAYERS, 1, KV_COUNT, HEAD_DIM), jnp.float32)).astype(jnp.bfloat16),
    }


def rms_norm(acts, gain):
    acts_f = acts.astype(jnp.float32)
    inv_rms = lax.rsqrt(jnp.mean(acts_f * acts_f, axis=-1, keepdims=True) + NORM_EPS)
    return (acts_f * inv_rms * gain.astype(jnp.float32)).astype(jnp.bfloat16)


def rotate(proj, positions):
    half_dim = HEAD_DIM // 2
    inv_freq = ROPE_BASE ** (-jnp.arange(half_dim, dtype=jnp.float32) * (2.0 / HEAD_DIM))
    angles = positions.astype(jnp.float32)[:, None, None] * inv_freq
    cosine = jnp.cos(angles)
    sine_v = jnp.sin(angles)
    first_h = proj[..., :half_dim]
    second_h = proj[..., half_dim:]
    return jnp.concatenate([first_h * cosine - second_h * sine_v, second_h * cosine + first_h * sine_v], axis=-1)


def softmax_mix(scores, valid, values, form):
    masked = jnp.where(valid, scores, -1e30)
    probs = jax.nn.softmax(masked, axis=-1).astype(jnp.bfloat16)
    return jnp.einsum(form, probs.astype(jnp.float32), values.astype(jnp.float32)).astype(jnp.bfloat16)


def micro_block(acts, dec_pos, pre_begin, layer_w, kd_m, vd_m, k_cache, v_cache):
    g_att, wq_l, wk_l, wv_l, wo_l, g_ffn, wg_l, wu_l, wd_l = layer_w
    n_rows = DEC_ROWS + SEG_LEN
    pre_pos = pre_begin + jnp.arange(SEG_LEN)
    positions = jnp.concatenate([dec_pos, pre_pos])
    normed = rms_norm(acts, g_att)
    q_all = rotate(jnp.dot(normed, wq_l, preferred_element_type=jnp.float32).reshape(n_rows, Q_HEADS, HEAD_DIM), positions).astype(jnp.bfloat16)
    k_all = rotate(jnp.dot(normed, wk_l, preferred_element_type=jnp.float32).reshape(n_rows, KV_COUNT, HEAD_DIM), positions).astype(jnp.bfloat16)
    v_all = jnp.dot(normed, wv_l, preferred_element_type=jnp.float32).astype(jnp.bfloat16).reshape(n_rows, KV_COUNT, HEAD_DIM)
    row_ids = jnp.arange(DEC_ROWS)
    kd_m = kd_m.at[row_ids, dec_pos].set(k_all[:DEC_ROWS])
    vd_m = vd_m.at[row_ids, dec_pos].set(v_all[:DEC_ROWS])
    k_cache = lax.dynamic_update_slice(k_cache, k_all[DEC_ROWS:], (pre_begin, 0, 0))
    v_cache = lax.dynamic_update_slice(v_cache, v_all[DEC_ROWS:], (pre_begin, 0, 0))
    q_grp = q_all.reshape(n_rows, KV_COUNT, GROUP_SIZE, HEAD_DIM).astype(jnp.float32)
    att_scale = HEAD_DIM ** -0.5
    cache_pos = jnp.arange(CACHE_LEN)
    dec_scores = jnp.einsum('bkgd,bskd->bkgs', q_grp[:DEC_ROWS], kd_m.astype(jnp.float32)) * att_scale
    dec_valid = (cache_pos[None, :] <= dec_pos[:, None])[:, None, None, :]
    dec_out = softmax_mix(dec_scores, dec_valid, vd_m, 'bkgs,bskd->bkgd').reshape(DEC_ROWS, Q_HEADS * HEAD_DIM)
    pre_scores = jnp.einsum('ikgd,skd->ikgs', q_grp[DEC_ROWS:], k_cache.astype(jnp.float32)) * att_scale
    pre_valid = (cache_pos[None, :] <= pre_pos[:, None])[:, None, None, :]
    pre_out = softmax_mix(pre_scores, pre_valid, v_cache, 'ikgs,skd->ikgd').reshape(SEG_LEN, Q_HEADS * HEAD_DIM)
    attn_out = jnp.concatenate([dec_out, pre_out], axis=0)
    acts = (acts.astype(jnp.float32) + jnp.dot(attn_out, wo_l, preferred_element_type=jnp.float32)).astype(jnp.bfloat16)
    normed2 = rms_norm(acts, g_ffn)
    gate_f = jnp.dot(normed2, wg_l, preferred_element_type=jnp.float32)
    up_proj = jnp.dot(normed2, wu_l, preferred_element_type=jnp.float32)
    hidden_act = (jax.nn.silu(gate_f) * up_proj).astype(jnp.bfloat16)
    acts = (acts.astype(jnp.float32) + jnp.dot(hidden_act, wd_l, preferred_element_type=jnp.float32)).astype(jnp.bfloat16)
    return acts, kd_m, vd_m, k_cache, v_cache


def reference(x_dec, x_pre, dec_len, pre_len, g_attn, w_q, w_k, w_v, w_o, g_mlp, w_gate, w_up, w_down, g_final, w_head, k_dec, v_dec, k_pre, v_pre):
    acts_init = jnp.concatenate([x_dec, x_pre], axis=1)
    pre_starts = pre_len[0] + jnp.arange(N_MICRO) * SEG_LEN

    def layer_fn(acts_all, layer_in):
        layer_w = layer_in[:9]
        kd_l, vd_l, kp_l, vp_l = layer_in[9:]

        def micro_fn(pre_cache, micro_in):
            kp_c, vp_c = pre_cache
            acts_m, dec_pos, pre_begin, kd_m, vd_m = micro_in
            acts_m, kd_m, vd_m, kp_c, vp_c = micro_block(acts_m, dec_pos, pre_begin, layer_w, kd_m, vd_m, kp_c, vp_c)
            return (kp_c, vp_c), (acts_m, kd_m, vd_m)

        (kp_l, vp_l), (acts_all, kd_l, vd_l) = lax.scan(micro_fn, (kp_l, vp_l), (acts_all, dec_len, pre_starts, kd_l, vd_l))
        return acts_all, (kd_l, vd_l, kp_l, vp_l)

    acts_last, caches = lax.scan(layer_fn, acts_init, (g_attn, w_q, w_k, w_v, w_o, g_mlp, w_gate, w_up, w_down, k_dec, v_dec, k_pre, v_pre))
    kd_new, vd_new, kp_new, vp_new = caches
    kept = jnp.concatenate([acts_last[:, :DEC_ROWS], acts_last[:, -1:]], axis=1)
    final_h = rms_norm(kept, g_final)
    logits = jnp.dot(final_h.reshape(-1, HIDDEN), w_head, preferred_element_type=jnp.float32).reshape(N_MICRO, DEC_ROWS + 1, VOCAB_SIZE)
    return (logits, kd_new, vd_new, kp_new, vp_new)
```

```python
import functools

import jax
import jax.numpy as jnp
import numpy as np
from jax import lax
from jax.experimental import pallas as pl
from jax.experimental.pallas import tpu as pltpu
from jax.sharding import PartitionSpec as P

F32 = jnp.float32
BF16 = jnp.bfloat16
MESH = pl.DeviceIdType.MESH
NORM_EPS = 1e-6
ROPE_BASE = 10000.0
NEG = -1e30

HID = 576
NQ = 9
NKV = 3
GRP = 3
HD = 64
HALF = 32
KVW = NKV * HD
FFN = 1536
NM = 4
DR = 8
SEG = 64
CL = 512
VOC = 1024
ND = NM * DR
NP = NM * SEG
LAST = 3
LN = 128


def nt(a, b):
    return lax.dot_general(a, b, (((1,), (1,)), ((), ())), preferred_element_type=F32)


def nn(a, b):
    return jnp.dot(a, b, preferred_element_type=F32)


def rms(x, g):
    inv = lax.rsqrt(jnp.mean(x * x, axis=-1, keepdims=True) + NORM_EPS)
    return (x * inv * g).astype(BF16)


def rope_t(m, cos, sin):
    parts = []
    for j in range(m.shape[0] // HD):
        a = m[j * HD:j * HD + HALF]
        b = m[j * HD + HALF:(j + 1) * HD]
        parts += [a * cos - b * sin, b * cos + a * sin]
    return jnp.concatenate(parts, axis=0)


def lane_iota(shape):
    return lax.broadcasted_iota(jnp.int32, shape, len(shape) - 1)


def pipe_kernel(xd, xp, dlen, plen, ga, wq, wk, wv, wo, gm, wg, wu, wd, gf, wh, kd, vd, kp, vp, ifr,
                kdn, vdn, kpn, vpn, logits,
                xd_s, xp_s, dl_s, pl_s, ga_s, wq_s, wk_s, wv_s, wo_s, gm_s, wg_s, wu_s, wd_s, gf_s, wh_s,
                kd_s, vd_s, kp_s, vp_s, ifr_s,
                wqt_s, cosd_s, sind_s, cosp_s, sinp_s, cosl_s, sinl_s, qa_s, qb_s, self_s, vn_s, oa_s, ob_s,
                kdn_s, vdn_s, ot_s, act_s, x4_s, sd_s, sp_s, fh_s, fr_s, lg_s,
                in_sem, kd_sem, vd_sem, out_sem, sdd, sdp, rcd, rcp, sdf, rcf):
    st = lax.axis_index('stage')
    rep = lax.axis_index('replica')
    order = [(dlen, dl_s), (plen, pl_s), (xd, xd_s), (ga, ga_s), (ifr, ifr_s), (wq, wq_s), (wk, wk_s), (wv, wv_s),
             (kp, kp_s), (vp, vp_s), (wo, wo_s), (gm, gm_s), (wg, wg_s), (wu, wu_s), (wd, wd_s), (xp, xp_s), (gf, gf_s), (wh, wh_s)]
    cps = [pltpu.make_async_copy(a, b, in_sem.at[i]) for i, (a, b) in enumerate(order)]
    by = {id(b): c for (a, b), c in zip(order, cps)}
    kcp = [pltpu.make_async_copy(kd.at[m], kd_s.at[m], kd_sem.at[m]) for m in range(NM)]
    vcp = [pltpu.make_async_copy(vd.at[m], vd_s.at[m], vd_sem.at[m]) for m in range(NM)]

    def ld(ref):
        return by[id(ref)]

    for r in (dl_s, pl_s, ga_s, ifr_s, wq_s, wk_s, wv_s):
        ld(r).start()

    @pl.when(st == 0)
    def _():
        ld(xd_s).start()

    for m in range(NM):
        kcp[m].start()
        vcp[m].start()
    for r in (wo_s, gm_s, wg_s, wu_s, wd_s, kp_s, vp_s):
        ld(r).start()

    @pl.when(st == 0)
    def _():
        ld(xp_s).start()

    ld(gf_s).start()
    ld(wh_s).start()

    bar = pltpu.get_barrier_semaphore()
    for k in range(4):
        @pl.when(st != k)
        def _(k=k):
            pl.semaphore_signal(bar, inc=1, device_id={'stage': k}, device_id_type=MESH)

    ld(dl_s).wait()
    ld(pl_s).wait()
    ld(ifr_s).wait()
    p0 = pl_s[0]
    li = lane_iota((1, LN))
    posd = jnp.zeros((1, LN), jnp.int32)
    for b in range(ND):
        posd = jnp.where(li == b, dl_s[b // DR, b % DR], posd)
    fr = ifr_s[...]
    ang = fr[:, :LN] * posd.astype(F32)
    cosd_s[...] = jnp.cos(ang)
    sind_s[...] = jnp.sin(ang)
    ang = fr * (p0 + lane_iota((1, NP))).astype(F32)
    cosp_s[...] = jnp.cos(ang)
    sinp_s[...] = jnp.sin(ang)
    ang = fr[:, :LN] * (p0 + li * SEG + (SEG - 1)).astype(F32)
    cosl_s[...] = jnp.cos(ang)
    sinl_s[...] = jnp.sin(ang)
    qa_s[...] = jnp.zeros_like(qa_s)
    qb_s[...] = jnp.zeros_like(qb_s)
    ob_s[...] = jnp.zeros_like(ob_s)

    ld(ga_s).wait()
    ld(wq_s).wait()
    wqt_s[...] = wq_s[...].astype(F32).T.astype(BF16)
    ld(wk_s).wait()
    ld(wv_s).wait()
    gat = ga_s[...].astype(F32)

    lgrp = lane_iota((8, KVW)) // HD

    def qkv_dec(h, cos, sin, b0, n):
        hp = jnp.concatenate([h, jnp.zeros((LN - h.shape[0], HID), BF16)], axis=0)
        qt = rope_t(nt(wqt_s[...], hp), cos, sin).astype(BF16).astype(F32)
        kt = rope_t(nt(wk_s[...], hp), cos, sin).astype(BF16).astype(F32)
        vt = nt(wv_s[...], hp).astype(BF16).astype(F32)
        qt = qt * (HD ** -0.5)
        row = lax.broadcasted_iota(jnp.int32, (24, LN), 0)
        sf = jnp.zeros((24, LN), F32)
        for g in range(NKV):
            for r in range(GRP):
                j = g * GRP + r
                s = jnp.sum(qt[j * HD:(j + 1) * HD] * kt[g * HD:(g + 1) * HD], axis=0, keepdims=True)
                sf = jnp.where(row == 8 * g + r, s, sf)
        for r in range(GRP):
            qr = [qt[(g * GRP + r) * HD:(g * GRP + r + 1) * HD] for g in range(NKV)]
            qa_s[pl.ds(b0 * 8 + r, n, stride=8), :] = jnp.concatenate(qr[:2], axis=0).T[:n]
            qb_s[pl.ds(b0 * 8 + r, n, stride=8), :] = jnp.concatenate([qr[2], jnp.zeros((HD, LN), F32)], axis=0).T[:n]
        vn_s[b0:b0 + n, :LN] = vt[:LN].T[:n]
        vn_s[b0:b0 + n, LN:] = jnp.concatenate([vt[LN:], jnp.zeros((HD, LN), F32)], axis=0).T[:n, :HD]
        return kt, vt, sf

    def attn_dec(b, kt, vt, pos, selfcol):
        qb = jnp.concatenate([qa_s[pl.ds(b * 8, 8), :], qb_s[pl.ds(b * 8, 8), :HD]], axis=1)
        lhs = jnp.concatenate([jnp.where(lgrp == g, qb, 0.0) for g in range(NKV)], axis=0).astype(BF16)
        s = nn(lhs, kt)
        s = jnp.where(lane_iota((24, CL)) < pos, s, NEG)
        mx = jnp.maximum(jnp.max(s, axis=-1, keepdims=True), selfcol)
        p = jnp.exp(s - mx)
        ps = jnp.exp(selfcol - mx)
        rl = 1.0 / (jnp.sum(p, axis=-1, keepdims=True) + ps)
        o = nt((p * rl).astype(BF16), vt)
        o = o + (ps * rl).astype(BF16).astype(F32) * vn_s[pl.ds(b, 1), :]
        acc = jnp.where(lgrp == 0, o[0:8], 0.0)
        for g in range(1, NKV):
            acc = jnp.where(lgrp == g, o[8 * g:8 * g + 8], acc)
        oa_s[pl.ds(b * 8, 8), :] = acc[:, :LN]
        ob_s[pl.ds(b * 8, 8), :HD] = acc[:, LN:]

    def self_col(b):
        return jnp.sum(jnp.where(lane_iota((24, LN)) == b, self_s[...], 0.0), axis=-1, keepdims=True)

    def dec_out(b0, n):
        return [jnp.concatenate([oa_s[pl.ds(b0 * 8 + r, n, stride=8), :], ob_s[pl.ds(b0 * 8 + r, n, stride=8), :][:, :HD]], axis=1).astype(BF16)
                for r in range(GRP)]

    def wo_rows(r):
        return jnp.concatenate([wo_s[(g * GRP + r) * HD:(g * GRP + r + 1) * HD, :] for g in range(NKV)], axis=0)

    def mlp(x, rows):
        h2 = rms(x, gm_s[...].astype(F32))
        step = 512
        for c in range(FFN // step):
            gt = nn(h2, wg_s[:, c * step:(c + 1) * step])
            up = nn(h2, wu_s[:, c * step:(c + 1) * step])
            act_s[:rows, c * step:(c + 1) * step] = (gt * (1.0 / (1.0 + jnp.exp(-gt))) * up).astype(BF16)
        return (x + nt(act_s[:rows, :], wd_s[...])).astype(BF16)

    def round32(x):
        return x.astype(BF16).astype(F32)

    def to(k):
        return {'stage': k}

    def hop(src, dst, s_sem, r_sem):
        return pltpu.make_async_remote_copy(src, dst, s_sem, r_sem, device_id=to(jnp.minimum(st + 1, LAST)), device_id_type=MESH)

    @pl.when(st == 0)
    def _():
        ld(xd_s).wait()

    @pl.when(st > 0)
    def _():
        hop(sd_s, xd_s, sdd, rcd).wait_recv()

    hd = rms(xd_s[...].astype(F32), gat)
    ktd, vtd, sfd = qkv_dec(hd, cosd_s[...], sind_s[...], 0, ND)
    self_s[...] = sfd
    kdn_s[...] = ktd
    vdn_s[...] = vtd
    okd = pltpu.make_async_copy(kdn_s, kdn, out_sem.at[0])
    ovd = pltpu.make_async_copy(vdn_s, vdn, out_sem.at[1])
    okd.start()
    ovd.start()

    def dec_loop(m, carry):
        pltpu.make_async_copy(kd.at[m], kd_s.at[m], kd_sem.at[m]).wait()
        pltpu.make_async_copy(vd.at[m], vd_s.at[m], vd_sem.at[m]).wait()
        for i in range(DR):
            b = m * DR + i
            attn_dec(b, kd_s[m, i].reshape(KVW, CL), vd_s[m, i].reshape(KVW, CL), dl_s[m, i], self_col(b))
        return carry

    lax.fori_loop(0, NM, dec_loop, 0)

    for r in (wo_s, gm_s, wg_s, wu_s, wd_s):
        ld(r).wait()
    pl.semaphore_wait(bar, 3)

    @pl.when(st < LAST)
    def _():
        a = dec_out(0, ND)
        y = nn(a[0], wo_rows(0)) + nn(a[1], wo_rows(1)) + nn(a[2], wo_rows(2))
        x1 = round32(xd_s[...].astype(F32) + y)
        sd_s[...] = mlp(x1, ND)
        hop(sd_s, xd_s, sdd, rcd).start()

    @pl.when(st == 0)
    def _():
        ld(xp_s).wait()

    @pl.when(st > 0)
    def _():
        hop(sp_s, xp_s, sdp, rcp).wait_recv()

    ld(kp_s).wait()
    ld(vp_s).wait()
    hp = rms(xp_s[...].astype(F32), gat)
    ktp = rope_t(nt(wk_s[...], hp), cosp_s[...], sinp_s[...]).astype(BF16)
    vtp = nt(wv_s[...], hp).astype(BF16)
    place = jnp.where(lax.broadcasted_iota(jnp.int32, (NP, CL), 0) + p0 == lane_iota((NP, CL)), 1.0, 0.0).astype(BF16)
    lp = lane_iota((KVW, CL)) - p0
    fresh = (lp >= 0) & (lp < NP)
    kpu = jnp.where(fresh, nn(ktp, place), kp_s[...].reshape(KVW, CL).astype(F32))
    vpu = jnp.where(fresh, nn(vtp, place), vp_s[...].reshape(KVW, CL).astype(F32))
    kp_s[...] = kpu.astype(BF16).reshape(NKV, HD, CL)
    vp_s[...] = vpu.astype(BF16).reshape(NKV, HD, CL)
    okp = pltpu.make_async_copy(kp_s, kpn, out_sem.at[2])
    ovp = pltpu.make_async_copy(vp_s, vpn, out_sem.at[3])
    okp.start()
    ovp.start()

    @pl.when(st < LAST)
    def _():
        kfull = kpu.T.astype(BF16)
        vfull = vp_s[...].reshape(KVW, CL)
        qt = (rope_t(nt(wqt_s[...], hp), cosp_s[...], sinp_s[...]).astype(BF16).astype(F32) * (HD ** -0.5)).astype(BF16)
        bias = jnp.where(lax.broadcasted_iota(jnp.int32, (CL, NP), 0) <= lane_iota((CL, NP)) + p0, 0.0, NEG)
        for j in range(NQ):
            g = j // GRP
            parts = []
            if g:
                parts.append(jnp.zeros((g * HD, NP), BF16))
            parts.append(qt[j * HD:(j + 1) * HD])
            if g < NKV - 1:
                parts.append(jnp.zeros(((NKV - 1 - g) * HD, NP), BF16))
            s = nn(kfull, jnp.concatenate(parts, axis=0)) + bias
            p = jnp.exp(s - jnp.max(s, axis=0, keepdims=True))
            pr = (p * (1.0 / jnp.sum(p, axis=0, keepdims=True))).astype(BF16)
            ot_s[j * HD:(j + 1) * HD, :] = nn(vfull[g * HD:(g + 1) * HD], pr)
        x1 = round32(xp_s[...].astype(F32) + nn(ot_s[...].T.astype(BF16), wo_s[...]))
        sp_s[...] = mlp(x1, NP)
        hop(sp_s, xp_s, sdp, rcp).start()

    def bcast(k):
        return pltpu.make_async_remote_copy(fh_s, fr_s, sdf.at[k], rcf, device_id=to(k), device_id_type=MESH)

    ld(gf_s).wait()
    ld(wh_s).wait()

    def head(ref):
        lg_s[...] = nn(ref[...], wh_s[...])

    @pl.when(st == LAST)
    def _():
        x4_s[...] = jnp.zeros_like(x4_s)
        for m in range(NM):
            r0 = m * SEG + SEG - 8
            x4_s[m:m + 1, :] = xp_s[r0:r0 + 8, :].astype(F32)[7:8]
        x4 = x4_s[...]
        h4 = rms(x4, gat)
        h4 = jnp.concatenate([h4, jnp.zeros_like(h4)], axis=0)
        _, _, sf4 = qkv_dec(h4, cosl_s[...], sinl_s[...], ND, 8)
        for m in range(NM):
            col = jnp.sum(jnp.where(lane_iota((24, LN)) == m, sf4, 0.0), axis=-1, keepdims=True)
            attn_dec(ND + m, kp_s[...].reshape(KVW, CL), vp_s[...].reshape(KVW, CL), p0 + m * SEG + SEG - 1, col)
        for m in range(NM, 8):
            oa_s[pl.ds((ND + m) * 8, 8), :] = jnp.zeros((8, LN), F32)
        a = dec_out(0, ND + 8)
        y = nn(a[0], wo_rows(0)) + nn(a[1], wo_rows(1)) + nn(a[2], wo_rows(2))
        x1 = round32(jnp.concatenate([xd_s[...].astype(F32), x4], axis=0) + y)
        x2 = mlp(x1, ND + 8)
        fh = rms(x2.astype(F32), gf_s[...].astype(F32))
        ri = lax.broadcasted_iota(jnp.int32, (ND + 8, ND + 8), 0)
        src = jnp.where(ri < ND, (ri % NM) * DR + ri // NM, ri)
        fh_s[...] = nn(jnp.where(lane_iota((ND + 8, ND + 8)) == src, 1.0, 0.0).astype(BF16), fh).astype(BF16)
        for k in range(LAST):
            bcast(k).start()
        head(fh_s)

    @pl.when(st < LAST)
    def _():
        bcast(0).wait_recv()
        head(fr_s)

    for i in range(DR + 1):
        logits[i] = lg_s[i * NM:(i + 1) * NM, :]

    okd.wait()
    ovd.wait()
    okp.wait()
    ovp.wait()

    @pl.when(st < LAST)
    def _():
        hop(sd_s, xd_s, sdd, rcd).wait_send()
        hop(sp_s, xp_s, sdp, rcp).wait_send()

    @pl.when(st == LAST)
    def _():
        for k in range(LAST):
            bcast(k).wait_send()


def cache_kernel(dlen, kd, vd, kdn, vdn, kpn, vpn, ko, vo, kpo, vpo, ks, vs, kn_s, vn_s, kp_s, vp_s, ksem, vsem, nsem):
    cin = []
    for m in range(NM):
        cin.append((pltpu.make_async_copy(kd.at[m], ks.at[m], ksem.at[m]), pltpu.make_async_copy(vd.at[m], vs.at[m], vsem.at[m])))
    small = [pltpu.make_async_copy(a, b, nsem.at[i]) for i, (a, b) in enumerate(
        [(kdn, kn_s), (vdn, vn_s), (kpn, kp_s), (vpn, vp_s)])]
    for c in small:
        c.start()
    for a, b in cin:
        a.start()
        b.start()
    for c in small:
        c.wait()
    outs = [pltpu.make_async_copy(kp_s, kpo, nsem.at[2]), pltpu.make_async_copy(vp_s, vpo, nsem.at[3])]
    for c in outs:
        c.start()
    lane = lane_iota((HD, LN))
    for m in range(NM):
        for cp, scr, new, out, sem in ((cin[m][0], ks, kn_s, ko, ksem), (cin[m][1], vs, vn_s, vo, vsem)):
            cp.wait()
            for i in range(DR):
                b = m * DR + i
                pos = dlen[m, i]
                sl = pl.ds(pl.multiple_of((pos // LN) * LN, LN), LN)
                for g in range(NKV):
                    col = new[g * HD:(g + 1) * HD, b:b + 1]
                    old = scr[m, i, g, :, sl].astype(F32)
                    scr[m, i, g, :, sl] = jnp.where(lane == pos % LN, col, old).astype(BF16)
            c = pltpu.make_async_copy(scr.at[m], out.at[m], sem.at[m])
            c.start()
            outs.append(c)
    for c in outs:
        c.wait()


ANY = pl.BlockSpec(memory_space=pltpu.HBM)


def solution(mesh):
    part = P('replica')
    layer = P('stage')
    cache = P('stage', 'replica')
    in_specs = (part,) * 4 + (layer,) * 9 + (P(), P()) + (cache,) * 4
    out_specs = (part,) + (cache,) * 4
    inv_freq = np.float32(ROPE_BASE) ** (-np.arange(HALF, dtype=np.float32) * np.float32(2.0 / HD))
    ifr_c = np.broadcast_to(inv_freq[:, None], (HALF, NP)).astype(np.float32)

    def device_fn(x_dec, x_pre, dec_len, pre_len, g_attn, w_q, w_k, w_v, w_o, g_mlp, w_gate, w_up, w_down, g_final, w_head, k_dec, v_dec, k_pre, v_pre):
        kd = jnp.transpose(k_dec[0], (0, 1, 3, 4, 2))
        vd = jnp.transpose(v_dec[0], (0, 1, 3, 4, 2))
        kp = jnp.transpose(k_pre[0], (1, 2, 0))
        vp = jnp.transpose(v_pre[0], (1, 2, 0))
        args = (x_dec.reshape(ND, HID), x_pre.reshape(NP, HID), dec_len, pre_len, g_attn, w_q[0], w_k[0].T, w_v[0].T, w_o[0], g_mlp,
                w_gate[0], w_up[0], w_down[0].T, g_final.reshape(1, HID), w_head, kd, vd, kp, vp, jnp.asarray(ifr_c))
        vm = lambda shape, dt: pltpu.VMEM(shape, dt)
        scratch = [
            vm((ND, HID), BF16), vm((NP, HID), BF16), pltpu.SMEM((NM, DR), jnp.int32), pltpu.SMEM((1,), jnp.int32), vm((1, HID), BF16),
            vm((HID, HID), BF16), vm((KVW, HID), BF16), vm((KVW, HID), BF16), vm((HID, HID), BF16), vm((1, HID), BF16),
            vm((HID, FFN), BF16), vm((HID, FFN), BF16), vm((HID, FFN), BF16), vm((1, HID), BF16), vm((HID, VOC), BF16),
            vm(kd.shape, BF16), vm(vd.shape, BF16), vm(kp.shape, BF16), vm(vp.shape, BF16), vm((HALF, NP), F32),
            vm((HID, HID), BF16), vm((HALF, LN), F32), vm((HALF, LN), F32), vm((HALF, NP), F32), vm((HALF, NP), F32),
            vm((HALF, LN), F32), vm((HALF, LN), F32),
            vm(((ND + 8) * 8, LN), F32), vm(((ND + 8) * 8, LN), F32), vm((24, LN), F32), vm((ND + 8, KVW), F32),
            vm(((ND + 8) * 8, LN), F32), vm(((ND + 8) * 8, LN), F32),
            vm((KVW, LN), F32), vm((KVW, LN), F32), vm((HID, NP), F32), vm((NP, FFN), BF16), vm((8, HID), F32),
            vm((ND, HID), BF16), vm((NP, HID), BF16), vm((ND + 8, HID), BF16), vm((ND + 8, HID), BF16), vm((ND + 8, VOC), F32),
            pltpu.SemaphoreType.DMA((18,)), pltpu.SemaphoreType.DMA((NM,)), pltpu.SemaphoreType.DMA((NM,)), pltpu.SemaphoreType.DMA((4,)),
            pltpu.SemaphoreType.DMA, pltpu.SemaphoreType.DMA, pltpu.SemaphoreType.DMA, pltpu.SemaphoreType.DMA,
            pltpu.SemaphoreType.DMA((3,)), pltpu.SemaphoreType.DMA,
        ]
        kdn, vdn, kpn, vpn, logits = pl.pallas_call(
            pipe_kernel,
            out_shape=(jax.ShapeDtypeStruct((KVW, LN), F32), jax.ShapeDtypeStruct((KVW, LN), F32),
                       jax.ShapeDtypeStruct(kp.shape, BF16), jax.ShapeDtypeStruct(vp.shape, BF16),
                       jax.ShapeDtypeStruct((DR + 1, NM, VOC), F32)),
            in_specs=[ANY] * len(args),
            out_specs=(ANY, ANY, ANY, ANY, pl.BlockSpec(memory_space=pltpu.VMEM)),
            scratch_shapes=scratch,
            name='pipe',
            compiler_params=pltpu.CompilerParams(collective_id=0, has_side_effects=True, vmem_limit_bytes=60 * 1024 * 1024),
        )(*args)
        ko, vo, kpo, vpo = pl.pallas_call(
            cache_kernel,
            out_shape=tuple(jax.ShapeDtypeStruct(a.shape, BF16) for a in (kd, vd, kp, vp)),
            in_specs=[pl.BlockSpec(memory_space=pltpu.SMEM)] + [ANY] * 6,
            out_specs=(ANY,) * 4,
            scratch_shapes=[vm(kd.shape, BF16), vm(vd.shape, BF16), vm((KVW, LN), F32), vm((KVW, LN), F32), vm(kp.shape, BF16), vm(vp.shape, BF16),
                            pltpu.SemaphoreType.DMA((NM,)), pltpu.SemaphoreType.DMA((NM,)), pltpu.SemaphoreType.DMA((4,))],
            name='caches',
            compiler_params=pltpu.CompilerParams(vmem_limit_bytes=40 * 1024 * 1024),
        )(dec_len, kd, vd, kdn, vdn, kpn, vpn)
        back = lambda a: jnp.transpose(a, (0, 1, 4, 2, 3))[None]
        backp = lambda a: jnp.transpose(a, (2, 0, 1))[None]
        return jnp.transpose(logits, (1, 0, 2)), back(ko), back(vo), backp(kpo), backp(vpo)

    return jax.shard_map(device_fn, mesh=mesh, in_specs=in_specs, out_specs=out_specs, check_vma=False)
```

```python
import functools

import jax
import jax.numpy as jnp
import numpy as np
from jax import lax
from jax.experimental import pallas as pl
from jax.experimental.pallas import tpu as pltpu
from jax.sharding import PartitionSpec as P

F32 = jnp.float32
BF16 = jnp.bfloat16
MESH = pl.DeviceIdType.MESH
NORM_EPS = 1e-6
ROPE_BASE = 10000.0
NEG = -1e30

HID = 576
NQ = 9
NKV = 3
GRP = 3
HD = 64
HALF = 32
KVW = NKV * HD
FFN = 1536
NM = 4
DR = 8
SEG = 64
CL = 512
VOC = 1024
ND = NM * DR
NP = NM * SEG
LAST = 3
LN = 128


def nt(a, b):
    return lax.dot_general(a, b, (((1,), (1,)), ((), ())), preferred_element_type=F32)


def nn(a, b):
    return jnp.dot(a, b, preferred_element_type=F32)


def rms(x, g):
    inv = lax.rsqrt(jnp.mean(x * x, axis=-1, keepdims=True) + NORM_EPS)
    return (x * inv * g).astype(BF16)


def rope_t(m, cos, sin):
    parts = []
    for j in range(m.shape[0] // HD):
        a = m[j * HD:j * HD + HALF]
        b = m[j * HD + HALF:(j + 1) * HD]
        parts += [a * cos - b * sin, b * cos + a * sin]
    return jnp.concatenate(parts, axis=0)


def lane_iota(shape):
    return lax.broadcasted_iota(jnp.int32, shape, len(shape) - 1)


def pipe_kernel(xd, xp, dlen, plen, ga, wq, wk, wv, wo, gm, wg, wu, wd, gf, kd, vd, kp, vp, ifr, tok,
                kdn, vdn, kpn, vpn, fh_o,
                xd_s, xp_s, dl_s, pl_s, ga_s, wq_s, wk_s, wv_s, wo_s, gm_s, wg_s, wu_s, wd_s, gf_s,
                kd_s, vd_s, kp_s, vp_s, ifr_s,
                wqt_s, cosd_s, sind_s, cosp_s, sinp_s, cosl_s, sinl_s, qa_s, qb_s, self_s, vn_s, oa_s, ob_s,
                kdn_s, vdn_s, ot_s, act_s, x4_s, sd_s, sp_s, fh_s,
                in_sem, kd_sem, vd_sem, out_sem, sdd, sdp, rcd, rcp):
    st = lax.axis_index('stage')
    order = [(dlen, dl_s), (plen, pl_s), (xd, xd_s), (ga, ga_s), (ifr, ifr_s), (wq, wq_s), (wk, wk_s), (wv, wv_s),
             (kp, kp_s), (vp, vp_s), (wo, wo_s), (gm, gm_s), (wg, wg_s), (wu, wu_s), (wd, wd_s), (xp, xp_s), (gf, gf_s)]
    cps = [pltpu.make_async_copy(a, b, in_sem.at[i]) for i, (a, b) in enumerate(order)]
    by = {id(b): c for (a, b), c in zip(order, cps)}
    kcp = [pltpu.make_async_copy(kd.at[m], kd_s.at[m], kd_sem.at[m]) for m in range(NM)]
    vcp = [pltpu.make_async_copy(vd.at[m], vd_s.at[m], vd_sem.at[m]) for m in range(NM)]

    def ld(ref):
        return by[id(ref)]

    for r in (dl_s, pl_s, ga_s, ifr_s, wq_s, wk_s, wv_s):
        ld(r).start()

    @pl.when(st == 0)
    def _():
        ld(xd_s).start()

    for m in range(NM):
        kcp[m].start()
        vcp[m].start()
    for r in (wo_s, gm_s, wg_s, wu_s, wd_s, kp_s, vp_s):
        ld(r).start()

    @pl.when(st == 0)
    def _():
        ld(xp_s).start()

    ld(gf_s).start()

    bar = pltpu.get_barrier_semaphore()

    @pl.when(st > 0)
    def _():
        pl.semaphore_signal(bar, inc=1, device_id={'stage': jnp.maximum(st - 1, 0)}, device_id_type=MESH)

    @pl.when(st < LAST)
    def _():
        pl.semaphore_signal(bar, inc=1, device_id={'stage': jnp.minimum(st + 1, LAST)}, device_id_type=MESH)

    ld(dl_s).wait()
    ld(pl_s).wait()
    ld(ifr_s).wait()
    p0 = pl_s[0]
    li = lane_iota((1, LN))
    posd = jnp.zeros((1, LN), jnp.int32)
    for b in range(ND):
        posd = jnp.where(li == b, dl_s[b // DR, b % DR], posd)
    fr = ifr_s[...]
    ang = fr[:, :LN] * posd.astype(F32)
    cosd_s[...] = jnp.cos(ang)
    sind_s[...] = jnp.sin(ang)
    ang = fr * (p0 + lane_iota((1, NP))).astype(F32)
    cosp_s[...] = jnp.cos(ang)
    sinp_s[...] = jnp.sin(ang)
    ang = fr[:, :LN] * (p0 + li * SEG + (SEG - 1)).astype(F32)
    cosl_s[...] = jnp.cos(ang)
    sinl_s[...] = jnp.sin(ang)
    qa_s[...] = jnp.zeros_like(qa_s)
    qb_s[...] = jnp.zeros_like(qb_s)
    ob_s[...] = jnp.zeros_like(ob_s)

    ld(ga_s).wait()
    ld(wq_s).wait()
    wqt_s[...] = wq_s[...].astype(F32).T.astype(BF16)
    ld(wk_s).wait()
    ld(wv_s).wait()
    gat = ga_s[...].astype(F32)

    lgrp = lane_iota((8, KVW)) // HD

    def qkv_dec(h, cos, sin, b0, n):
        hp = jnp.concatenate([h, jnp.zeros((LN - h.shape[0], HID), BF16)], axis=0)
        qt = rope_t(nt(wqt_s[...], hp), cos, sin).astype(BF16).astype(F32)
        kt = rope_t(nt(wk_s[...], hp), cos, sin).astype(BF16).astype(F32)
        vt = nt(wv_s[...], hp).astype(BF16).astype(F32)
        qt = qt * (HD ** -0.5)
        row = lax.broadcasted_iota(jnp.int32, (24, LN), 0)
        sf = jnp.zeros((24, LN), F32)
        for g in range(NKV):
            for r in range(GRP):
                j = g * GRP + r
                s = jnp.sum(qt[j * HD:(j + 1) * HD] * kt[g * HD:(g + 1) * HD], axis=0, keepdims=True)
                sf = jnp.where(row == 8 * g + r, s, sf)
        for r in range(GRP):
            qr = [qt[(g * GRP + r) * HD:(g * GRP + r + 1) * HD] for g in range(NKV)]
            qa_s[pl.ds(b0 * 8 + r, n, stride=8), :] = jnp.concatenate(qr[:2], axis=0).T[:n]
            qb_s[pl.ds(b0 * 8 + r, n, stride=8), :] = jnp.concatenate([qr[2], jnp.zeros((HD, LN), F32)], axis=0).T[:n]
        vn_s[b0:b0 + n, :LN] = vt[:LN].T[:n]
        vn_s[b0:b0 + n, LN:] = jnp.concatenate([vt[LN:], jnp.zeros((HD, LN), F32)], axis=0).T[:n, :HD]
        return kt, vt, sf

    def attn_dec(b, kt, vt, pos, selfcol):
        qb = jnp.concatenate([qa_s[pl.ds(b * 8, 8), :], qb_s[pl.ds(b * 8, 8), :HD]], axis=1)
        lhs = jnp.concatenate([jnp.where(lgrp == g, qb, 0.0) for g in range(NKV)], axis=0).astype(BF16)
        s = nn(lhs, kt)
        s = jnp.where(lane_iota((24, CL)) < pos, s, NEG)
        mx = jnp.maximum(jnp.max(s, axis=-1, keepdims=True), selfcol)
        p = jnp.exp(s - mx)
        ps = jnp.exp(selfcol - mx)
        rl = 1.0 / (jnp.sum(p, axis=-1, keepdims=True) + ps)
        o = nt((p * rl).astype(BF16), vt)
        o = o + (ps * rl).astype(BF16).astype(F32) * vn_s[pl.ds(b, 1), :]
        acc = jnp.where(lgrp == 0, o[0:8], 0.0)
        for g in range(1, NKV):
            acc = jnp.where(lgrp == g, o[8 * g:8 * g + 8], acc)
        oa_s[pl.ds(b * 8, 8), :] = acc[:, :LN]
        ob_s[pl.ds(b * 8, 8), :HD] = acc[:, LN:]

    def self_col(b):
        return jnp.sum(jnp.where(lane_iota((24, LN)) == b, self_s[...], 0.0), axis=-1, keepdims=True)

    def dec_out(b0, n):
        return [jnp.concatenate([oa_s[pl.ds(b0 * 8 + r, n, stride=8), :], ob_s[pl.ds(b0 * 8 + r, n, stride=8), :][:, :HD]], axis=1).astype(BF16)
                for r in range(GRP)]

    def wo_rows(r):
        return jnp.concatenate([wo_s[(g * GRP + r) * HD:(g * GRP + r + 1) * HD, :] for g in range(NKV)], axis=0)

    def mlp(x, rows):
        h2 = rms(x, gm_s[...].astype(F32))
        step = 512
        for c in range(FFN // step):
            gt = nn(h2, wg_s[:, c * step:(c + 1) * step])
            up = nn(h2, wu_s[:, c * step:(c + 1) * step])
            act_s[:rows, c * step:(c + 1) * step] = (gt * (1.0 / (1.0 + jnp.exp(-gt))) * up).astype(BF16)
        return (x + nt(act_s[:rows, :], wd_s[...])).astype(BF16)

    def round32(x):
        return x.astype(BF16).astype(F32)

    def to(k):
        return {'stage': k}

    def hop(src, dst, s_sem, r_sem):
        return pltpu.make_async_remote_copy(src, dst, s_sem, r_sem, device_id=to(jnp.minimum(st + 1, LAST)), device_id_type=MESH)

    @pl.when(st == 0)
    def _():
        ld(xd_s).wait()

    @pl.when(st > 0)
    def _():
        hop(sd_s, xd_s, sdd, rcd).wait_recv()

    hd = rms(xd_s[...].astype(F32), gat)
    ktd, vtd, sfd = qkv_dec(hd, cosd_s[...], sind_s[...], 0, ND)
    self_s[...] = sfd
    kdn_s[...] = ktd
    vdn_s[...] = vtd
    okd = pltpu.make_async_copy(kdn_s, kdn, out_sem.at[0])
    ovd = pltpu.make_async_copy(vdn_s, vdn, out_sem.at[1])
    okd.start()
    ovd.start()

    def dec_loop(m, carry):
        pltpu.make_async_copy(kd.at[m], kd_s.at[m], kd_sem.at[m]).wait()
        pltpu.make_async_copy(vd.at[m], vd_s.at[m], vd_sem.at[m]).wait()
        for i in range(DR):
            b = m * DR + i
            attn_dec(b, kd_s[m, i].reshape(KVW, CL), vd_s[m, i].reshape(KVW, CL), dl_s[m, i], self_col(b))
        return carry

    lax.fori_loop(0, NM, dec_loop, 0)

    for r in (wo_s, gm_s, wg_s, wu_s, wd_s):
        ld(r).wait()

    @pl.when((st == 0) | (st == LAST))
    def _():
        pl.semaphore_wait(bar, 1)

    @pl.when((st > 0) & (st < LAST))
    def _():
        pl.semaphore_wait(bar, 2)

    @pl.when(st < LAST)
    def _():
        a = dec_out(0, ND)
        y = nn(a[0], wo_rows(0)) + nn(a[1], wo_rows(1)) + nn(a[2], wo_rows(2))
        x1 = round32(xd_s[...].astype(F32) + y)
        sd_s[...] = mlp(x1, ND)
        hop(sd_s, xd_s, sdd, rcd).start()

    @pl.when(st == 0)
    def _():
        ld(xp_s).wait()

    @pl.when(st > 0)
    def _():
        hop(sp_s, xp_s, sdp, rcp).wait_recv()

    ld(kp_s).wait()
    ld(vp_s).wait()
    hp = rms(xp_s[...].astype(F32), gat)
    ktp = rope_t(nt(wk_s[...], hp), cosp_s[...], sinp_s[...]).astype(BF16)
    vtp = nt(wv_s[...], hp).astype(BF16)
    place = jnp.where(lax.broadcasted_iota(jnp.int32, (NP, CL), 0) + p0 == lane_iota((NP, CL)), 1.0, 0.0).astype(BF16)
    lp = lane_iota((KVW, CL)) - p0
    fresh = (lp >= 0) & (lp < NP)
    kpu = jnp.where(fresh, nn(ktp, place), kp_s[...].reshape(KVW, CL).astype(F32))
    vpu = jnp.where(fresh, nn(vtp, place), vp_s[...].reshape(KVW, CL).astype(F32))
    kp_s[...] = kpu.astype(BF16).reshape(NKV, HD, CL)
    vp_s[...] = vpu.astype(BF16).reshape(NKV, HD, CL)
    okp = pltpu.make_async_copy(kp_s, kpn, out_sem.at[2])
    ovp = pltpu.make_async_copy(vp_s, vpn, out_sem.at[3])
    okp.start()
    ovp.start()

    @pl.when(st < LAST)
    def _():
        kfull = kpu.T.astype(BF16)
        vfull = vp_s[...].reshape(KVW, CL)
        qt = (rope_t(nt(wqt_s[...], hp), cosp_s[...], sinp_s[...]).astype(BF16).astype(F32) * (HD ** -0.5)).astype(BF16)
        bias = jnp.where(lax.broadcasted_iota(jnp.int32, (CL, NP), 0) <= lane_iota((CL, NP)) + p0, 0.0, NEG)
        for j in range(NQ):
            g = j // GRP
            parts = []
            if g:
                parts.append(jnp.zeros((g * HD, NP), BF16))
            parts.append(qt[j * HD:(j + 1) * HD])
            if g < NKV - 1:
                parts.append(jnp.zeros(((NKV - 1 - g) * HD, NP), BF16))
            s = nn(kfull, jnp.concatenate(parts, axis=0)) + bias
            p = jnp.exp(s - jnp.max(s, axis=0, keepdims=True))
            pr = (p * (1.0 / jnp.sum(p, axis=0, keepdims=True))).astype(BF16)
            ot_s[j * HD:(j + 1) * HD, :] = nn(vfull[g * HD:(g + 1) * HD], pr)
        x1 = round32(xp_s[...].astype(F32) + nn(ot_s[...].T.astype(BF16), wo_s[...]))
        sp_s[...] = mlp(x1, NP)
        hop(sp_s, xp_s, sdp, rcp).start()

    ld(gf_s).wait()

    @pl.when(st == LAST)
    def _():
        x4_s[...] = jnp.zeros_like(x4_s)
        for m in range(NM):
            r0 = m * SEG + SEG - 8
            x4_s[m:m + 1, :] = xp_s[r0:r0 + 8, :].astype(F32)[7:8]
        x4 = x4_s[...]
        h4 = rms(x4, gat)
        h4 = jnp.concatenate([h4, jnp.zeros_like(h4)], axis=0)
        _, _, sf4 = qkv_dec(h4, cosl_s[...], sinl_s[...], ND, 8)
        for m in range(NM):
            col = jnp.sum(jnp.where(lane_iota((24, LN)) == m, sf4, 0.0), axis=-1, keepdims=True)
            attn_dec(ND + m, kp_s[...].reshape(KVW, CL), vp_s[...].reshape(KVW, CL), p0 + m * SEG + SEG - 1, col)
        for m in range(NM, 8):
            oa_s[pl.ds((ND + m) * 8, 8), :] = jnp.zeros((8, LN), F32)
        a = dec_out(0, ND + 8)
        y = nn(a[0], wo_rows(0)) + nn(a[1], wo_rows(1)) + nn(a[2], wo_rows(2))
        x1 = round32(jnp.concatenate([xd_s[...].astype(F32), x4], axis=0) + y)
        x2 = mlp(x1, ND + 8)
        fh = rms(x2.astype(F32), gf_s[...].astype(F32))
        ri = lax.broadcasted_iota(jnp.int32, (ND + 8, ND + 8), 0)
        src = jnp.where(ri < ND, (ri % NM) * DR + ri // NM, ri)
        fh_s[...] = nn(jnp.where(lane_iota((ND + 8, ND + 8)) == src, 1.0, 0.0).astype(BF16), fh).astype(BF16)
        ofh = pltpu.make_async_copy(fh_s, fh_o, out_sem.at[4])
        ofh.start()
        ofh.wait()

    okd.wait()
    ovd.wait()
    okp.wait()
    ovp.wait()

    @pl.when(st < LAST)
    def _():
        hop(sd_s, xd_s, sdd, rcd).wait_send()
        hop(sp_s, xp_s, sdp, rcp).wait_send()


def head_kernel(fh, wh, tok, logits, fh_s, fr_s, wh_s, lsem, ssem, rsem):
    st = lax.axis_index('stage')
    lfh = pltpu.make_async_copy(fh, fh_s, lsem.at[0])
    lwh = pltpu.make_async_copy(wh, wh_s, lsem.at[1])

    @pl.when(st == LAST)
    def _():
        lfh.start()

    lwh.start()
    bar = pltpu.get_barrier_semaphore()

    def send(k):
        return pltpu.make_async_remote_copy(fh_s, fr_s, ssem.at[k], rsem, device_id={'stage': k}, device_id_type=MESH)

    def head(ref):
        lwh.wait()
        lg = nn(ref[...], wh_s[...])
        for i in range(DR + 1):
            logits[i] = lg[i * NM:(i + 1) * NM]

    @pl.when(st < LAST)
    def _():
        pl.semaphore_signal(bar, inc=1, device_id={'stage': LAST}, device_id_type=MESH)

    @pl.when(st == LAST)
    def _():
        for k in range(LAST):
            pl.semaphore_signal(bar, inc=1, device_id={'stage': k}, device_id_type=MESH)
        pl.semaphore_wait(bar, LAST)
        lfh.wait()
        for k in range(LAST):
            send(k).start()
        head(fh_s)
        for k in range(LAST):
            send(k).wait_send()

    @pl.when(st < LAST)
    def _():
        pl.semaphore_wait(bar, 1)
        send(0).wait_recv()
        head(fr_s)


def tile_start(pos):
    return pl.ds(pl.multiple_of((pos // LN) * LN, LN), LN)


def copy_all(kd, vd, ko, vo, ks, vs, ksem, vsem, edit):
    ins = [(pltpu.make_async_copy(kd.at[m], ks.at[m], ksem.at[m]), pltpu.make_async_copy(vd.at[m], vs.at[m], vsem.at[m])) for m in range(NM)]
    for a, b in ins:
        a.start()
        b.start()
    outs = []
    for m in range(NM):
        for c, scr, out, sem, w in ((ins[m][0], ks, ko, ksem, 0), (ins[m][1], vs, vo, vsem, 1)):
            c.wait()
            if edit is not None:
                edit(m, scr, w)
            o = pltpu.make_async_copy(scr.at[m], out.at[m], sem.at[m])
            o.start()
            outs.append(o)
    for o in outs:
        o.wait()


def pre_kernel(kd, vd, ko, vo, tok, ks, vs, ksem, vsem):
    st = lax.axis_index('stage')
    tok[...] = jnp.zeros_like(tok)

    @pl.when(st >= 2)
    def _():
        copy_all(kd, vd, ko, vo, ks, vs, ksem, vsem, None)


def load_new(srcs, dsts, sem):
    cs = [pltpu.make_async_copy(a, b, sem.at[i]) for i, (a, b) in enumerate(zip(srcs, dsts))]
    for c in cs:
        c.start()
    return cs


def update_tiles(dlen, bk, bv, ko, vo, kpo, vpo, kt, vt, new, cs, ksem, vsem, nsem):
    lane = lane_iota((HD, LN))

    def cp(hbm, scr, sem, m, i, out):
        h = hbm.at[m, i, :, :, tile_start(dlen[m, i])]
        v = scr.at[m, i]
        return pltpu.make_async_copy(v, h, sem.at[m]) if out else pltpu.make_async_copy(h, v, sem.at[m])

    for m in range(NM):
        for i in range(DR):
            cp(bk, kt, ksem, m, i, False).start()
            cp(bv, vt, vsem, m, i, False).start()
    for c in cs:
        c.wait()
    po = [pltpu.make_async_copy(new[2], kpo, nsem.at[2]), pltpu.make_async_copy(new[3], vpo, nsem.at[3])]
    for o in po:
        o.start()
    for m in range(NM):
        for hbm, scr, sem, nw in ((ko, kt, ksem, new[0]), (vo, vt, vsem, new[1])):
            for i in range(DR):
                cp(hbm, scr, sem, m, i, False).wait()
            for i in range(DR):
                pos = dlen[m, i]
                for g in range(NKV):
                    col = nw[g * HD:(g + 1) * HD, m * DR + i:m * DR + i + 1]
                    scr[m, i, g] = jnp.where(lane == pos % LN, col, scr[m, i, g].astype(F32)).astype(BF16)
            for i in range(DR):
                cp(hbm, scr, sem, m, i, True).start()
    for m in range(NM):
        for i in range(DR):
            cp(ko, kt, ksem, m, i, True).wait()
            cp(vo, vt, vsem, m, i, True).wait()
    for o in po:
        o.wait()


def mid_kernel(dlen, kd, vd, bk, bv, kdn, vdn, kpn, vpn, ko, vo, kpo, vpo, tok, ks, vs, kt, vt, kn_s, vn_s, kp_s, vp_s, ksem, vsem, nsem):
    st = lax.axis_index('stage')
    tok[...] = jnp.zeros_like(tok)
    new = (kn_s, vn_s, kp_s, vp_s)

    @pl.when(st < 2)
    def _():
        cs = load_new((kdn, vdn, kpn, vpn), new, nsem)
        for c in cs:
            c.wait()
        po = [pltpu.make_async_copy(kp_s, kpo, nsem.at[2]), pltpu.make_async_copy(vp_s, vpo, nsem.at[3])]
        for o in po:
            o.start()
        lane = lane_iota((HD, LN))

        def edit(m, scr, w):
            for i in range(DR):
                pos = dlen[m, i]
                sl = tile_start(pos)
                for g in range(NKV):
                    col = new[w][g * HD:(g + 1) * HD, m * DR + i:m * DR + i + 1]
                    scr[m, i, g, :, sl] = jnp.where(lane == pos % LN, col, scr[m, i, g, :, sl].astype(F32)).astype(BF16)

        copy_all(kd, vd, ko, vo, ks, vs, ksem, vsem, edit)
        for o in po:
            o.wait()

    @pl.when(st == 2)
    def _():
        cs = load_new((kdn, vdn, kpn, vpn), new, nsem)
        update_tiles(dlen, bk, bv, ko, vo, kpo, vpo, kt, vt, new, cs, ksem, vsem, nsem)


def post_kernel(dlen, kdn, vdn, kpn, vpn, lg, bk, bv, bkp, bvp, ko, vo, kpo, vpo, kt, vt, kn_s, vn_s, kp_s, vp_s, ksem, vsem, nsem):
    st = lax.axis_index('stage')

    @pl.when(st == LAST)
    def _():
        new = (kn_s, vn_s, kp_s, vp_s)
        cs = load_new((kdn, vdn, kpn, vpn), new, nsem)
        update_tiles(dlen, bk, bv, ko, vo, kpo, vpo, kt, vt, new, cs, ksem, vsem, nsem)


ANY = pl.BlockSpec(memory_space=pltpu.HBM)


def solution(mesh):
    part = P('replica')
    layer = P('stage')
    cache = P('stage', 'replica')
    in_specs = (part,) * 4 + (layer,) * 9 + (P(), P()) + (cache,) * 4
    out_specs = (part,) + (cache,) * 4
    inv_freq = np.float32(ROPE_BASE) ** (-np.arange(HALF, dtype=np.float32) * np.float32(2.0 / HD))
    ifr_c = np.broadcast_to(inv_freq[:, None], (HALF, NP)).astype(np.float32)

    def device_fn(x_dec, x_pre, dec_len, pre_len, g_attn, w_q, w_k, w_v, w_o, g_mlp, w_gate, w_up, w_down, g_final, w_head, k_dec, v_dec, k_pre, v_pre):
        kd = jnp.transpose(k_dec[0], (0, 1, 3, 4, 2))
        vd = jnp.transpose(v_dec[0], (0, 1, 3, 4, 2))
        kp = jnp.transpose(k_pre[0], (1, 2, 0))
        vp = jnp.transpose(v_pre[0], (1, 2, 0))
        args = (x_dec.reshape(ND, HID), x_pre.reshape(NP, HID), dec_len, pre_len, g_attn, w_q[0], w_k[0].T, w_v[0].T, w_o[0], g_mlp,
                w_gate[0], w_up[0], w_down[0].T, g_final.reshape(1, HID), kd, vd, kp, vp, jnp.asarray(ifr_c))
        vm = lambda shape, dt: pltpu.VMEM(shape, dt)
        scratch = [
            vm((ND, HID), BF16), vm((NP, HID), BF16), pltpu.SMEM((NM, DR), jnp.int32), pltpu.SMEM((1,), jnp.int32), vm((1, HID), BF16),
            vm((HID, HID), BF16), vm((KVW, HID), BF16), vm((KVW, HID), BF16), vm((HID, HID), BF16), vm((1, HID), BF16),
            vm((HID, FFN), BF16), vm((HID, FFN), BF16), vm((HID, FFN), BF16), vm((1, HID), BF16),
            vm(kd.shape, BF16), vm(vd.shape, BF16), vm(kp.shape, BF16), vm(vp.shape, BF16), vm((HALF, NP), F32),
            vm((HID, HID), BF16), vm((HALF, LN), F32), vm((HALF, LN), F32), vm((HALF, NP), F32), vm((HALF, NP), F32),
            vm((HALF, LN), F32), vm((HALF, LN), F32),
            vm(((ND + 8) * 8, LN), F32), vm(((ND + 8) * 8, LN), F32), vm((24, LN), F32), vm((ND + 8, KVW), F32),
            vm(((ND + 8) * 8, LN), F32), vm(((ND + 8) * 8, LN), F32),
            vm((KVW, LN), F32), vm((KVW, LN), F32), vm((HID, NP), F32), vm((NP, FFN), BF16), vm((8, HID), F32),
            vm((ND, HID), BF16), vm((NP, HID), BF16), vm((ND + 8, HID), BF16),
            pltpu.SemaphoreType.DMA((17,)), pltpu.SemaphoreType.DMA((NM,)), pltpu.SemaphoreType.DMA((NM,)), pltpu.SemaphoreType.DMA((5,)),
            pltpu.SemaphoreType.DMA, pltpu.SemaphoreType.DMA, pltpu.SemaphoreType.DMA, pltpu.SemaphoreType.DMA,
        ]
        sds = jax.ShapeDtypeStruct
        big = pltpu.CompilerParams(vmem_limit_bytes=62 * 1024 * 1024)
        cshape = sds(kd.shape, BF16)
        pshape = sds(kp.shape, BF16)
        nsems = [pltpu.SemaphoreType.DMA((NM,)), pltpu.SemaphoreType.DMA((NM,))]
        tile = vm((NM, DR, NKV, HD, LN), BF16)
        news = [vm((KVW, LN), F32), vm((KVW, LN), F32), vm(kp.shape, BF16), vm(vp.shape, BF16)]
        smem = pl.BlockSpec(memory_space=pltpu.SMEM)
        vmem = pl.BlockSpec(memory_space=pltpu.VMEM)
        tshape = sds((8, LN), F32)
        bk, bv, tok = pl.pallas_call(
            pre_kernel, out_shape=(cshape, cshape, tshape), in_specs=[ANY, ANY], out_specs=(ANY, ANY, vmem),
            scratch_shapes=[vm(kd.shape, BF16), vm(vd.shape, BF16)] + nsems, name='pre', compiler_params=big)(kd, vd)
        args = args + (tok,)
        kdn, vdn, kpn, vpn, fh = pl.pallas_call(
            pipe_kernel,
            out_shape=(sds((KVW, LN), F32), sds((KVW, LN), F32), pshape, pshape, sds((ND + 8, HID), BF16)),
            in_specs=[ANY] * len(args),
            out_specs=(ANY,) * 5,
            scratch_shapes=scratch,
            name='pipe',
            compiler_params=pltpu.CompilerParams(collective_id=0, has_side_effects=True, vmem_limit_bytes=62 * 1024 * 1024),
        )(*args)
        bk, bv, bkp, bvp, tok2 = pl.pallas_call(
            mid_kernel, out_shape=(cshape, cshape, pshape, pshape, tshape), in_specs=[smem] + [ANY] * 8, out_specs=(ANY,) * 4 + (vmem,),
            input_output_aliases={3: 0, 4: 1},
            scratch_shapes=[vm(kd.shape, BF16), vm(vd.shape, BF16), tile, tile] + news + nsems + [pltpu.SemaphoreType.DMA((4,))],
            name='mid', compiler_params=big)(dec_len, kd, vd, bk, bv, kdn, vdn, kpn, vpn)
        logits = pl.pallas_call(
            head_kernel, out_shape=sds((DR + 1, NM, VOC), F32), in_specs=[ANY] * 3, out_specs=vmem,
            scratch_shapes=[vm((ND + 8, HID), BF16), vm((ND + 8, HID), BF16), vm((HID, VOC), BF16),
                            pltpu.SemaphoreType.DMA((2,)), pltpu.SemaphoreType.DMA((LAST,)), pltpu.SemaphoreType.DMA],
            name='head', compiler_params=pltpu.CompilerParams(collective_id=1, has_side_effects=True))(fh, w_head, tok2)
        ko, vo, kpo, vpo = pl.pallas_call(
            post_kernel, out_shape=(cshape, cshape, pshape, pshape), in_specs=[smem] + [ANY] * 9, out_specs=(ANY,) * 4,
            input_output_aliases={6: 0, 7: 1, 8: 2, 9: 3},
            scratch_shapes=[tile, tile] + news + nsems + [pltpu.SemaphoreType.DMA((4,))],
            name='post', compiler_params=big)(dec_len, kdn, vdn, kpn, vpn, logits, bk, bv, bkp, bvp)
        back = lambda a: jnp.transpose(a, (0, 1, 4, 2, 3))[None]
        backp = lambda a: jnp.transpose(a, (2, 0, 1))[None]
        return jnp.transpose(logits, (1, 0, 2)), back(ko), back(vo), backp(kpo), backp(vpo)

    return jax.shard_map(device_fn, mesh=mesh, in_specs=in_specs, out_specs=out_specs, check_vma=False)
```

```python
import functools

import jax
import jax.numpy as jnp
import numpy as np
from jax import lax
from jax.experimental import pallas as pl
from jax.experimental.pallas import tpu as pltpu
from jax.sharding import PartitionSpec as P

F32 = jnp.float32
BF16 = jnp.bfloat16
MESH = pl.DeviceIdType.MESH
NORM_EPS = 1e-6
ROPE_BASE = 10000.0
NEG = -1e30

HID = 576
NQ = 9
NKV = 3
GRP = 3
HD = 64
HALF = 32
KVW = NKV * HD
FFN = 1536
NM = 4
DR = 8
SEG = 64
CL = 512
VOC = 1024
ND = NM * DR
NP = NM * SEG
LAST = 3
LN = 128


def nt(a, b):
    return lax.dot_general(a, b, (((1,), (1,)), ((), ())), preferred_element_type=F32)


def nn(a, b):
    return jnp.dot(a, b, preferred_element_type=F32)


def rms(x, g):
    inv = lax.rsqrt(jnp.mean(x * x, axis=-1, keepdims=True) + NORM_EPS)
    return (x * inv * g).astype(BF16)


def rope_t(m, cos, sin):
    parts = []
    for j in range(m.shape[0] // HD):
        a = m[j * HD:j * HD + HALF]
        b = m[j * HD + HALF:(j + 1) * HD]
        parts += [a * cos - b * sin, b * cos + a * sin]
    return jnp.concatenate(parts, axis=0)


def lane_iota(shape):
    return lax.broadcasted_iota(jnp.int32, shape, len(shape) - 1)


def pipe_kernel(xd, xp, dlen, plen, ga, wq, wk, wv, wo, gm, wg, wu, wd, gf, kd, vd, kp, vp, ifr, tok,
                kdn, vdn, kpn, vpn, fh_o,
                xd_s, xp_s, dl_s, pl_s, ga_s, wq_s, wk_s, wv_s, wo_s, gm_s, wg_s, wu_s, wd_s, gf_s,
                kd_s, vd_s, kp_s, vp_s, ifr_s,
                wqt_s, cosd_s, sind_s, cosp_s, sinp_s, cosl_s, sinl_s, qa_s, qb_s, self_s, vn_s, oa_s, ob_s,
                kdn_s, vdn_s, sc_s, ps_s, pb_s, bias_s, ot_s, act_s, x4_s, sd_s, sp_s, fh_s,
                in_sem, kd_sem, vd_sem, out_sem, sdd, sdp, rcd, rcp):
    st = lax.axis_index('stage')
    order = [(dlen, dl_s), (plen, pl_s), (xd, xd_s), (ga, ga_s), (ifr, ifr_s), (wq, wq_s), (wk, wk_s), (wv, wv_s),
             (kp, kp_s), (vp, vp_s), (wo, wo_s), (gm, gm_s), (wg, wg_s), (wu, wu_s), (wd, wd_s), (xp, xp_s), (gf, gf_s)]
    cps = [pltpu.make_async_copy(a, b, in_sem.at[i]) for i, (a, b) in enumerate(order)]
    by = {id(b): c for (a, b), c in zip(order, cps)}
    kcp = [pltpu.make_async_copy(kd.at[m], kd_s.at[m], kd_sem.at[m]) for m in range(NM)]
    vcp = [pltpu.make_async_copy(vd.at[m], vd_s.at[m], vd_sem.at[m]) for m in range(NM)]

    def ld(ref):
        return by[id(ref)]

    for r in (dl_s, pl_s, ga_s, ifr_s, wq_s, wk_s, wv_s):
        ld(r).start()

    @pl.when(st == 0)
    def _():
        ld(xd_s).start()

    for m in range(NM):
        kcp[m].start()
        vcp[m].start()
    for r in (wo_s, gm_s, wg_s, wu_s, wd_s, kp_s, vp_s):
        ld(r).start()

    @pl.when(st == 0)
    def _():
        ld(xp_s).start()

    ld(gf_s).start()

    bar = pltpu.get_barrier_semaphore()

    @pl.when(st > 0)
    def _():
        pl.semaphore_signal(bar, inc=1, device_id={'stage': jnp.maximum(st - 1, 0)}, device_id_type=MESH)

    @pl.when(st < LAST)
    def _():
        pl.semaphore_signal(bar, inc=1, device_id={'stage': jnp.minimum(st + 1, LAST)}, device_id_type=MESH)

    ld(dl_s).wait()
    ld(pl_s).wait()
    ld(ifr_s).wait()
    p0 = pl_s[0]
    li = lane_iota((1, LN))
    posd = jnp.zeros((1, LN), jnp.int32)
    for b in range(ND):
        posd = jnp.where(li == b, dl_s[b // DR, b % DR], posd)
    fr = ifr_s[...]
    ang = fr[:, :LN] * posd.astype(F32)
    cosd_s[...] = jnp.cos(ang)
    sind_s[...] = jnp.sin(ang)
    ang = fr * (p0 + lane_iota((1, NP))).astype(F32)
    cosp_s[...] = jnp.cos(ang)
    sinp_s[...] = jnp.sin(ang)
    ang = fr[:, :LN] * (p0 + li * SEG + (SEG - 1)).astype(F32)
    cosl_s[...] = jnp.cos(ang)
    sinl_s[...] = jnp.sin(ang)
    qa_s[...] = jnp.zeros_like(qa_s)
    qb_s[...] = jnp.zeros_like(qb_s)
    ob_s[...] = jnp.zeros_like(ob_s)

    ld(ga_s).wait()
    ld(wq_s).wait()
    wqt_s[...] = wq_s[...].astype(F32).T.astype(BF16)
    ld(wk_s).wait()
    ld(wv_s).wait()
    gat = ga_s[...].astype(F32)

    lgrp = lane_iota((8, KVW)) // HD

    def qkv_dec(h, cos, sin, b0, n):
        hp = jnp.concatenate([h, jnp.zeros((LN - h.shape[0], HID), BF16)], axis=0)
        qt = rope_t(nt(wqt_s[...], hp), cos, sin).astype(BF16).astype(F32)
        kt = rope_t(nt(wk_s[...], hp), cos, sin).astype(BF16).astype(F32)
        vt = nt(wv_s[...], hp).astype(BF16).astype(F32)
        qt = qt * (HD ** -0.5)
        row = lax.broadcasted_iota(jnp.int32, (24, LN), 0)
        sf = jnp.zeros((24, LN), F32)
        for g in range(NKV):
            for r in range(GRP):
                j = g * GRP + r
                s = jnp.sum(qt[j * HD:(j + 1) * HD] * kt[g * HD:(g + 1) * HD], axis=0, keepdims=True)
                sf = jnp.where(row == 8 * g + r, s, sf)
        for r in range(GRP):
            qr = [qt[(g * GRP + r) * HD:(g * GRP + r + 1) * HD] for g in range(NKV)]
            qa_s[pl.ds(b0 * 8 + r, n, stride=8), :] = jnp.concatenate(qr[:2], axis=0).T[:n]
            qb_s[pl.ds(b0 * 8 + r, n, stride=8), :] = jnp.concatenate([qr[2], jnp.zeros((HD, LN), F32)], axis=0).T[:n]
        vn_s[b0:b0 + n, :LN] = vt[:LN].T[:n]
        vn_s[b0:b0 + n, LN:] = jnp.concatenate([vt[LN:], jnp.zeros((HD, LN), F32)], axis=0).T[:n, :HD]
        return kt, vt, sf

    def dec_scores(b, kt, slot):
        qb = jnp.concatenate([qa_s[b * 8:b * 8 + 8, :], qb_s[b * 8:b * 8 + 8, :HD]], axis=1)
        lhs = jnp.concatenate([jnp.where(lgrp == g, qb, 0.0) for g in range(NKV)], axis=0).astype(BF16)
        sc_s[slot * 24:slot * 24 + 24, :] = nn(lhs, kt)

    def dec_mix(b, vt, pos, selfcol, slot):
        s = jnp.where(lane_iota((24, CL)) < pos, sc_s[slot * 24:slot * 24 + 24, :], NEG)
        mx = jnp.maximum(jnp.max(s, axis=-1, keepdims=True), selfcol)
        p = jnp.exp(s - mx)
        ps = jnp.exp(selfcol - mx)
        rl = 1.0 / (jnp.sum(p, axis=-1, keepdims=True) + ps)
        o = nt((p * rl).astype(BF16), vt)
        o = o + (ps * rl).astype(BF16).astype(F32) * vn_s[b:b + 1, :]
        acc = jnp.where(lgrp == 0, o[0:8], 0.0)
        for g in range(1, NKV):
            acc = jnp.where(lgrp == g, o[8 * g:8 * g + 8], acc)
        oa_s[b * 8:b * 8 + 8, :] = acc[:, :LN]
        ob_s[b * 8:b * 8 + 8, :HD] = acc[:, LN:]

    def self_col(b):
        return jnp.sum(jnp.where(lane_iota((24, LN)) == b, self_s[...], 0.0), axis=-1, keepdims=True)

    def dec_out(b0, n):
        return [jnp.concatenate([oa_s[pl.ds(b0 * 8 + r, n, stride=8), :], ob_s[pl.ds(b0 * 8 + r, n, stride=8), :][:, :HD]], axis=1).astype(BF16)
                for r in range(GRP)]

    def wo_rows(r):
        return jnp.concatenate([wo_s[(g * GRP + r) * HD:(g * GRP + r + 1) * HD, :] for g in range(NKV)], axis=0)

    def mlp(x, rows):
        h2 = rms(x, gm_s[...].astype(F32))
        step = 512
        for c in range(FFN // step):
            gt = nn(h2, wg_s[:, c * step:(c + 1) * step])
            up = nn(h2, wu_s[:, c * step:(c + 1) * step])
            act_s[:rows, c * step:(c + 1) * step] = (gt * (1.0 / (1.0 + jnp.exp(-gt))) * up).astype(BF16)
        return (x + nt(act_s[:rows, :], wd_s[...])).astype(BF16)

    def round32(x):
        return x.astype(BF16).astype(F32)

    def to(k):
        return {'stage': k}

    def hop(src, dst, s_sem, r_sem):
        return pltpu.make_async_remote_copy(src, dst, s_sem, r_sem, device_id=to(jnp.minimum(st + 1, LAST)), device_id_type=MESH)

    @pl.when(st == 0)
    def _():
        ld(xd_s).wait()

    @pl.when(st > 0)
    def _():
        hop(sd_s, xd_s, sdd, rcd).wait_recv()

    hd = rms(xd_s[...].astype(F32), gat)
    ktd, vtd, sfd = qkv_dec(hd, cosd_s[...], sind_s[...], 0, ND)
    self_s[...] = sfd
    kdn_s[...] = ktd
    vdn_s[...] = vtd
    okd = pltpu.make_async_copy(kdn_s, kdn, out_sem.at[0])
    ovd = pltpu.make_async_copy(vdn_s, vdn, out_sem.at[1])
    okd.start()
    ovd.start()

    def dec_qk(m):
        for i in range(DR):
            dec_scores(m * DR + i, kd_s[m, i].reshape(KVW, CL), (m % 2) * DR + i)

    kcp[0].wait()
    dec_qk(0)
    for m in range(NM):
        if m + 1 < NM:
            kcp[m + 1].wait()
        vcp[m].wait()
        if m + 1 < NM:
            dec_qk(m + 1)
        for i in range(DR):
            b = m * DR + i
            dec_mix(b, vd_s[m, i].reshape(KVW, CL), dl_s[m, i], self_col(b), (m % 2) * DR + i)

    for r in (wo_s, gm_s, wg_s, wu_s, wd_s):
        ld(r).wait()

    @pl.when((st == 0) | (st == LAST))
    def _():
        pl.semaphore_wait(bar, 1)

    @pl.when((st > 0) & (st < LAST))
    def _():
        pl.semaphore_wait(bar, 2)

    @pl.when(st < LAST)
    def _():
        a = dec_out(0, ND)
        y = nn(a[0], wo_rows(0)) + nn(a[1], wo_rows(1)) + nn(a[2], wo_rows(2))
        x1 = round32(xd_s[...].astype(F32) + y)
        sd_s[...] = mlp(x1, ND)
        hop(sd_s, xd_s, sdd, rcd).start()

    @pl.when(st == 0)
    def _():
        ld(xp_s).wait()

    @pl.when(st > 0)
    def _():
        hop(sp_s, xp_s, sdp, rcp).wait_recv()

    ld(kp_s).wait()
    ld(vp_s).wait()
    hp = rms(xp_s[...].astype(F32), gat)
    ktp = rope_t(nt(wk_s[...], hp), cosp_s[...], sinp_s[...]).astype(BF16)
    vtp = nt(wv_s[...], hp).astype(BF16)
    place = jnp.where(lax.broadcasted_iota(jnp.int32, (NP, CL), 0) + p0 == lane_iota((NP, CL)), 1.0, 0.0).astype(BF16)
    lp = lane_iota((KVW, CL)) - p0
    fresh = (lp >= 0) & (lp < NP)
    kpu = jnp.where(fresh, nn(ktp, place), kp_s[...].reshape(KVW, CL).astype(F32))
    vpu = jnp.where(fresh, nn(vtp, place), vp_s[...].reshape(KVW, CL).astype(F32))
    kp_s[...] = kpu.astype(BF16).reshape(NKV, HD, CL)
    vp_s[...] = vpu.astype(BF16).reshape(NKV, HD, CL)
    okp = pltpu.make_async_copy(kp_s, kpn, out_sem.at[2])
    ovp = pltpu.make_async_copy(vp_s, vpn, out_sem.at[3])
    okp.start()
    ovp.start()

    @pl.when(st < LAST)
    def _():
        kfull = kpu.T.astype(BF16)
        vfull = vp_s[...].reshape(KVW, CL)
        qt = (rope_t(nt(wqt_s[...], hp), cosp_s[...], sinp_s[...]).astype(BF16).astype(F32) * (HD ** -0.5)).astype(BF16)
        bias_s[...] = jnp.where(lax.broadcasted_iota(jnp.int32, (CL, NP), 0) <= lane_iota((CL, NP)) + p0, 0.0, NEG)
        hi = (CL - LN, CL)

        def scores(j):
            g = j // GRP
            parts = []
            if g:
                parts.append(jnp.zeros((g * HD, NP), BF16))
            parts.append(qt[j * HD:(j + 1) * HD])
            if g < NKV - 1:
                parts.append(jnp.zeros(((NKV - 1 - g) * HD, NP), BF16))
            ps_s[j % 2] = nn(kfull, jnp.concatenate(parts, axis=0))

        def fold(x, op):
            x = x.reshape(x.shape[0] // 8, 8, x.shape[1])
            return op(x, axis=0)

        def mix(j):
            g = j // GRP
            sl = j % 2
            ck = 64
            for h in range(2):
                ln = slice(h * LN, (h + 1) * LN)
                mx = jnp.full((8, LN), NEG, F32)
                for c in range(0, hi[h], ck):
                    mx = jnp.maximum(mx, fold(ps_s[sl, c:c + ck, ln] + bias_s[c:c + ck, ln], jnp.max))
                mx = jnp.max(mx, axis=0, keepdims=True)
                sm = jnp.zeros((8, LN), F32)
                for c in range(0, hi[h], ck):
                    p = jnp.exp(ps_s[sl, c:c + ck, ln] + bias_s[c:c + ck, ln] - mx)
                    ps_s[sl, c:c + ck, ln] = p
                    sm = sm + fold(p, jnp.sum)
                rl = 1.0 / jnp.sum(sm, axis=0, keepdims=True)
                for c in range(0, hi[h], ck):
                    pb_s[sl, c:c + ck, ln] = (ps_s[sl, c:c + ck, ln] * rl).astype(BF16)
            ot_s[j * HD:(j + 1) * HD, :] = nn(vfull[g * HD:(g + 1) * HD], pb_s[sl])

        for k in range(2):
            pb_s[k, CL - LN:, :LN] = jnp.zeros((LN, LN), BF16)
        scores(0)
        for j in range(NQ):
            if j + 1 < NQ:
                scores(j + 1)
            mix(j)
        x1 = round32(xp_s[...].astype(F32) + nn(ot_s[...].T.astype(BF16), wo_s[...]))
        sp_s[...] = mlp(x1, NP)
        hop(sp_s, xp_s, sdp, rcp).start()

    ld(gf_s).wait()

    @pl.when(st == LAST)
    def _():
        x4_s[...] = jnp.zeros_like(x4_s)
        for m in range(NM):
            r0 = m * SEG + SEG - 8
            x4_s[m:m + 1, :] = xp_s[r0:r0 + 8, :].astype(F32)[7:8]
        x4 = x4_s[...]
        h4 = rms(x4, gat)
        h4 = jnp.concatenate([h4, jnp.zeros_like(h4)], axis=0)
        _, _, sf4 = qkv_dec(h4, cosl_s[...], sinl_s[...], ND, 8)
        for m in range(NM):
            dec_scores(ND + m, kp_s[...].reshape(KVW, CL), m)
        for m in range(NM):
            col = jnp.sum(jnp.where(lane_iota((24, LN)) == m, sf4, 0.0), axis=-1, keepdims=True)
            dec_mix(ND + m, vp_s[...].reshape(KVW, CL), p0 + m * SEG + SEG - 1, col, m)
        for m in range(NM, 8):
            oa_s[pl.ds((ND + m) * 8, 8), :] = jnp.zeros((8, LN), F32)
        a = dec_out(0, ND + 8)
        y = nn(a[0], wo_rows(0)) + nn(a[1], wo_rows(1)) + nn(a[2], wo_rows(2))
        x1 = round32(jnp.concatenate([xd_s[...].astype(F32), x4], axis=0) + y)
        x2 = mlp(x1, ND + 8)
        fh = rms(x2.astype(F32), gf_s[...].astype(F32).reshape(1, HID))
        ri = lax.broadcasted_iota(jnp.int32, (ND + 8, ND + 8), 0)
        src = jnp.where(ri < ND, (ri % NM) * DR + ri // NM, ri)
        fh_s[...] = nn(jnp.where(lane_iota((ND + 8, ND + 8)) == src, 1.0, 0.0).astype(BF16), fh).astype(BF16)
        ofh = pltpu.make_async_copy(fh_s, fh_o, out_sem.at[4])
        ofh.start()
        ofh.wait()

    okd.wait()
    ovd.wait()
    okp.wait()
    ovp.wait()

    @pl.when(st < LAST)
    def _():
        hop(sd_s, xd_s, sdd, rcd).wait_send()
        hop(sp_s, xp_s, sdp, rcp).wait_send()


def head_kernel(fh, wh, tok, logits, fh_s, fr_s, wh_s, lsem, ssem, rsem):
    st = lax.axis_index('stage')
    lfh = pltpu.make_async_copy(fh, fh_s, lsem.at[0])
    lwh = pltpu.make_async_copy(wh, wh_s, lsem.at[1])

    @pl.when(st == LAST)
    def _():
        lfh.start()

    lwh.start()
    bar = pltpu.get_barrier_semaphore()

    def send(k):
        return pltpu.make_async_remote_copy(fh_s, fr_s, ssem.at[k], rsem, device_id={'stage': k}, device_id_type=MESH)

    def head(ref):
        lwh.wait()
        lg = nn(ref[...], wh_s[...])
        for i in range(DR + 1):
            logits[i] = lg[i * NM:(i + 1) * NM]

    @pl.when(st < LAST)
    def _():
        pl.semaphore_signal(bar, inc=1, device_id={'stage': LAST}, device_id_type=MESH)

    @pl.when(st == LAST)
    def _():
        for k in range(LAST):
            pl.semaphore_signal(bar, inc=1, device_id={'stage': k}, device_id_type=MESH)
        pl.semaphore_wait(bar, LAST)
        lfh.wait()
        for k in range(LAST):
            send(k).start()
        head(fh_s)
        for k in range(LAST):
            send(k).wait_send()

    @pl.when(st < LAST)
    def _():
        pl.semaphore_wait(bar, 1)
        send(0).wait_recv()
        head(fr_s)


def tile_start(pos):
    return pl.ds(pl.multiple_of((pos // LN) * LN, LN), LN)


def copy_all(kd, vd, ko, vo, ks, vs, ksem, vsem, edit):
    ins = [(pltpu.make_async_copy(kd.at[m], ks.at[m], ksem.at[m]), pltpu.make_async_copy(vd.at[m], vs.at[m], vsem.at[m])) for m in range(NM)]
    for a, b in ins:
        a.start()
        b.start()
    outs = []
    for m in range(NM):
        for c, scr, out, sem, w in ((ins[m][0], ks, ko, ksem, 0), (ins[m][1], vs, vo, vsem, 1)):
            c.wait()
            if edit is not None:
                edit(m, scr, w)
            o = pltpu.make_async_copy(scr.at[m], out.at[m], sem.at[m])
            o.start()
            outs.append(o)
    for o in outs:
        o.wait()


def pre_kernel(kd, vd, ko, vo, tok, ks, vs, ksem, vsem):
    st = lax.axis_index('stage')

    @pl.when(st >= 2)
    def _():
        copy_all(kd, vd, ko, vo, ks, vs, ksem, vsem, None)


def load_new(srcs, dsts, sem):
    cs = [pltpu.make_async_copy(a, b, sem.at[i]) for i, (a, b) in enumerate(zip(srcs, dsts))]
    for c in cs:
        c.start()
    return cs


def update_tiles(dlen, bk, bv, ko, vo, kpo, vpo, kt, vt, new, cs, ksem, vsem, nsem):
    lane = lane_iota((HD, LN))

    def cp(hbm, scr, sem, m, i, out):
        h = hbm.at[m, i, :, :, tile_start(dlen[m, i])]
        v = scr.at[m, i]
        return pltpu.make_async_copy(v, h, sem.at[m]) if out else pltpu.make_async_copy(h, v, sem.at[m])

    cs[4].wait()
    for m in range(NM):
        for i in range(DR):
            cp(bk, kt, ksem, m, i, False).start()
            cp(bv, vt, vsem, m, i, False).start()
    for c in cs[:4]:
        c.wait()
    po = [pltpu.make_async_copy(new[2], kpo, nsem.at[2]), pltpu.make_async_copy(new[3], vpo, nsem.at[3])]
    for o in po:
        o.start()
    for m in range(NM):
        for hbm, scr, sem, nw in ((ko, kt, ksem, new[0]), (vo, vt, vsem, new[1])):
            for i in range(DR):
                cp(hbm, scr, sem, m, i, False).wait()
            for i in range(DR):
                pos = dlen[m, i]
                for g in range(NKV):
                    col = nw[g * HD:(g + 1) * HD, m * DR + i:m * DR + i + 1]
                    scr[m, i, g] = jnp.where(lane == pos % LN, col, scr[m, i, g].astype(F32)).astype(BF16)
            for i in range(DR):
                cp(hbm, scr, sem, m, i, True).start()
    for m in range(NM):
        for i in range(DR):
            cp(ko, kt, ksem, m, i, True).wait()
            cp(vo, vt, vsem, m, i, True).wait()
    for o in po:
        o.wait()


def mid_kernel(dlen_h, kd, vd, bk, bv, kdn, vdn, kpn, vpn, ko, vo, kpo, vpo, tok, ks, vs, kt, vt, kn_s, vn_s, kp_s, vp_s, dlen, ksem, vsem, nsem):
    st = lax.axis_index('stage')
    new = (kn_s, vn_s, kp_s, vp_s)

    @pl.when(st < 2)
    def _():
        cs = load_new((kdn, vdn, kpn, vpn, dlen_h), new + (dlen,), nsem)
        for c in cs:
            c.wait()
        po = [pltpu.make_async_copy(kp_s, kpo, nsem.at[2]), pltpu.make_async_copy(vp_s, vpo, nsem.at[3])]
        for o in po:
            o.start()
        lane = lane_iota((HD, LN))

        def edit(m, scr, w):
            for i in range(DR):
                pos = dlen[m, i]
                sl = tile_start(pos)
                for g in range(NKV):
                    col = new[w][g * HD:(g + 1) * HD, m * DR + i:m * DR + i + 1]
                    scr[m, i, g, :, sl] = jnp.where(lane == pos % LN, col, scr[m, i, g, :, sl].astype(F32)).astype(BF16)

        copy_all(kd, vd, ko, vo, ks, vs, ksem, vsem, edit)
        for o in po:
            o.wait()

    @pl.when(st == 2)
    def _():
        cs = load_new((kdn, vdn, kpn, vpn, dlen_h), new + (dlen,), nsem)
        update_tiles(dlen, bk, bv, ko, vo, kpo, vpo, kt, vt, new, cs, ksem, vsem, nsem)


def post_kernel(dlen_h, kdn, vdn, kpn, vpn, lg, bk, bv, bkp, bvp, ko, vo, kpo, vpo, kt, vt, kn_s, vn_s, kp_s, vp_s, dlen, ksem, vsem, nsem):
    st = lax.axis_index('stage')

    @pl.when(st == LAST)
    def _():
        new = (kn_s, vn_s, kp_s, vp_s)
        cs = load_new((kdn, vdn, kpn, vpn, dlen_h), new + (dlen,), nsem)
        update_tiles(dlen, bk, bv, ko, vo, kpo, vpo, kt, vt, new, cs, ksem, vsem, nsem)


ANY = pl.BlockSpec(memory_space=pltpu.HBM)


def solution(mesh):
    part = P('replica')
    layer = P('stage')
    cache = P('stage', 'replica')
    in_specs = (part,) * 4 + (layer,) * 9 + (P(), P()) + (cache,) * 4
    out_specs = (part,) + (cache,) * 4
    inv_freq = np.float32(ROPE_BASE) ** (-np.arange(HALF, dtype=np.float32) * np.float32(2.0 / HD))
    ifr_c = np.broadcast_to(inv_freq[:, None], (HALF, NP)).astype(np.float32)

    def device_fn(x_dec, x_pre, dec_len, pre_len, g_attn, w_q, w_k, w_v, w_o, g_mlp, w_gate, w_up, w_down, g_final, w_head, k_dec, v_dec, k_pre, v_pre):
        kd = jnp.transpose(k_dec[0], (0, 1, 3, 4, 2))
        vd = jnp.transpose(v_dec[0], (0, 1, 3, 4, 2))
        kp = jnp.transpose(k_pre[0], (1, 2, 0))
        vp = jnp.transpose(v_pre[0], (1, 2, 0))
        args = (x_dec.reshape(ND, HID), x_pre.reshape(NP, HID), dec_len, pre_len, g_attn, w_q[0], w_k[0].T, w_v[0].T, w_o[0], g_mlp,
                w_gate[0], w_up[0], w_down[0].T, g_final, kd, vd, kp, vp, jnp.asarray(ifr_c))
        vm = lambda shape, dt: pltpu.VMEM(shape, dt)
        scratch = [
            vm((ND, HID), BF16), vm((NP, HID), BF16), pltpu.SMEM((NM, DR), jnp.int32), pltpu.SMEM((1,), jnp.int32), vm((1, HID), BF16),
            vm((HID, HID), BF16), vm((KVW, HID), BF16), vm((KVW, HID), BF16), vm((HID, HID), BF16), vm((1, HID), BF16),
            vm((HID, FFN), BF16), vm((HID, FFN), BF16), vm((HID, FFN), BF16), vm((HID,), BF16),
            vm(kd.shape, BF16), vm(vd.shape, BF16), vm(kp.shape, BF16), vm(vp.shape, BF16), vm((HALF, NP), F32),
            vm((HID, HID), BF16), vm((HALF, LN), F32), vm((HALF, LN), F32), vm((HALF, NP), F32), vm((HALF, NP), F32),
            vm((HALF, LN), F32), vm((HALF, LN), F32),
            vm(((ND + 8) * 8, LN), F32), vm(((ND + 8) * 8, LN), F32), vm((24, LN), F32), vm((ND + 8, KVW), F32),
            vm(((ND + 8) * 8, LN), F32), vm(((ND + 8) * 8, LN), F32),
            vm((KVW, LN), F32), vm((KVW, LN), F32), vm((2 * DR * 24, CL), F32), vm((2, CL, NP), F32), vm((2, CL, NP), BF16), vm((CL, NP), F32),
            vm((HID, NP), F32), vm((NP, FFN), BF16), vm((8, HID), F32),
            vm((ND, HID), BF16), vm((NP, HID), BF16), vm((ND + 8, HID), BF16),
            pltpu.SemaphoreType.DMA((17,)), pltpu.SemaphoreType.DMA((NM,)), pltpu.SemaphoreType.DMA((NM,)), pltpu.SemaphoreType.DMA((5,)),
            pltpu.SemaphoreType.DMA, pltpu.SemaphoreType.DMA, pltpu.SemaphoreType.DMA, pltpu.SemaphoreType.DMA,
        ]
        sds = jax.ShapeDtypeStruct
        big = pltpu.CompilerParams(vmem_limit_bytes=62 * 1024 * 1024)
        cshape = sds(kd.shape, BF16)
        pshape = sds(kp.shape, BF16)
        nsems = [pltpu.SemaphoreType.DMA((NM,)), pltpu.SemaphoreType.DMA((NM,))]
        tile = vm((NM, DR, NKV, HD, LN), BF16)
        news = [vm((KVW, LN), F32), vm((KVW, LN), F32), vm(kp.shape, BF16), vm(vp.shape, BF16), pltpu.SMEM((NM, DR), jnp.int32)]
        vmem = pl.BlockSpec(memory_space=pltpu.VMEM)
        tshape = sds((8, LN), F32)
        bk, bv, tok = pl.pallas_call(
            pre_kernel, out_shape=(cshape, cshape, tshape), in_specs=[ANY, ANY], out_specs=(ANY, ANY, ANY),
            scratch_shapes=[vm(kd.shape, BF16), vm(vd.shape, BF16)] + nsems, name='pre', compiler_params=big)(kd, vd)
        args = args + (tok,)
        kdn, vdn, kpn, vpn, fh = pl.pallas_call(
            pipe_kernel,
            out_shape=(sds((KVW, LN), F32), sds((KVW, LN), F32), pshape, pshape, sds((ND + 8, HID), BF16)),
            in_specs=[ANY] * len(args),
            out_specs=(ANY,) * 5,
            scratch_shapes=scratch,
            name='pipe',
            compiler_params=pltpu.CompilerParams(collective_id=0, has_side_effects=True, vmem_limit_bytes=62 * 1024 * 1024),
        )(*args)
        bk, bv, bkp, bvp, tok2 = pl.pallas_call(
            mid_kernel, out_shape=(cshape, cshape, pshape, pshape, tshape), in_specs=[ANY] * 9, out_specs=(ANY,) * 5,
            input_output_aliases={3: 0, 4: 1},
            scratch_shapes=[vm(kd.shape, BF16), vm(vd.shape, BF16), tile, tile] + news + nsems + [pltpu.SemaphoreType.DMA((5,))],
            name='mid', compiler_params=big)(dec_len, kd, vd, bk, bv, kdn, vdn, kpn, vpn)
        logits = pl.pallas_call(
            head_kernel, out_shape=sds((DR + 1, NM, VOC), F32), in_specs=[ANY] * 3, out_specs=vmem,
            scratch_shapes=[vm((ND + 8, HID), BF16), vm((ND + 8, HID), BF16), vm((HID, VOC), BF16),
                            pltpu.SemaphoreType.DMA((2,)), pltpu.SemaphoreType.DMA((LAST,)), pltpu.SemaphoreType.DMA],
            name='head', compiler_params=pltpu.CompilerParams(collective_id=1, has_side_effects=True))(fh, w_head, tok2)
        ko, vo, kpo, vpo = pl.pallas_call(
            post_kernel, out_shape=(cshape, cshape, pshape, pshape), in_specs=[ANY] * 10, out_specs=(ANY,) * 4,
            input_output_aliases={6: 0, 7: 1, 8: 2, 9: 3},
            scratch_shapes=[tile, tile] + news + nsems + [pltpu.SemaphoreType.DMA((5,))],
            name='post', compiler_params=big)(dec_len, kdn, vdn, kpn, vpn, logits, bk, bv, bkp, bvp)
        back = lambda a: jnp.transpose(a, (0, 1, 4, 2, 3))[None]
        backp = lambda a: jnp.transpose(a, (2, 0, 1))[None]
        return jnp.transpose(logits, (1, 0, 2)), back(ko), back(vo), backp(kpo), backp(vpo)

    return jax.shard_map(device_fn, mesh=mesh, in_specs=in_specs, out_specs=out_specs, check_vma=False)
```

```python
import functools

import jax
import jax.numpy as jnp
import numpy as np
from jax import lax
from jax.experimental import pallas as pl
from jax.experimental.pallas import tpu as pltpu
from jax.sharding import PartitionSpec as P

F32 = jnp.float32
BF16 = jnp.bfloat16
MESH = pl.DeviceIdType.MESH
NORM_EPS = 1e-6
ROPE_BASE = 10000.0
NEG = -1e30

HID = 576
NQ = 9
NKV = 3
GRP = 3
HD = 64
HALF = 32
KVW = NKV * HD
FFN = 1536
NM = 4
DR = 8
SEG = 64
CL = 512
VOC = 1024
ND = NM * DR
NP = NM * SEG
LAST = 3
LN = 128
CP = 128
CD = 16
CR = CP + CD
ES = CD + 8
FR = ND + 8


def nt(a, b):
    return lax.dot_general(a, b, (((1,), (1,)), ((), ())), preferred_element_type=F32)


def nn(a, b):
    return jnp.dot(a, b, preferred_element_type=F32)


def rms(x, g):
    inv = lax.rsqrt(jnp.mean(x * x, axis=-1, keepdims=True) + NORM_EPS)
    return (x * inv * g).astype(BF16)


def rope_t(m, cos, sin):
    parts = []
    for j in range(m.shape[0] // HD):
        a = m[j * HD:j * HD + HALF]
        b = m[j * HD + HALF:(j + 1) * HD]
        parts += [a * cos - b * sin, b * cos + a * sin]
    return jnp.concatenate(parts, axis=0)


def lane_iota(shape):
    return lax.broadcasted_iota(jnp.int32, shape, len(shape) - 1)


def pipe_kernel(xd, xp, dlen, plen, ga, wq, wk, wv, wo, gm, wg, wu, wd, gf, kd, vd, kp, vp, ifr, tok,
                kdn, vdn, kpn, vpn, fh_o,
                xc_s, dl_s, pl_s, ga_s, wq_s, w3_s, wo_s, gm_s, wg_s, wu_s, wd_s, gf_s,
                kd_s, vd_s, kp_s, vp_s, ifr_s,
                cos_s, sin_s, qt_s, qa_s, qb_s, self_s, vn_s, oa_s, ob_s,
                kdn_s, vdn_s, sc_s, ps_s, pb_s, bias_s, ot_s, act_s, so_s, fh_s,
                in_sem, kd_sem, vd_sem, out_sem, ssem, rsem):
    st = lax.axis_index('stage')
    order = [(dlen, dl_s), (plen, pl_s), (ga, ga_s), (ifr, ifr_s), (wq, wq_s), (wk, w3_s.at[HID:HID + KVW]), (wv, w3_s.at[HID + KVW:]),
             (kp, kp_s), (vp, vp_s), (wo, wo_s), (gm, gm_s), (wg, wg_s), (wu, wu_s), (wd, wd_s), (gf, gf_s),
             (xp.at[0:CP], xc_s.at[0, 0:CP]), (xd.at[0:CD], xc_s.at[0, CP:CR]), (xp.at[CP:2 * CP], xc_s.at[1, 0:CP]), (xd.at[CD:2 * CD], xc_s.at[1, CP:CR])]
    names = ['dl', 'pl', 'ga', 'ifr', 'wq', 'wk', 'wv', 'kp', 'vp', 'wo', 'gm', 'wg', 'wu', 'wd', 'gf', 'p0', 'd0', 'p1', 'd1']
    cps = {n: pltpu.make_async_copy(a, b, in_sem.at[i]) for i, (n, (a, b)) in enumerate(zip(names, order))}
    kcp = [pltpu.make_async_copy(kd.at[m], kd_s.at[m], kd_sem.at[m]) for m in range(NM)]
    vcp = [pltpu.make_async_copy(vd.at[m], vd_s.at[m], vd_sem.at[m]) for m in range(NM)]

    def start(*ns):
        for n in ns:
            cps[n].start()

    def wait(*ns):
        for n in ns:
            cps[n].wait()

    start('dl', 'pl', 'ifr', 'ga', 'wq', 'wk', 'wv')

    @pl.when(st == 0)
    def _():
        start('p0', 'd0')

    bar = pltpu.get_barrier_semaphore()

    @pl.when(st > 0)
    def _():
        pl.semaphore_signal(bar, inc=1, device_id={'stage': jnp.maximum(st - 1, 0)}, device_id_type=MESH)

    @pl.when(st < LAST)
    def _():
        pl.semaphore_signal(bar, inc=1, device_id={'stage': jnp.minimum(st + 1, LAST)}, device_id_type=MESH)

    wait('dl', 'pl', 'ifr')
    p0 = pl_s[0]
    li = lane_iota((1, 2 * LN))
    fr = ifr_s[...]
    for c in range(2):
        pos = p0 + (c * CP) + li
        for k in range(CD):
            pos = jnp.where(li == LN + k, dl_s[2 * c + k // DR, k % DR], pos)
        for k in range(2):
            pos = jnp.where(li == LN + CD + k, p0 + (c * CP + k * SEG + SEG - 1), pos)
        ang = fr * pos.astype(F32)
        cos_s[c] = jnp.cos(ang)
        sin_s[c] = jnp.sin(ang)
    qa_s[...] = jnp.zeros_like(qa_s)
    qb_s[...] = jnp.zeros_like(qb_s)
    ob_s[...] = jnp.zeros_like(ob_s)
    for k in range(2):
        pb_s[k] = jnp.zeros((CL, 2 * LN), BF16)

    start('kp', 'vp')
    for m in range(2):
        kcp[m].start()
        vcp[m].start()
    start('wo', 'gm')
    wait('ga', 'wq')
    w3_s[:HID, :] = wq_s[...].astype(F32).T.astype(BF16)
    wait('wk', 'wv')
    gat = ga_s[...].astype(F32)

    lgrp = lane_iota((8, KVW)) // HD

    def dec_scores(e, kt, slot):
        qb = jnp.concatenate([qa_s[e * 8:e * 8 + 8, :], qb_s[e * 8:e * 8 + 8, :HD]], axis=1)
        lhs = jnp.concatenate([jnp.where(lgrp == g, qb, 0.0) for g in range(NKV)], axis=0).astype(BF16)
        sc_s[slot * 24:slot * 24 + 24, :] = nn(lhs, kt)

    def dec_mix(c, k, vt, pos, slot):
        e = c * ES + k
        selfcol = jnp.sum(jnp.where(lane_iota((24, LN)) == k, self_s[c], 0.0), axis=-1, keepdims=True)
        s = jnp.where(lane_iota((24, CL)) < pos, sc_s[slot * 24:slot * 24 + 24, :], NEG)
        mx = jnp.maximum(jnp.max(s, axis=-1, keepdims=True), selfcol)
        p = jnp.exp(s - mx)
        ps = jnp.exp(selfcol - mx)
        rl = 1.0 / (jnp.sum(p, axis=-1, keepdims=True) + ps)
        o = nt((p * rl).astype(BF16), vt)
        o = o + (ps * rl).astype(BF16).astype(F32) * vn_s[e:e + 1, :]
        acc = jnp.where(lgrp == 0, o[0:8], 0.0)
        for g in range(1, NKV):
            acc = jnp.where(lgrp == g, o[8 * g:8 * g + 8], acc)
        oa_s[e * 8:e * 8 + 8, :] = acc[:, :LN]
        ob_s[e * 8:e * 8 + 8, :HD] = acc[:, LN:]

    def dec_out(e, n):
        return jnp.concatenate([x for r in range(GRP) for x in
                                (oa_s[pl.ds(e * 8 + r, n, stride=8), :], ob_s[pl.ds(e * 8 + r, n, stride=8), :][:, :HD])], axis=1)

    def wo_perm():
        return jnp.concatenate([wo_s[(g * GRP + r) * HD:(g * GRP + r + 1) * HD, :] for r in range(GRP) for g in range(NKV)], axis=0)

    def mlp(x, rows):
        h2 = rms(x, gm_s[...].astype(F32))
        step = 512
        for c in range(FFN // step):
            gt = nn(h2, wg_s[:, c * step:(c + 1) * step])
            up = nn(h2, wu_s[:, c * step:(c + 1) * step])
            act_s[:rows, c * step:(c + 1) * step] = (gt * (1.0 / (1.0 + jnp.exp(-gt))) * up).astype(BF16)
        return (x + nt(act_s[:rows, :], wd_s[...])).astype(BF16)

    def round32(x):
        return x.astype(BF16).astype(F32)

    def hop(c):
        return pltpu.make_async_remote_copy(so_s.at[c], xc_s.at[c], ssem.at[c], rsem.at[c],
                                            device_id={'stage': jnp.minimum(st + 1, LAST)}, device_id_type=MESH)

    def last_rows(x):
        return [x[k * SEG + SEG - 1:k * SEG + SEG] for k in range(2)]

    for c in range(2):
        lim = CL - CP if c == 0 else CL

        @pl.when(st == 0)
        def _():
            wait('p%d' % c, 'd%d' % c)

        @pl.when(st > 0)
        def _():
            hop(c).wait_recv()

        x = xc_s[c].astype(F32)
        h = x * lax.rsqrt(jnp.mean(x * x, axis=-1, keepdims=True) + NORM_EPS) * gat
        h = jnp.concatenate([h] + last_rows(h) + [jnp.zeros((2 * LN - CR - 2, HID), F32)], axis=0).astype(BF16)
        qkv = nt(w3_s[...], h)
        cos, sin = cos_s[c], sin_s[c]
        qt = round32(rope_t(qkv[:HID], cos, sin)) * (HD ** -0.5)
        kt = round32(rope_t(qkv[HID:HID + KVW], cos, sin))
        vt = round32(qkv[HID + KVW:])
        qt_s[...] = qt[:, :LN].astype(BF16)
        qe, ke, ve = qt[:, LN:], kt[:, LN:], vt[:, LN:]
        row = lax.broadcasted_iota(jnp.int32, (24, LN), 0)
        sf = jnp.zeros((24, LN), F32)
        for g in range(NKV):
            for r in range(GRP):
                j = g * GRP + r
                v = jnp.sum(qe[j * HD:(j + 1) * HD] * ke[g * HD:(g + 1) * HD], axis=0, keepdims=True)
                sf = jnp.where(row == 8 * g + r, v, sf)
        self_s[c] = sf
        n = CD + 8
        e0 = c * ES
        pad = jnp.zeros((HD, LN), F32)
        for r in range(GRP):
            qr = [qe[(g * GRP + r) * HD:(g * GRP + r + 1) * HD] for g in range(NKV)]
            qa_s[pl.ds(e0 * 8 + r, n, stride=8), :] = jnp.concatenate(qr[:2], axis=0).T[:n]
            qb_s[pl.ds(e0 * 8 + r, n, stride=8), :] = jnp.concatenate([qr[2], pad], axis=0).T[:n]
        vn_s[e0:e0 + n, :LN] = ve[:LN].T[:n]
        vn_s[e0:e0 + n, LN:] = jnp.concatenate([ve[LN:], pad], axis=0).T[:n, :HD]
        kdn_s[c] = ke
        vdn_s[c] = ve
        pltpu.make_async_copy(kdn_s.at[c], kdn.at[c], out_sem.at[c]).start()
        pltpu.make_async_copy(vdn_s.at[c], vdn.at[c], out_sem.at[2 + c]).start()

        if c == 0:
            wait('kp', 'vp')
            start('wg', 'wu', 'wd', 'gf')
        off = p0 + c * CP
        place = jnp.where(lax.broadcasted_iota(jnp.int32, (CP, CL), 0) + off == lane_iota((CP, CL)), 1.0, 0.0).astype(BF16)
        lp = lane_iota((KVW, CL)) - off
        fresh = (lp >= 0) & (lp < CP)
        kpu = jnp.where(fresh, nn(kt[:, :LN].astype(BF16), place), kp_s[...].reshape(KVW, CL).astype(F32))
        vpu = jnp.where(fresh, nn(vt[:, :LN].astype(BF16), place), vp_s[...].reshape(KVW, CL).astype(F32))
        kp_s[...] = kpu.astype(BF16).reshape(NKV, HD, CL)
        vp_s[...] = vpu.astype(BF16).reshape(NKV, HD, CL)
        if c == 1:
            pltpu.make_async_copy(kp_s, kpn, out_sem.at[4]).start()
            pltpu.make_async_copy(vp_s, vpn, out_sem.at[5]).start()

        for m in (2 * c, 2 * c + 1):
            kcp[m].wait()
            vcp[m].wait()
        if c == 0:
            @pl.when(st == 0)
            def _():
                start('p1', 'd1')
            for m in (2, 3):
                kcp[m].start()
                vcp[m].start()
            wait('wo', 'gm')

        def dqk(i):
            for k in range(DR):
                dec_scores(c * ES + i * DR + k, kd_s[2 * c + i, k].reshape(KVW, CL), i * DR + k)

        def dmix(i):
            for k in range(DR):
                dec_mix(c, i * DR + k, vd_s[2 * c + i, k].reshape(KVW, CL), dl_s[2 * c + i, k], i * DR + k)

        @pl.when(st < LAST)
        def _():
            kfull = kpu[:, :lim].T.astype(BF16)
            bias_s[:lim, :] = jnp.where(lax.broadcasted_iota(jnp.int32, (lim, LN), 0) <= lane_iota((lim, LN)) + off, 0.0, NEG)

            def heads(t):
                return [j for j in (2 * t, 2 * t + 1) if j < NQ]

            def scores(t):
                cols = []
                for j in heads(t):
                    g = j // GRP
                    parts = [jnp.zeros((g * HD, LN), BF16)] * (g > 0) + [qt_s[j * HD:(j + 1) * HD, :]]
                    parts += [jnp.zeros(((NKV - 1 - g) * HD, LN), BF16)] * (g < NKV - 1)
                    cols.append(jnp.concatenate(parts, axis=0))
                w = len(cols) * LN
                ps_s[t % 2, :lim, :w] = nn(kfull, jnp.concatenate(cols, axis=1))

            def fold(v, op):
                return op(v.reshape(v.shape[0] // 8, 8, v.shape[1]), axis=0)

            def mix(t):
                sl = t % 2
                ck = 64
                hs = heads(t)
                for i, j in enumerate(hs):
                    ln = slice(i * LN, (i + 1) * LN)
                    mx = jnp.full((8, LN), NEG, F32)
                    for q in range(0, lim, ck):
                        mx = jnp.maximum(mx, fold(ps_s[sl, q:q + ck, ln] + bias_s[q:q + ck, :], jnp.max))
                    mx = jnp.max(mx, axis=0, keepdims=True)
                    sm = jnp.zeros((8, LN), F32)
                    for q in range(0, lim, ck):
                        p = jnp.exp(ps_s[sl, q:q + ck, ln] + bias_s[q:q + ck, :] - mx)
                        ps_s[sl, q:q + ck, ln] = p
                        sm = sm + fold(p, jnp.sum)
                    rl = 1.0 / jnp.sum(sm, axis=0, keepdims=True)
                    for q in range(0, lim, ck):
                        pb_s[sl, q:q + ck, ln] = (ps_s[sl, q:q + ck, ln] * rl).astype(BF16)
                g0, g1 = hs[0] // GRP, hs[-1] // GRP
                o = nn(vp_s[...].reshape(KVW, CL)[g0 * HD:(g1 + 1) * HD, :lim], pb_s[sl, :lim, :len(hs) * LN])
                for i, j in enumerate(hs):
                    g, r = j // GRP, j % GRP
                    d = (r * NKV + g) * HD
                    ot_s[d:d + HD, :] = o[(g - g0) * HD:(g - g0 + 1) * HD, i * LN:(i + 1) * LN]

            scores(0)
            dqk(0)
            scores(1)
            mix(0)
            dmix(0)
            scores(2)
            dqk(1)
            mix(1)
            scores(3)
            mix(2)
            dmix(1)
            scores(4)
            mix(3)
            mix(4)
            a = jnp.concatenate([ot_s[...].T, dec_out(e0, CD)], axis=0).astype(BF16)
            x1 = round32(xc_s[c].astype(F32) + nn(a, wo_perm()))
            if c == 0:
                wait('wg', 'wu', 'wd')
            so_s[c] = mlp(x1, CR)
            if c == 0:
                @pl.when(st == 0)
                def _():
                    pl.semaphore_wait(bar, 1)

                @pl.when(st > 0)
                def _():
                    pl.semaphore_wait(bar, 2)
            hop(c).start()

        @pl.when(st == LAST)
        def _():
            for k in range(2):
                dec_scores(e0 + CD + k, kp_s[...].reshape(KVW, CL), 2 * DR + k)
            dqk(0)
            dqk(1)
            for k in range(2):
                dec_mix(c, CD + k, vp_s[...].reshape(KVW, CL), off + k * SEG + SEG - 1, 2 * DR + k)
            dmix(0)
            dmix(1)
            if c == 0:
                wait('wg', 'wu', 'wd', 'gf')
                pl.semaphore_wait(bar, 1)
            else:
                ls = [dec_out(k * ES + CD, 8)[:2] for k in range(2)]
                a = jnp.concatenate([dec_out(0, CD), dec_out(ES, CD)] + ls + [jnp.zeros((4, HID), F32)], axis=0).astype(BF16)
                xs = [xc_s[k].astype(F32) for k in range(2)]
                xf = jnp.concatenate([xs[0][CP:], xs[1][CP:]] + last_rows(xs[0]) + last_rows(xs[1]) + [jnp.zeros((4, HID), F32)], axis=0)
                x2 = mlp(round32(xf + nn(a, wo_perm())), FR)
                fh = rms(x2.astype(F32), gf_s[...].astype(F32).reshape(1, HID))
                ri = lax.broadcasted_iota(jnp.int32, (FR, FR), 0)
                src = jnp.where(ri < ND, (ri % NM) * DR + ri // NM, ri)
                fh_s[...] = nn(jnp.where(lane_iota((FR, FR)) == src, 1.0, 0.0).astype(BF16), fh).astype(BF16)
                ofh = pltpu.make_async_copy(fh_s, fh_o, out_sem.at[6])
                ofh.start()
                ofh.wait()

    for c in range(2):
        pltpu.make_async_copy(kdn_s.at[c], kdn.at[c], out_sem.at[c]).wait()
        pltpu.make_async_copy(vdn_s.at[c], vdn.at[c], out_sem.at[2 + c]).wait()
    pltpu.make_async_copy(kp_s, kpn, out_sem.at[4]).wait()
    pltpu.make_async_copy(vp_s, vpn, out_sem.at[5]).wait()

    @pl.when(st < LAST)
    def _():
        wait('gf')
        for c in range(2):
            hop(c).wait_send()


def head_kernel(fh, wh, tok, logits, fh_s, fr_s, wh_s, lsem, ssem, rsem):
    st = lax.axis_index('stage')
    lfh = pltpu.make_async_copy(fh, fh_s, lsem.at[0])
    lwh = pltpu.make_async_copy(wh, wh_s, lsem.at[1])

    @pl.when(st == LAST)
    def _():
        lfh.start()

    lwh.start()
    bar = pltpu.get_barrier_semaphore()

    def send(k):
        return pltpu.make_async_remote_copy(fh_s, fr_s, ssem.at[k], rsem, device_id={'stage': k}, device_id_type=MESH)

    def head(ref):
        lwh.wait()
        lg = nn(ref[...], wh_s[...])
        for i in range(DR + 1):
            logits[i] = lg[i * NM:(i + 1) * NM]

    @pl.when(st < LAST)
    def _():
        pl.semaphore_signal(bar, inc=1, device_id={'stage': LAST}, device_id_type=MESH)

    @pl.when(st == LAST)
    def _():
        for k in range(LAST):
            pl.semaphore_signal(bar, inc=1, device_id={'stage': k}, device_id_type=MESH)
        pl.semaphore_wait(bar, LAST)
        lfh.wait()
        for k in range(LAST):
            send(k).start()
        head(fh_s)
        for k in range(LAST):
            send(k).wait_send()

    @pl.when(st < LAST)
    def _():
        pl.semaphore_wait(bar, 1)
        send(0).wait_recv()
        head(fr_s)


def tile_start(pos):
    return pl.ds(pl.multiple_of((pos // LN) * LN, LN), LN)


def copy_all(kd, vd, ko, vo, ks, vs, ksem, vsem, edit):
    ins = [(pltpu.make_async_copy(kd.at[m], ks.at[m], ksem.at[m]), pltpu.make_async_copy(vd.at[m], vs.at[m], vsem.at[m])) for m in range(NM)]
    for a, b in ins:
        a.start()
        b.start()
    outs = []
    for m in range(NM):
        for c, scr, out, sem, w in ((ins[m][0], ks, ko, ksem, 0), (ins[m][1], vs, vo, vsem, 1)):
            c.wait()
            if edit is not None:
                edit(m, scr, w)
            o = pltpu.make_async_copy(scr.at[m], out.at[m], sem.at[m])
            o.start()
            outs.append(o)
    for o in outs:
        o.wait()


def pre_kernel(kd, vd, ko, vo, tok, ks, vs, ksem, vsem):
    st = lax.axis_index('stage')

    @pl.when(st >= 2)
    def _():
        copy_all(kd, vd, ko, vo, ks, vs, ksem, vsem, None)


def load_new(srcs, dsts, sem):
    cs = [pltpu.make_async_copy(a, b, sem.at[i]) for i, (a, b) in enumerate(zip(srcs, dsts))]
    for c in cs:
        c.start()
    return cs


def update_tiles(dlen, bk, bv, ko, vo, kpo, vpo, kt, vt, new, cs, ksem, vsem, nsem):
    lane = lane_iota((HD, LN))

    def cp(hbm, scr, sem, m, i, out):
        h = hbm.at[m, i, :, :, tile_start(dlen[m, i])]
        v = scr.at[m, i]
        return pltpu.make_async_copy(v, h, sem.at[m]) if out else pltpu.make_async_copy(h, v, sem.at[m])

    cs[4].wait()
    for m in range(NM):
        for i in range(DR):
            cp(bk, kt, ksem, m, i, False).start()
            cp(bv, vt, vsem, m, i, False).start()
    for c in cs[:4]:
        c.wait()
    po = [pltpu.make_async_copy(new[2], kpo, nsem.at[2]), pltpu.make_async_copy(new[3], vpo, nsem.at[3])]
    for o in po:
        o.start()
    for m in range(NM):
        for hbm, scr, sem, nw in ((ko, kt, ksem, new[0]), (vo, vt, vsem, new[1])):
            for i in range(DR):
                cp(hbm, scr, sem, m, i, False).wait()
            for i in range(DR):
                pos = dlen[m, i]
                for g in range(NKV):
                    col = nw[m // 2, g * HD:(g + 1) * HD, m % 2 * DR + i:m % 2 * DR + i + 1]
                    scr[m, i, g] = jnp.where(lane == pos % LN, col, scr[m, i, g].astype(F32)).astype(BF16)
            for i in range(DR):
                cp(hbm, scr, sem, m, i, True).start()
    for m in range(NM):
        for i in range(DR):
            cp(ko, kt, ksem, m, i, True).wait()
            cp(vo, vt, vsem, m, i, True).wait()
    for o in po:
        o.wait()


def mid_kernel(dlen_h, kd, vd, bk, bv, kdn, vdn, kpn, vpn, ko, vo, kpo, vpo, tok, ks, vs, kt, vt, kn_s, vn_s, kp_s, vp_s, dlen, ksem, vsem, nsem):
    st = lax.axis_index('stage')
    new = (kn_s, vn_s, kp_s, vp_s)

    @pl.when(st < 2)
    def _():
        cs = load_new((kdn, vdn, kpn, vpn, dlen_h), new + (dlen,), nsem)
        for c in cs:
            c.wait()
        po = [pltpu.make_async_copy(kp_s, kpo, nsem.at[2]), pltpu.make_async_copy(vp_s, vpo, nsem.at[3])]
        for o in po:
            o.start()
        lane = lane_iota((HD, LN))

        def edit(m, scr, w):
            for i in range(DR):
                pos = dlen[m, i]
                sl = tile_start(pos)
                for g in range(NKV):
                    col = new[w][m // 2, g * HD:(g + 1) * HD, m % 2 * DR + i:m % 2 * DR + i + 1]
                    scr[m, i, g, :, sl] = jnp.where(lane == pos % LN, col, scr[m, i, g, :, sl].astype(F32)).astype(BF16)

        copy_all(kd, vd, ko, vo, ks, vs, ksem, vsem, edit)
        for o in po:
            o.wait()

    @pl.when(st == 2)
    def _():
        cs = load_new((kdn, vdn, kpn, vpn, dlen_h), new + (dlen,), nsem)
        update_tiles(dlen, bk, bv, ko, vo, kpo, vpo, kt, vt, new, cs, ksem, vsem, nsem)


def post_kernel(dlen_h, kdn, vdn, kpn, vpn, lg, bk, bv, bkp, bvp, ko, vo, kpo, vpo, kt, vt, kn_s, vn_s, kp_s, vp_s, dlen, ksem, vsem, nsem):
    st = lax.axis_index('stage')

    @pl.when(st == LAST)
    def _():
        new = (kn_s, vn_s, kp_s, vp_s)
        cs = load_new((kdn, vdn, kpn, vpn, dlen_h), new + (dlen,), nsem)
        update_tiles(dlen, bk, bv, ko, vo, kpo, vpo, kt, vt, new, cs, ksem, vsem, nsem)


ANY = pl.BlockSpec(memory_space=pltpu.HBM)


def solution(mesh):
    part = P('replica')
    layer = P('stage')
    cache = P('stage', 'replica')
    in_specs = (part,) * 4 + (layer,) * 9 + (P(), P()) + (cache,) * 4
    out_specs = (part,) + (cache,) * 4
    inv_freq = np.float32(ROPE_BASE) ** (-np.arange(HALF, dtype=np.float32) * np.float32(2.0 / HD))
    ifr_c = np.broadcast_to(inv_freq[:, None], (HALF, NP)).astype(np.float32)

    def device_fn(x_dec, x_pre, dec_len, pre_len, g_attn, w_q, w_k, w_v, w_o, g_mlp, w_gate, w_up, w_down, g_final, w_head, k_dec, v_dec, k_pre, v_pre):
        kd = jnp.transpose(k_dec[0], (0, 1, 3, 4, 2))
        vd = jnp.transpose(v_dec[0], (0, 1, 3, 4, 2))
        kp = jnp.transpose(k_pre[0], (1, 2, 0))
        vp = jnp.transpose(v_pre[0], (1, 2, 0))
        args = (x_dec.reshape(ND, HID), x_pre.reshape(NP, HID), dec_len, pre_len, g_attn, w_q[0], w_k[0].T, w_v[0].T, w_o[0], g_mlp,
                w_gate[0], w_up[0], w_down[0].T, g_final, kd, vd, kp, vp, jnp.asarray(ifr_c))
        vm = lambda shape, dt: pltpu.VMEM(shape, dt)
        scratch = [
            vm((2, CR, HID), BF16), pltpu.SMEM((NM, DR), jnp.int32), pltpu.SMEM((1,), jnp.int32), vm((1, HID), BF16),
            vm((HID, HID), BF16), vm((HID + 2 * KVW, HID), BF16), vm((HID, HID), BF16), vm((1, HID), BF16),
            vm((HID, FFN), BF16), vm((HID, FFN), BF16), vm((HID, FFN), BF16), vm((HID,), BF16),
            vm(kd.shape, BF16), vm(vd.shape, BF16), vm(kp.shape, BF16), vm(vp.shape, BF16), vm((HALF, 2 * LN), F32),
            vm((2, HALF, 2 * LN), F32), vm((2, HALF, 2 * LN), F32), vm((HID, LN), BF16),
            vm((2 * ES * 8, LN), F32), vm((2 * ES * 8, LN), F32), vm((2, 24, LN), F32), vm((2 * ES, KVW), F32),
            vm((2 * ES * 8, LN), F32), vm((2 * ES * 8, LN), F32),
            vm((2, KVW, LN), F32), vm((2, KVW, LN), F32), vm(((2 * DR + 2) * 24, CL), F32), vm((2, CL, 2 * LN), F32), vm((2, CL, 2 * LN), BF16),
            vm((CL, LN), F32), vm((HID, LN), F32), vm((CR, FFN), BF16), vm((2, CR, HID), BF16), vm((FR, HID), BF16),
            pltpu.SemaphoreType.DMA((19,)), pltpu.SemaphoreType.DMA((NM,)), pltpu.SemaphoreType.DMA((NM,)), pltpu.SemaphoreType.DMA((7,)),
            pltpu.SemaphoreType.DMA((2,)), pltpu.SemaphoreType.DMA((2,)),
        ]
        sds = jax.ShapeDtypeStruct
        big = pltpu.CompilerParams(vmem_limit_bytes=62 * 1024 * 1024)
        cshape = sds(kd.shape, BF16)
        pshape = sds(kp.shape, BF16)
        nsems = [pltpu.SemaphoreType.DMA((NM,)), pltpu.SemaphoreType.DMA((NM,))]
        tile = vm((NM, DR, NKV, HD, LN), BF16)
        news = [vm((2, KVW, LN), F32), vm((2, KVW, LN), F32), vm(kp.shape, BF16), vm(vp.shape, BF16), pltpu.SMEM((NM, DR), jnp.int32)]
        vmem = pl.BlockSpec(memory_space=pltpu.VMEM)
        tshape = sds((8, LN), F32)
        bk, bv, tok = pl.pallas_call(
            pre_kernel, out_shape=(cshape, cshape, tshape), in_specs=[ANY, ANY], out_specs=(ANY, ANY, ANY),
            scratch_shapes=[vm(kd.shape, BF16), vm(vd.shape, BF16)] + nsems, name='pre', compiler_params=big)(kd, vd)
        args = args + (tok,)
        kdn, vdn, kpn, vpn, fh = pl.pallas_call(
            pipe_kernel,
            out_shape=(sds((2, KVW, LN), F32), sds((2, KVW, LN), F32), pshape, pshape, sds((ND + 8, HID), BF16)),
            in_specs=[ANY] * len(args),
            out_specs=(ANY,) * 5,
            scratch_shapes=scratch,
            name='pipe',
            compiler_params=pltpu.CompilerParams(collective_id=0, has_side_effects=True, vmem_limit_bytes=62 * 1024 * 1024),
        )(*args)
        bk, bv, bkp, bvp, tok2 = pl.pallas_call(
            mid_kernel, out_shape=(cshape, cshape, pshape, pshape, tshape), in_specs=[ANY] * 9, out_specs=(ANY,) * 5,
            input_output_aliases={3: 0, 4: 1},
            scratch_shapes=[vm(kd.shape, BF16), vm(vd.shape, BF16), tile, tile] + news + nsems + [pltpu.SemaphoreType.DMA((5,))],
            name='mid', compiler_params=big)(dec_len, kd, vd, bk, bv, kdn, vdn, kpn, vpn)
        logits = pl.pallas_call(
            head_kernel, out_shape=sds((DR + 1, NM, VOC), F32), in_specs=[ANY] * 3, out_specs=vmem,
            scratch_shapes=[vm((ND + 8, HID), BF16), vm((ND + 8, HID), BF16), vm((HID, VOC), BF16),
                            pltpu.SemaphoreType.DMA((2,)), pltpu.SemaphoreType.DMA((LAST,)), pltpu.SemaphoreType.DMA],
            name='head', compiler_params=pltpu.CompilerParams(collective_id=1, has_side_effects=True))(fh, w_head, tok2)
        ko, vo, kpo, vpo = pl.pallas_call(
            post_kernel, out_shape=(cshape, cshape, pshape, pshape), in_specs=[ANY] * 10, out_specs=(ANY,) * 4,
            input_output_aliases={6: 0, 7: 1, 8: 2, 9: 3},
            scratch_shapes=[tile, tile] + news + nsems + [pltpu.SemaphoreType.DMA((5,))],
            name='post', compiler_params=big)(dec_len, kdn, vdn, kpn, vpn, logits, bk, bv, bkp, bvp)
        back = lambda a: jnp.transpose(a, (0, 1, 4, 2, 3))[None]
        backp = lambda a: jnp.transpose(a, (2, 0, 1))[None]
        return jnp.transpose(logits, (1, 0, 2)), back(ko), back(vo), backp(kpo), backp(vpo)

    return jax.shard_map(device_fn, mesh=mesh, in_specs=in_specs, out_specs=out_specs, check_vma=False)
```

```python
import functools

import jax
import jax.numpy as jnp
import numpy as np
from jax import lax
from jax.experimental import pallas as pl
from jax.experimental.pallas import tpu as pltpu
from jax.sharding import PartitionSpec as P

F32 = jnp.float32
BF16 = jnp.bfloat16
MESH = pl.DeviceIdType.MESH
NORM_EPS = 1e-6
ROPE_BASE = 10000.0
NEG = -1e30

HID = 576
NQ = 9
NKV = 3
GRP = 3
HD = 64
HALF = 32
KVW = NKV * HD
FFN = 1536
NM = 4
DR = 8
SEG = 64
CL = 512
VOC = 1024
ND = NM * DR
NP = NM * SEG
LAST = 3
LN = 128
CP = 128
CD = 16
CR = CP + CD
ES = CD + 8
FR = ND + 8


def nt(a, b):
    return lax.dot_general(a, b, (((1,), (1,)), ((), ())), preferred_element_type=F32)


def nn(a, b):
    return jnp.dot(a, b, preferred_element_type=F32)


def rms(x, g):
    inv = lax.rsqrt(jnp.mean(x * x, axis=-1, keepdims=True) + NORM_EPS)
    return (x * inv * g).astype(BF16)


def rope_t(m, cos, sin):
    parts = []
    for j in range(m.shape[0] // HD):
        a = m[j * HD:j * HD + HALF]
        b = m[j * HD + HALF:(j + 1) * HD]
        parts += [a * cos - b * sin, b * cos + a * sin]
    return jnp.concatenate(parts, axis=0)


def lane_iota(shape):
    return lax.broadcasted_iota(jnp.int32, shape, len(shape) - 1)


def pipe_kernel(xd, xp, dlen, plen, ga, wq, wk, wv, wo, gm, wg, wu, wd, gf, kd, vd, kp, vp, ifr, tok,
                kdn, vdn, kpn, vpn, fh_o,
                xc_s, dl_s, pl_s, ga_s, wq_s, w3_s, wo_s, gm_s, wg_s, wu_s, wd_s, wdt_s, gf_s,
                kd_s, vd_s, kp_s, vp_s, ifr_s,
                cos_s, sin_s, qt_s, qa_s, qb_s, self_s, vn_s, oa_s, ob_s,
                kdn_s, vdn_s, sc_s, ps_s, pb_s, bias_s, ot_s, act_s, so_s, fh_s,
                in_sem, kd_sem, vd_sem, out_sem, ssem, rsem):
    st = lax.axis_index('stage')
    order = [(dlen, dl_s), (plen, pl_s), (ga, ga_s), (ifr, ifr_s), (wq, wq_s), (wk, w3_s.at[HID:HID + KVW]), (wv, w3_s.at[HID + KVW:]),
             (kp, kp_s), (vp, vp_s), (wo, wo_s), (gm, gm_s), (wg, wg_s), (wu, wu_s), (wd, wd_s), (gf, gf_s),
             (xp.at[0:CP], xc_s.at[0, 0:CP]), (xd.at[0:CD], xc_s.at[0, CP:CR]), (xp.at[CP:2 * CP], xc_s.at[1, 0:CP]), (xd.at[CD:2 * CD], xc_s.at[1, CP:CR])]
    names = ['dl', 'pl', 'ga', 'ifr', 'wq', 'wk', 'wv', 'kp', 'vp', 'wo', 'gm', 'wg', 'wu', 'wd', 'gf', 'p0', 'd0', 'p1', 'd1']
    cps = {n: pltpu.make_async_copy(a, b, in_sem.at[i]) for i, (n, (a, b)) in enumerate(zip(names, order))}
    kcp = [pltpu.make_async_copy(kd.at[m], kd_s.at[m], kd_sem.at[m]) for m in range(NM)]
    vcp = [pltpu.make_async_copy(vd.at[m], vd_s.at[m], vd_sem.at[m]) for m in range(NM)]

    def start(*ns):
        for n in ns:
            cps[n].start()

    def wait(*ns):
        for n in ns:
            cps[n].wait()

    start('dl', 'pl', 'ifr', 'ga', 'wq', 'wk', 'wv')

    @pl.when(st == 0)
    def _():
        start('p0', 'd0')

    bar = pltpu.get_barrier_semaphore()

    @pl.when(st > 0)
    def _():
        pl.semaphore_signal(bar, inc=1, device_id={'stage': jnp.maximum(st - 1, 0)}, device_id_type=MESH)

    @pl.when(st < LAST)
    def _():
        pl.semaphore_signal(bar, inc=1, device_id={'stage': jnp.minimum(st + 1, LAST)}, device_id_type=MESH)

    wait('dl', 'pl', 'ifr')
    p0 = pl_s[0]
    li = lane_iota((1, 2 * LN))
    fr = ifr_s[...]
    for c in range(2):
        pos = p0 + (c * CP) + li
        for k in range(CD):
            pos = jnp.where(li == LN + k, dl_s[2 * c + k // DR, k % DR], pos)
        for k in range(2):
            pos = jnp.where(li == LN + CD + k, p0 + (c * CP + k * SEG + SEG - 1), pos)
        ang = fr * pos.astype(F32)
        cos_s[c] = jnp.cos(ang)
        sin_s[c] = jnp.sin(ang)
    qa_s[...] = jnp.zeros_like(qa_s)
    qb_s[...] = jnp.zeros_like(qb_s)
    ob_s[...] = jnp.zeros_like(ob_s)
    for k in range(2):
        pb_s[k] = jnp.zeros((CL, 2 * LN), BF16)

    start('kp', 'vp')
    for m in range(2):
        kcp[m].start()
        vcp[m].start()
    start('wo', 'gm')

    @pl.when(st > 0)
    def _():
        start('wg', 'wu', 'wd', 'gf')

    wait('ga', 'wq')
    w3_s[:HID, :] = wq_s[...].astype(F32).T.astype(BF16)
    wait('wk', 'wv')

    @pl.when(st > 0)
    def _():
        wait('wd')
        for k in range(0, FFN, LN):
            wdt_s[k:k + LN, :] = wd_s[:, k:k + LN].astype(F32).T.astype(BF16)

    gat = ga_s[...].astype(F32)

    lgrp = lane_iota((8, KVW)) // HD

    def dec_scores(e, kt, slot):
        qb = jnp.concatenate([qa_s[e * 8:e * 8 + 8, :], qb_s[e * 8:e * 8 + 8, :HD]], axis=1)
        lhs = jnp.concatenate([jnp.where(lgrp == g, qb, 0.0) for g in range(NKV)], axis=0).astype(BF16)
        sc_s[slot * 24:slot * 24 + 24, :] = nn(lhs, kt)

    def dec_mix(c, k, vt, pos, slot):
        e = c * ES + k
        selfcol = jnp.sum(jnp.where(lane_iota((24, LN)) == k, self_s[c], 0.0), axis=-1, keepdims=True)
        s = jnp.where(lane_iota((24, CL)) < pos, sc_s[slot * 24:slot * 24 + 24, :], NEG)
        mx = jnp.maximum(jnp.max(s, axis=-1, keepdims=True), selfcol)
        p = jnp.exp(s - mx)
        ps = jnp.exp(selfcol - mx)
        rl = 1.0 / (jnp.sum(p, axis=-1, keepdims=True) + ps)
        o = nt((p * rl).astype(BF16), vt)
        o = o + (ps * rl).astype(BF16).astype(F32) * vn_s[e:e + 1, :]
        acc = jnp.where(lgrp == 0, o[0:8], 0.0)
        for g in range(1, NKV):
            acc = jnp.where(lgrp == g, o[8 * g:8 * g + 8], acc)
        oa_s[e * 8:e * 8 + 8, :] = acc[:, :LN]
        ob_s[e * 8:e * 8 + 8, :HD] = acc[:, LN:]

    def dec_out(e, n):
        return jnp.concatenate([x for r in range(GRP) for x in
                                (oa_s[pl.ds(e * 8 + r, n, stride=8), :], ob_s[pl.ds(e * 8 + r, n, stride=8), :][:, :HD])], axis=1)

    def wo_perm():
        return jnp.concatenate([wo_s[(g * GRP + r) * HD:(g * GRP + r + 1) * HD, :] for r in range(GRP) for g in range(NKV)], axis=0)

    def mlp(x, rows, put):
        h2 = rms(x, gm_s[...].astype(F32))
        step = 512
        for c in range(FFN // step):
            gt = nn(h2, wg_s[:, c * step:(c + 1) * step])
            up = nn(h2, wu_s[:, c * step:(c + 1) * step])
            act_s[:rows, c * step:(c + 1) * step] = (gt * (1.0 / (1.0 + jnp.exp(-gt))) * up).astype(BF16)
        put(x, rows)

    def round32(x):
        return x.astype(BF16).astype(F32)

    def hop(c):
        return pltpu.make_async_remote_copy(so_s.at[c], xc_s.at[c], ssem.at[c], rsem.at[c],
                                            device_id={'stage': jnp.minimum(st + 1, LAST)}, device_id_type=MESH)

    def last_rows(x):
        return [x[k * SEG + SEG - 1:k * SEG + SEG] for k in range(2)]

    for c in range(2):
        lim = CL - CP if c == 0 else CL

        @pl.when(st == 0)
        def _():
            wait('p%d' % c, 'd%d' % c)

        @pl.when(st > 0)
        def _():
            hop(c).wait_recv()

        if c == 0:
            wait('kp', 'vp')

            @pl.when(st == 0)
            def _():
                start('wg', 'wu', 'wd', 'gf')
        else:
            for m in (2, 3):
                kcp[m].wait()
                vcp[m].wait()
        off = p0 + c * CP
        e0 = c * ES

        def project():
            x = xc_s[c].astype(F32)
            h = x * lax.rsqrt(jnp.mean(x * x, axis=-1, keepdims=True) + NORM_EPS) * gat
            h = jnp.concatenate([h] + last_rows(h) + [jnp.zeros((2 * LN - CR - 2, HID), F32)], axis=0).astype(BF16)
            half = (HID + 2 * KVW) // 2
            qkv = jnp.concatenate([nt(w3_s[:half, :], h), nt(w3_s[half:, :], h)], axis=0)
            cos, sin = cos_s[c], sin_s[c]
            qt = round32(rope_t(qkv[:HID], cos, sin)) * (HD ** -0.5)
            kt = round32(rope_t(qkv[HID:HID + KVW], cos, sin))
            vt = round32(qkv[HID + KVW:])
            qt_s[...] = qt[:, :LN].astype(BF16)
            qe, ke, ve = qt[:, LN:], kt[:, LN:], vt[:, LN:]
            row = lax.broadcasted_iota(jnp.int32, (24, LN), 0)
            sf = jnp.zeros((24, LN), F32)
            for g in range(NKV):
                for r in range(GRP):
                    j = g * GRP + r
                    v = jnp.sum(qe[j * HD:(j + 1) * HD] * ke[g * HD:(g + 1) * HD], axis=0, keepdims=True)
                    sf = jnp.where(row == 8 * g + r, v, sf)
            self_s[c] = sf
            n = CD + 8
            pad = jnp.zeros((HD, LN), F32)
            for r in range(GRP):
                qr = [qe[(g * GRP + r) * HD:(g * GRP + r + 1) * HD] for g in range(NKV)]
                qa_s[pl.ds(e0 * 8 + r, n, stride=8), :] = jnp.concatenate(qr[:2], axis=0).T[:n]
                qb_s[pl.ds(e0 * 8 + r, n, stride=8), :] = jnp.concatenate([qr[2], pad], axis=0).T[:n]
            vn_s[e0:e0 + n, :LN] = ve[:LN].T[:n]
            vn_s[e0:e0 + n, LN:] = jnp.concatenate([ve[LN:], pad], axis=0).T[:n, :HD]
            kdn_s[c] = ke
            vdn_s[c] = ve
            pltpu.make_async_copy(kdn_s.at[c], kdn.at[c], out_sem.at[c]).start()
            pltpu.make_async_copy(vdn_s.at[c], vdn.at[c], out_sem.at[2 + c]).start()
            return kt, vt

        def put_prompt(kt, vt):
            place = jnp.where(lax.broadcasted_iota(jnp.int32, (CP, CL), 0) + off == lane_iota((CP, CL)), 1.0, 0.0).astype(BF16)
            lp = lane_iota((KVW, CL)) - off
            fresh = (lp >= 0) & (lp < CP)
            kpu = jnp.where(fresh, nn(kt[:, :LN].astype(BF16), place), kp_s[...].reshape(KVW, CL).astype(F32))
            vpu = jnp.where(fresh, nn(vt[:, :LN].astype(BF16), place), vp_s[...].reshape(KVW, CL).astype(F32))
            kp_s[...] = kpu.astype(BF16).reshape(NKV, HD, CL)
            vp_s[...] = vpu.astype(BF16).reshape(NKV, HD, CL)
            if c == 1:
                pltpu.make_async_copy(kp_s, kpn, out_sem.at[4]).start()
                pltpu.make_async_copy(vp_s, vpn, out_sem.at[5]).start()
            return kpu

        def loads():
            if c == 0:
                for m in (0, 1):
                    kcp[m].wait()
                    vcp[m].wait()

                @pl.when(st == 0)
                def _():
                    start('p1', 'd1')
                for m in (2, 3):
                    kcp[m].start()
                    vcp[m].start()
                wait('wo', 'gm')

        def dqk(i):
            for k in range(DR):
                dec_scores(c * ES + i * DR + k, kd_s[2 * c + i, k].reshape(KVW, CL), i * DR + k)

        def dmix(q):
            for k in range(4 * q, 4 * q + 4):
                m, i = 2 * c + k // DR, k % DR
                dec_mix(c, k, vd_s[m, i].reshape(KVW, CL), dl_s[m, i], k)

        @pl.when(st < LAST)
        def _():
            kt, vt = project()
            loads()
            kpu = put_prompt(kt, vt)
            kfull = kpu[:, :lim].T.astype(BF16)
            bias_s[:lim, :] = jnp.where(lax.broadcasted_iota(jnp.int32, (lim, LN), 0) <= lane_iota((lim, LN)) + off, 0.0, NEG)

            def heads(t):
                return [j for j in (2 * t, 2 * t + 1) if j < NQ]

            def scores(t):
                cols = []
                for j in heads(t):
                    g = j // GRP
                    parts = [jnp.zeros((g * HD, LN), BF16)] * (g > 0) + [qt_s[j * HD:(j + 1) * HD, :]]
                    parts += [jnp.zeros(((NKV - 1 - g) * HD, LN), BF16)] * (g < NKV - 1)
                    cols.append(jnp.concatenate(parts, axis=0))
                w = len(cols) * LN
                rhs = jnp.concatenate(cols, axis=1)
                for q in range(0, lim, lim // 2):
                    ps_s[t % 2, q:q + lim // 2, :w] = nn(kfull[q:q + lim // 2], rhs)

            def fold(v, op):
                return op(v.reshape(v.shape[0] // 8, 8, v.shape[1]), axis=0)

            def mix(t):
                sl = t % 2
                ck = 64
                hs = heads(t)
                for i, j in enumerate(hs):
                    ln = slice(i * LN, (i + 1) * LN)
                    mx = jnp.full((8, LN), NEG, F32)
                    for q in range(0, lim, ck):
                        mx = jnp.maximum(mx, fold(ps_s[sl, q:q + ck, ln] + bias_s[q:q + ck, :], jnp.max))
                    mx = jnp.max(mx, axis=0, keepdims=True)
                    sm = jnp.zeros((8, LN), F32)
                    for q in range(0, lim, ck):
                        p = jnp.exp(ps_s[sl, q:q + ck, ln] + bias_s[q:q + ck, :] - mx)
                        ps_s[sl, q:q + ck, ln] = p
                        sm = sm + fold(p, jnp.sum)
                    rl = 1.0 / jnp.sum(sm, axis=0, keepdims=True)
                    for q in range(0, lim, ck):
                        pb_s[sl, q:q + ck, ln] = (ps_s[sl, q:q + ck, ln] * rl).astype(BF16)
                g0, g1 = hs[0] // GRP, hs[-1] // GRP
                o = nn(vp_s[...].reshape(KVW, CL)[g0 * HD:(g1 + 1) * HD, :lim], pb_s[sl, :lim, :len(hs) * LN])
                for i, j in enumerate(hs):
                    g, r = j // GRP, j % GRP
                    d = (r * NKV + g) * HD
                    ot_s[d:d + HD, :] = o[(g - g0) * HD:(g - g0 + 1) * HD, i * LN:(i + 1) * LN]

            dqk(0)
            scores(0)
            scores(1)
            dmix(0)
            mix(0)
            scores(2)
            dmix(1)
            mix(1)
            dqk(1)
            scores(3)
            dmix(2)
            mix(2)
            scores(4)
            dmix(3)
            mix(3)
            mix(4)
            a = jnp.concatenate([ot_s[...].T, dec_out(e0, CD)], axis=0).astype(BF16)
            x1 = round32(xc_s[c].astype(F32) + nn(a, wo_perm()))
            if c == 0:
                wait('wg', 'wu')

                @pl.when(st == 0)
                def _():
                    wait('wd')

            def put(x, rows):
                @pl.when(st == 0)
                def _():
                    so_s[c] = (x + nt(act_s[...], wd_s[...])).astype(BF16)

                @pl.when(st > 0)
                def _():
                    so_s[c] = (x + nn(act_s[...], wdt_s[...])).astype(BF16)

            mlp(x1, CR, put)
            if c == 0:
                @pl.when(st == 0)
                def _():
                    pl.semaphore_wait(bar, 1)

                @pl.when(st > 0)
                def _():
                    pl.semaphore_wait(bar, 2)
            hop(c).start()

        @pl.when(st == LAST)
        def _():
            kt, vt = project()
            loads()
            put_prompt(kt, vt)
            for k in range(2):
                dec_scores(e0 + CD + k, kp_s[...].reshape(KVW, CL), 2 * DR + k)
            dqk(0)
            dqk(1)
            for k in range(2):
                dec_mix(c, CD + k, vp_s[...].reshape(KVW, CL), off + k * SEG + SEG - 1, 2 * DR + k)
            for q in range(4):
                dmix(q)
            if c == 0:
                wait('wg', 'wu', 'gf')
                pl.semaphore_wait(bar, 1)
            else:
                ls = [dec_out(k * ES + CD, 8)[:2] for k in range(2)]
                a = jnp.concatenate([dec_out(0, CD), dec_out(ES, CD)] + ls + [jnp.zeros((4, HID), F32)], axis=0).astype(BF16)
                xs = [xc_s[k].astype(F32) for k in range(2)]
                xf = jnp.concatenate([xs[0][CP:], xs[1][CP:]] + last_rows(xs[0]) + last_rows(xs[1]) + [jnp.zeros((4, HID), F32)], axis=0)

                def put(x, rows):
                    x2 = round32(x + nn(act_s[:rows, :], wdt_s[...]))
                    fh = rms(x2, gf_s[...].astype(F32).reshape(1, HID))
                    ri = lax.broadcasted_iota(jnp.int32, (FR, FR), 0)
                    src = jnp.where(ri < ND, (ri % NM) * DR + ri // NM, ri)
                    fh_s[...] = nn(jnp.where(lane_iota((FR, FR)) == src, 1.0, 0.0).astype(BF16), fh).astype(BF16)

                mlp(round32(xf + nn(a, wo_perm())), FR, put)
                ofh = pltpu.make_async_copy(fh_s, fh_o, out_sem.at[6])
                ofh.start()
                ofh.wait()

    for c in range(2):
        pltpu.make_async_copy(kdn_s.at[c], kdn.at[c], out_sem.at[c]).wait()
        pltpu.make_async_copy(vdn_s.at[c], vdn.at[c], out_sem.at[2 + c]).wait()
    pltpu.make_async_copy(kp_s, kpn, out_sem.at[4]).wait()
    pltpu.make_async_copy(vp_s, vpn, out_sem.at[5]).wait()

    @pl.when(st < LAST)
    def _():
        wait('gf')
        for c in range(2):
            hop(c).wait_send()


def head_kernel(fh, tok, fo, fh_s, fr_s, lsem, ssem, rsem):
    st = lax.axis_index('stage')
    lfh = pltpu.make_async_copy(fh, fh_s, lsem)
    bar = pltpu.get_barrier_semaphore()

    def send(k):
        return pltpu.make_async_remote_copy(fh_s, fr_s, ssem.at[k], rsem, device_id={'stage': k}, device_id_type=MESH)

    @pl.when(st < LAST)
    def _():
        pl.semaphore_signal(bar, inc=1, device_id={'stage': LAST}, device_id_type=MESH)

    @pl.when(st == LAST)
    def _():
        lfh.start()
        for k in range(LAST):
            pl.semaphore_signal(bar, inc=1, device_id={'stage': k}, device_id_type=MESH)
        pl.semaphore_wait(bar, LAST)
        lfh.wait()
        for k in range(LAST):
            send(k).start()
        fo[...] = fh_s[...]
        for k in range(LAST):
            send(k).wait_send()

    @pl.when(st < LAST)
    def _():
        pl.semaphore_wait(bar, 1)
        send(0).wait_recv()
        fo[...] = fr_s[...]


def tile_start(pos):
    return pl.ds(pl.multiple_of((pos // LN) * LN, LN), LN)


def copy_all(kd, vd, ko, vo, ks, vs, ksem, vsem, edit):
    ins = [(pltpu.make_async_copy(kd.at[m], ks.at[m], ksem.at[m]), pltpu.make_async_copy(vd.at[m], vs.at[m], vsem.at[m])) for m in range(NM)]
    for a, b in ins:
        a.start()
        b.start()
    outs = []
    for m in range(NM):
        for c, scr, out, sem, w in ((ins[m][0], ks, ko, ksem, 0), (ins[m][1], vs, vo, vsem, 1)):
            c.wait()
            if edit is not None:
                edit(m, scr, w)
            o = pltpu.make_async_copy(scr.at[m], out.at[m], sem.at[m])
            o.start()
            outs.append(o)
    for o in outs:
        o.wait()


def pre_kernel(kd, vd, ko, vo, tok, ks, vs, ksem, vsem):
    st = lax.axis_index('stage')

    @pl.when(st >= 2)
    def _():
        copy_all(kd, vd, ko, vo, ks, vs, ksem, vsem, None)


def load_new(srcs, dsts, sem):
    cs = [pltpu.make_async_copy(a, b, sem.at[i]) for i, (a, b) in enumerate(zip(srcs, dsts))]
    for c in cs:
        c.start()
    return cs


def update_tiles(dlen, bk, bv, ko, vo, kpo, vpo, kt, vt, new, cs, ksem, vsem, nsem, extra=None):
    lane = lane_iota((HD, LN))

    def cp(hbm, scr, sem, m, i, out):
        h = hbm.at[m, i, :, :, tile_start(dlen[m, i])]
        v = scr.at[m, i]
        return pltpu.make_async_copy(v, h, sem.at[m]) if out else pltpu.make_async_copy(h, v, sem.at[m])

    cs[4].wait()
    for m in range(NM):
        for i in range(DR):
            cp(bk, kt, ksem, m, i, False).start()
            cp(bv, vt, vsem, m, i, False).start()
    for c in cs[:4]:
        c.wait()
    po = [pltpu.make_async_copy(new[2], kpo, nsem.at[2]), pltpu.make_async_copy(new[3], vpo, nsem.at[3])]
    for o in po:
        o.start()
    if extra is not None:
        extra()
    for m in range(NM):
        for hbm, scr, sem, nw in ((ko, kt, ksem, new[0]), (vo, vt, vsem, new[1])):
            for i in range(DR):
                cp(hbm, scr, sem, m, i, False).wait()
            for i in range(DR):
                pos = dlen[m, i]
                for g in range(NKV):
                    col = nw[m // 2, g * HD:(g + 1) * HD, m % 2 * DR + i:m % 2 * DR + i + 1]
                    scr[m, i, g] = jnp.where(lane == pos % LN, col, scr[m, i, g].astype(F32)).astype(BF16)
            for i in range(DR):
                cp(hbm, scr, sem, m, i, True).start()
    for m in range(NM):
        for i in range(DR):
            cp(ko, kt, ksem, m, i, True).wait()
            cp(vo, vt, vsem, m, i, True).wait()
    for o in po:
        o.wait()


def mid_kernel(dlen_h, kd, vd, bk, bv, kdn, vdn, kpn, vpn, ko, vo, kpo, vpo, tok, ks, vs, kt, vt, kn_s, vn_s, kp_s, vp_s, dlen, ksem, vsem, nsem):
    st = lax.axis_index('stage')
    new = (kn_s, vn_s, kp_s, vp_s)

    @pl.when(st < 2)
    def _():
        cs = load_new((kdn, vdn, kpn, vpn, dlen_h), new + (dlen,), nsem)
        for c in cs:
            c.wait()
        po = [pltpu.make_async_copy(kp_s, kpo, nsem.at[2]), pltpu.make_async_copy(vp_s, vpo, nsem.at[3])]
        for o in po:
            o.start()
        lane = lane_iota((HD, LN))

        def edit(m, scr, w):
            for i in range(DR):
                pos = dlen[m, i]
                sl = tile_start(pos)
                for g in range(NKV):
                    col = new[w][m // 2, g * HD:(g + 1) * HD, m % 2 * DR + i:m % 2 * DR + i + 1]
                    scr[m, i, g, :, sl] = jnp.where(lane == pos % LN, col, scr[m, i, g, :, sl].astype(F32)).astype(BF16)

        copy_all(kd, vd, ko, vo, ks, vs, ksem, vsem, edit)
        for o in po:
            o.wait()

    @pl.when(st == 2)
    def _():
        cs = load_new((kdn, vdn, kpn, vpn, dlen_h), new + (dlen,), nsem)
        update_tiles(dlen, bk, bv, ko, vo, kpo, vpo, kt, vt, new, cs, ksem, vsem, nsem)


def post_kernel(dlen_h, kdn, vdn, kpn, vpn, fr, wh, bk, bv, bkp, bvp, ko, vo, kpo, vpo, logits,
                kt, vt, fr_s, wh_s, kn_s, vn_s, kp_s, vp_s, dlen, ksem, vsem, nsem, hsem):
    st = lax.axis_index('stage')
    lf = pltpu.make_async_copy(fr, fr_s, hsem.at[0])
    lw = pltpu.make_async_copy(wh, wh_s, hsem.at[1])

    def head():
        lf.wait()
        lw.wait()
        lg = nn(fr_s[...], wh_s[...])
        for i in range(DR + 1):
            logits[i] = lg[i * NM:(i + 1) * NM]

    @pl.when(st == LAST)
    def _():
        new = (kn_s, vn_s, kp_s, vp_s)
        cs = load_new((kdn, vdn, kpn, vpn, dlen_h), new + (dlen,), nsem)
        lf.start()
        lw.start()
        update_tiles(dlen, bk, bv, ko, vo, kpo, vpo, kt, vt, new, cs, ksem, vsem, nsem, head)

    @pl.when(st < LAST)
    def _():
        lf.start()
        lw.start()
        head()


ANY = pl.BlockSpec(memory_space=pltpu.HBM)


def solution(mesh):
    part = P('replica')
    layer = P('stage')
    cache = P('stage', 'replica')
    in_specs = (part,) * 4 + (layer,) * 9 + (P(), P()) + (cache,) * 4
    out_specs = (part,) + (cache,) * 4
    inv_freq = np.float32(ROPE_BASE) ** (-np.arange(HALF, dtype=np.float32) * np.float32(2.0 / HD))
    ifr_c = np.broadcast_to(inv_freq[:, None], (HALF, NP)).astype(np.float32)

    def device_fn(x_dec, x_pre, dec_len, pre_len, g_attn, w_q, w_k, w_v, w_o, g_mlp, w_gate, w_up, w_down, g_final, w_head, k_dec, v_dec, k_pre, v_pre):
        kd = jnp.transpose(k_dec[0], (0, 1, 3, 4, 2))
        vd = jnp.transpose(v_dec[0], (0, 1, 3, 4, 2))
        kp = jnp.transpose(k_pre[0], (1, 2, 0))
        vp = jnp.transpose(v_pre[0], (1, 2, 0))
        args = (x_dec.reshape(ND, HID), x_pre.reshape(NP, HID), dec_len, pre_len, g_attn, w_q[0], w_k[0].T, w_v[0].T, w_o[0], g_mlp,
                w_gate[0], w_up[0], w_down[0].T, g_final, kd, vd, kp, vp, jnp.asarray(ifr_c))
        vm = lambda shape, dt: pltpu.VMEM(shape, dt)
        scratch = [
            vm((2, CR, HID), BF16), pltpu.SMEM((NM, DR), jnp.int32), pltpu.SMEM((1,), jnp.int32), vm((1, HID), BF16),
            vm((HID, HID), BF16), vm((HID + 2 * KVW, HID), BF16), vm((HID, HID), BF16), vm((1, HID), BF16),
            vm((HID, FFN), BF16), vm((HID, FFN), BF16), vm((HID, FFN), BF16), vm((FFN, HID), BF16), vm((HID,), BF16),
            vm(kd.shape, BF16), vm(vd.shape, BF16), vm(kp.shape, BF16), vm(vp.shape, BF16), vm((HALF, 2 * LN), F32),
            vm((2, HALF, 2 * LN), F32), vm((2, HALF, 2 * LN), F32), vm((HID, LN), BF16),
            vm((2 * ES * 8, LN), F32), vm((2 * ES * 8, LN), F32), vm((2, 24, LN), F32), vm((2 * ES, KVW), F32),
            vm((2 * ES * 8, LN), F32), vm((2 * ES * 8, LN), F32),
            vm((2, KVW, LN), F32), vm((2, KVW, LN), F32), vm(((2 * DR + 2) * 24, CL), F32), vm((2, CL, 2 * LN), F32), vm((2, CL, 2 * LN), BF16),
            vm((CL, LN), F32), vm((HID, LN), F32), vm((CR, FFN), BF16), vm((2, CR, HID), BF16), vm((FR, HID), BF16),
            pltpu.SemaphoreType.DMA((19,)), pltpu.SemaphoreType.DMA((NM,)), pltpu.SemaphoreType.DMA((NM,)), pltpu.SemaphoreType.DMA((7,)),
            pltpu.SemaphoreType.DMA((2,)), pltpu.SemaphoreType.DMA((2,)),
        ]
        sds = jax.ShapeDtypeStruct
        big = pltpu.CompilerParams(vmem_limit_bytes=62 * 1024 * 1024)
        cshape = sds(kd.shape, BF16)
        pshape = sds(kp.shape, BF16)
        nsems = [pltpu.SemaphoreType.DMA((NM,)), pltpu.SemaphoreType.DMA((NM,))]
        tile = vm((NM, DR, NKV, HD, LN), BF16)
        news = [vm((2, KVW, LN), F32), vm((2, KVW, LN), F32), vm(kp.shape, BF16), vm(vp.shape, BF16), pltpu.SMEM((NM, DR), jnp.int32)]
        vmem = pl.BlockSpec(memory_space=pltpu.VMEM)
        tshape = sds((8, LN), F32)
        bk, bv, tok = pl.pallas_call(
            pre_kernel, out_shape=(cshape, cshape, tshape), in_specs=[ANY, ANY], out_specs=(ANY, ANY, ANY),
            scratch_shapes=[vm(kd.shape, BF16), vm(vd.shape, BF16)] + nsems, name='pre', compiler_params=big)(kd, vd)
        args = args + (tok,)
        kdn, vdn, kpn, vpn, fh = pl.pallas_call(
            pipe_kernel,
            out_shape=(sds((2, KVW, LN), F32), sds((2, KVW, LN), F32), pshape, pshape, sds((ND + 8, HID), BF16)),
            in_specs=[ANY] * len(args),
            out_specs=(ANY,) * 5,
            scratch_shapes=scratch,
            name='pipe',
            compiler_params=pltpu.CompilerParams(collective_id=0, has_side_effects=True, vmem_limit_bytes=62 * 1024 * 1024),
        )(*args)
        bk, bv, bkp, bvp, tok2 = pl.pallas_call(
            mid_kernel, out_shape=(cshape, cshape, pshape, pshape, tshape), in_specs=[ANY] * 9, out_specs=(ANY,) * 5,
            input_output_aliases={3: 0, 4: 1},
            scratch_shapes=[vm(kd.shape, BF16), vm(vd.shape, BF16), tile, tile] + news + nsems + [pltpu.SemaphoreType.DMA((5,))],
            name='mid', compiler_params=big)(dec_len, kd, vd, bk, bv, kdn, vdn, kpn, vpn)
        fr = pl.pallas_call(
            head_kernel, out_shape=sds((FR, HID), BF16), in_specs=[ANY] * 2, out_specs=vmem,
            scratch_shapes=[vm((FR, HID), BF16), vm((FR, HID), BF16),
                            pltpu.SemaphoreType.DMA, pltpu.SemaphoreType.DMA((LAST,)), pltpu.SemaphoreType.DMA],
            name='head', compiler_params=pltpu.CompilerParams(collective_id=1, has_side_effects=True))(fh, tok2)
        ko, vo, kpo, vpo, logits = pl.pallas_call(
            post_kernel, out_shape=(cshape, cshape, pshape, pshape, sds((DR + 1, NM, VOC), F32)), in_specs=[ANY] * 11,
            out_specs=(ANY,) * 4 + (vmem,), input_output_aliases={7: 0, 8: 1, 9: 2, 10: 3},
            scratch_shapes=[tile, tile, vm((FR, HID), BF16), vm((HID, VOC), BF16)] + news + nsems + [pltpu.SemaphoreType.DMA((5,)), pltpu.SemaphoreType.DMA((2,))],
            name='post', compiler_params=big)(dec_len, kdn, vdn, kpn, vpn, fr, w_head, bk, bv, bkp, bvp)
        back = lambda a: jnp.transpose(a, (0, 1, 4, 2, 3))[None]
        backp = lambda a: jnp.transpose(a, (2, 0, 1))[None]
        return jnp.transpose(logits, (1, 0, 2)), back(ko), back(vo), backp(kpo), backp(vpo)

    return jax.shard_map(device_fn, mesh=mesh, in_specs=in_specs, out_specs=out_specs, check_vma=False)
```

```python
import functools

import jax
import jax.numpy as jnp
import numpy as np
from jax import lax
from jax.experimental import pallas as pl
from jax.experimental.pallas import tpu as pltpu
from jax.sharding import PartitionSpec as P

F32 = jnp.float32
BF16 = jnp.bfloat16
MESH = pl.DeviceIdType.MESH
NORM_EPS = 1e-6
ROPE_BASE = 10000.0
NEG = -1e30

HID = 576
NQ = 9
NKV = 3
GRP = 3
HD = 64
HALF = 32
KVW = NKV * HD
FFN = 1536
NM = 4
DR = 8
SEG = 64
CL = 512
VOC = 1024
ND = NM * DR
NP = NM * SEG
LAST = 3
LN = 128
CP = 128
CD = 16
CR = CP + CD
ES = CD + 8
FR = ND + 8


def nt(a, b):
    return lax.dot_general(a, b, (((1,), (1,)), ((), ())), preferred_element_type=F32)


def nn(a, b):
    return jnp.dot(a, b, preferred_element_type=F32)


def rms(x, g):
    inv = lax.rsqrt(jnp.mean(x * x, axis=-1, keepdims=True) + NORM_EPS)
    return (x * inv * g).astype(BF16)


def rope_t(m, cos, sin):
    parts = []
    for j in range(m.shape[0] // HD):
        a = m[j * HD:j * HD + HALF]
        b = m[j * HD + HALF:(j + 1) * HD]
        parts += [a * cos - b * sin, b * cos + a * sin]
    return jnp.concatenate(parts, axis=0)


def lane_iota(shape):
    return lax.broadcasted_iota(jnp.int32, shape, len(shape) - 1)


def pipe_kernel(xd, xp, dlen, plen, ga, wq, wk, wv, wo, gm, wg, wu, wd, gf, kd, vd, kp, vp, ifr, tok,
                kdn, vdn, kpn, vpn, fh_o,
                xc_s, dl_s, pl_s, ga_s, wq_s, w3_s, wo_s, gm_s, wg_s, wu_s, wd_s, wdt_s, gf_s,
                kd_s, vd_s, kp_s, vp_s, ifr_s,
                cos_s, sin_s, qt_s, qa_s, qb_s, self_s, vn_s, oa_s, ob_s,
                kdn_s, vdn_s, sc_s, ps_s, pb_s, bias_s, ot_s, act_s, so_s, fh_s,
                in_sem, kd_sem, vd_sem, out_sem, ssem, rsem):
    st = lax.axis_index('stage')
    order = [(dlen, dl_s), (plen, pl_s), (ga, ga_s), (ifr, ifr_s), (wq, wq_s), (wk, w3_s.at[HID:HID + KVW]), (wv, w3_s.at[HID + KVW:]),
             (kp, kp_s), (vp, vp_s), (wo, wo_s), (gm, gm_s), (wg, wg_s), (wu, wu_s), (wd, wd_s), (gf, gf_s),
             (xp.at[0:CP], xc_s.at[0, 0:CP]), (xd.at[0:CD], xc_s.at[0, CP:CR]), (xp.at[CP:2 * CP], xc_s.at[1, 0:CP]), (xd.at[CD:2 * CD], xc_s.at[1, CP:CR])]
    names = ['dl', 'pl', 'ga', 'ifr', 'wq', 'wk', 'wv', 'kp', 'vp', 'wo', 'gm', 'wg', 'wu', 'wd', 'gf', 'p0', 'd0', 'p1', 'd1']
    cps = {n: pltpu.make_async_copy(a, b, in_sem.at[i]) for i, (n, (a, b)) in enumerate(zip(names, order))}
    kcp = [pltpu.make_async_copy(kd.at[m], kd_s.at[m], kd_sem.at[m]) for m in range(NM)]
    vcp = [pltpu.make_async_copy(vd.at[m], vd_s.at[m], vd_sem.at[m]) for m in range(NM)]

    def start(*ns):
        for n in ns:
            cps[n].start()

    def wait(*ns):
        for n in ns:
            cps[n].wait()

    start('dl', 'pl', 'ifr', 'ga', 'wq', 'wk', 'wv')

    @pl.when(st == 0)
    def _():
        start('p0', 'd0')

    bar = pltpu.get_barrier_semaphore()

    @pl.when(st > 0)
    def _():
        pl.semaphore_signal(bar, inc=1, device_id={'stage': jnp.maximum(st - 1, 0)}, device_id_type=MESH)

    @pl.when(st < LAST)
    def _():
        pl.semaphore_signal(bar, inc=1, device_id={'stage': jnp.minimum(st + 1, LAST)}, device_id_type=MESH)

    wait('dl', 'pl', 'ifr')
    for m in range(2):
        kcp[m].start()
        vcp[m].start()
    start('kp', 'vp')

    @pl.when(st > 0)
    def _():
        start('wo', 'gm', 'wg', 'wu', 'wd', 'gf')
        for m in (2, 3):
            kcp[m].start()
            vcp[m].start()

    p0 = pl_s[0]
    li = lane_iota((1, 2 * LN))
    fr = ifr_s[...]
    for c in range(2):
        pos = p0 + (c * CP) + li
        for k in range(CD):
            pos = jnp.where(li == LN + k, dl_s[2 * c + k // DR, k % DR], pos)
        for k in range(2):
            pos = jnp.where(li == LN + CD + k, p0 + (c * CP + k * SEG + SEG - 1), pos)
        ang = fr * pos.astype(F32)
        cos_s[c] = jnp.cos(ang)
        sin_s[c] = jnp.sin(ang)
    qa_s[...] = jnp.zeros_like(qa_s)
    qb_s[...] = jnp.zeros_like(qb_s)
    ob_s[...] = jnp.zeros_like(ob_s)
    for k in range(2):
        pb_s[k] = jnp.zeros((CL, 2 * LN), BF16)

    wait('ga', 'wq')
    w3_s[:HID, :] = wq_s[...].astype(F32).T.astype(BF16)
    wait('wk', 'wv')

    @pl.when(st > 0)
    def _():
        wait('wd')
        for k in range(0, FFN, LN):
            wdt_s[k:k + LN, :] = wd_s[:, k:k + LN].astype(F32).T.astype(BF16)

    gat = ga_s[...].astype(F32)

    lgrp = lane_iota((8, KVW)) // HD

    def dec_scores(e, kt, slot):
        qb = jnp.concatenate([qa_s[e * 8:e * 8 + 8, :], qb_s[e * 8:e * 8 + 8, :HD]], axis=1)
        lhs = jnp.concatenate([jnp.where(lgrp == g, qb, 0.0) for g in range(NKV)], axis=0).astype(BF16)
        sc_s[slot * 24:slot * 24 + 24, :] = nn(lhs, kt)

    def dec_mix(c, k, vt, pos, slot):
        e = c * ES + k
        selfcol = jnp.sum(jnp.where(lane_iota((24, LN)) == k, self_s[c], 0.0), axis=-1, keepdims=True)
        s = jnp.where(lane_iota((24, CL)) < pos, sc_s[slot * 24:slot * 24 + 24, :], NEG)
        mx = jnp.maximum(jnp.max(s, axis=-1, keepdims=True), selfcol)
        p = jnp.exp(s - mx)
        ps = jnp.exp(selfcol - mx)
        rl = 1.0 / (jnp.sum(p, axis=-1, keepdims=True) + ps)
        o = nt((p * rl).astype(BF16), vt)
        o = o + (ps * rl).astype(BF16).astype(F32) * vn_s[e:e + 1, :]
        acc = jnp.where(lgrp == 0, o[0:8], 0.0)
        for g in range(1, NKV):
            acc = jnp.where(lgrp == g, o[8 * g:8 * g + 8], acc)
        oa_s[e * 8:e * 8 + 8, :] = acc[:, :LN]
        ob_s[e * 8:e * 8 + 8, :HD] = acc[:, LN:]

    def dec_out(e, n):
        return jnp.concatenate([x for r in range(GRP) for x in
                                (oa_s[pl.ds(e * 8 + r, n, stride=8), :], ob_s[pl.ds(e * 8 + r, n, stride=8), :][:, :HD])], axis=1)

    def wo_perm():
        return jnp.concatenate([wo_s[(g * GRP + r) * HD:(g * GRP + r + 1) * HD, :] for r in range(GRP) for g in range(NKV)], axis=0)

    def mlp(x, rows, put):
        h2 = rms(x, gm_s[...].astype(F32))
        step = 512
        for c in range(FFN // step):
            gt = nn(h2, wg_s[:, c * step:(c + 1) * step])
            up = nn(h2, wu_s[:, c * step:(c + 1) * step])
            act_s[:rows, c * step:(c + 1) * step] = (gt * (1.0 / (1.0 + jnp.exp(-gt))) * up).astype(BF16)
        put(x, rows)

    def round32(x):
        return x.astype(BF16).astype(F32)

    def hop(c):
        return pltpu.make_async_remote_copy(so_s.at[c], xc_s.at[c], ssem.at[c], rsem.at[c],
                                            device_id={'stage': jnp.minimum(st + 1, LAST)}, device_id_type=MESH)

    def last_rows(x):
        return [x[k * SEG + SEG - 1:k * SEG + SEG] for k in range(2)]

    for c in range(2):
        lim = CL - CP if c == 0 else CL

        @pl.when(st == 0)
        def _():
            wait('p%d' % c, 'd%d' % c)

        @pl.when(st > 0)
        def _():
            hop(c).wait_recv()

        if c == 0:
            wait('kp', 'vp')
        else:
            for m in (2, 3):
                kcp[m].wait()
                vcp[m].wait()
        off = p0 + c * CP
        e0 = c * ES

        def project():
            x = xc_s[c].astype(F32)
            h = x * lax.rsqrt(jnp.mean(x * x, axis=-1, keepdims=True) + NORM_EPS) * gat
            h = jnp.concatenate([h] + last_rows(h) + [jnp.zeros((2 * LN - CR - 2, HID), F32)], axis=0).astype(BF16)
            half = (HID + 2 * KVW) // 2
            qkv = jnp.concatenate([nt(w3_s[:half, :], h), nt(w3_s[half:, :], h)], axis=0)
            cos, sin = cos_s[c], sin_s[c]
            qt = round32(rope_t(qkv[:HID], cos, sin)) * (HD ** -0.5)
            kt = round32(rope_t(qkv[HID:HID + KVW], cos, sin))
            vt = round32(qkv[HID + KVW:])
            qt_s[...] = qt[:, :LN].astype(BF16)
            qe, ke, ve = qt[:, LN:], kt[:, LN:], vt[:, LN:]
            row = lax.broadcasted_iota(jnp.int32, (24, LN), 0)
            sf = jnp.zeros((24, LN), F32)
            for g in range(NKV):
                for r in range(GRP):
                    j = g * GRP + r
                    v = jnp.sum(qe[j * HD:(j + 1) * HD] * ke[g * HD:(g + 1) * HD], axis=0, keepdims=True)
                    sf = jnp.where(row == 8 * g + r, v, sf)
            self_s[c] = sf
            n = CD + 8
            pad = jnp.zeros((HD, LN), F32)
            for r in range(GRP):
                qr = [qe[(g * GRP + r) * HD:(g * GRP + r + 1) * HD] for g in range(NKV)]
                qa_s[pl.ds(e0 * 8 + r, n, stride=8), :] = jnp.concatenate(qr[:2], axis=0).T[:n]
                qb_s[pl.ds(e0 * 8 + r, n, stride=8), :] = jnp.concatenate([qr[2], pad], axis=0).T[:n]
            vn_s[e0:e0 + n, :LN] = ve[:LN].T[:n]
            vn_s[e0:e0 + n, LN:] = jnp.concatenate([ve[LN:], pad], axis=0).T[:n, :HD]
            kdn_s[c] = ke
            vdn_s[c] = ve
            pltpu.make_async_copy(kdn_s.at[c], kdn.at[c], out_sem.at[c]).start()
            pltpu.make_async_copy(vdn_s.at[c], vdn.at[c], out_sem.at[2 + c]).start()
            return kt, vt

        def put_prompt(kt, vt):
            place = jnp.where(lax.broadcasted_iota(jnp.int32, (CP, CL), 0) + off == lane_iota((CP, CL)), 1.0, 0.0).astype(BF16)
            lp = lane_iota((KVW, CL)) - off
            fresh = (lp >= 0) & (lp < CP)
            kpu = jnp.where(fresh, nn(kt[:, :LN].astype(BF16), place), kp_s[...].reshape(KVW, CL).astype(F32))
            vpu = jnp.where(fresh, nn(vt[:, :LN].astype(BF16), place), vp_s[...].reshape(KVW, CL).astype(F32))
            kp_s[...] = kpu.astype(BF16).reshape(NKV, HD, CL)
            vp_s[...] = vpu.astype(BF16).reshape(NKV, HD, CL)
            if c == 1:
                pltpu.make_async_copy(kp_s, kpn, out_sem.at[4]).start()
                pltpu.make_async_copy(vp_s, vpn, out_sem.at[5]).start()
            return kpu

        def loads():
            if c == 0:
                for m in (0, 1):
                    kcp[m].wait()
                    vcp[m].wait()

                @pl.when(st == 0)
                def _():
                    start('wo', 'gm', 'wg', 'wu', 'wd', 'gf', 'p1', 'd1')

        def dqk(i):
            for k in range(DR):
                dec_scores(c * ES + i * DR + k, kd_s[2 * c + i, k].reshape(KVW, CL), i * DR + k)

        def dmix(q):
            for k in range(4 * q, 4 * q + 4):
                m, i = 2 * c + k // DR, k % DR
                dec_mix(c, k, vd_s[m, i].reshape(KVW, CL), dl_s[m, i], k)

        @pl.when(st < LAST)
        def _():
            kt, vt = project()
            loads()
            kpu = put_prompt(kt, vt)
            kfull = kpu[:, :lim].T.astype(BF16)
            bias_s[:lim, :] = jnp.where(lax.broadcasted_iota(jnp.int32, (lim, LN), 0) <= lane_iota((lim, LN)) + off, 0.0, NEG)

            def heads(t):
                return [j for j in (2 * t, 2 * t + 1) if j < NQ]

            def scores(t):
                cols = []
                for j in heads(t):
                    g = j // GRP
                    parts = [jnp.zeros((g * HD, LN), BF16)] * (g > 0) + [qt_s[j * HD:(j + 1) * HD, :]]
                    parts += [jnp.zeros(((NKV - 1 - g) * HD, LN), BF16)] * (g < NKV - 1)
                    cols.append(jnp.concatenate(parts, axis=0))
                w = len(cols) * LN
                rhs = jnp.concatenate(cols, axis=1)
                for q in range(0, lim, lim // 2):
                    ps_s[t % 2, q:q + lim // 2, :w] = nn(kfull[q:q + lim // 2], rhs)

            def fold(v, op):
                return op(v.reshape(v.shape[0] // 8, 8, v.shape[1]), axis=0)

            def mix(t):
                sl = t % 2
                ck = 64
                hs = heads(t)
                for i, j in enumerate(hs):
                    ln = slice(i * LN, (i + 1) * LN)
                    mx = jnp.full((8, LN), NEG, F32)
                    for q in range(0, lim, ck):
                        mx = jnp.maximum(mx, fold(ps_s[sl, q:q + ck, ln] + bias_s[q:q + ck, :], jnp.max))
                    mx = jnp.max(mx, axis=0, keepdims=True)
                    sm = jnp.zeros((8, LN), F32)
                    for q in range(0, lim, ck):
                        p = jnp.exp(ps_s[sl, q:q + ck, ln] + bias_s[q:q + ck, :] - mx)
                        ps_s[sl, q:q + ck, ln] = p
                        sm = sm + fold(p, jnp.sum)
                    rl = 1.0 / jnp.sum(sm, axis=0, keepdims=True)
                    for q in range(0, lim, ck):
                        pb_s[sl, q:q + ck, ln] = (ps_s[sl, q:q + ck, ln] * rl).astype(BF16)
                g0, g1 = hs[0] // GRP, hs[-1] // GRP
                o = nn(vp_s[...].reshape(KVW, CL)[g0 * HD:(g1 + 1) * HD, :lim], pb_s[sl, :lim, :len(hs) * LN])
                for i, j in enumerate(hs):
                    g, r = j // GRP, j % GRP
                    d = (r * NKV + g) * HD
                    ot_s[d:d + HD, :] = o[(g - g0) * HD:(g - g0 + 1) * HD, i * LN:(i + 1) * LN]

            dqk(0)
            scores(0)
            scores(1)
            dmix(0)
            mix(0)
            scores(2)
            dmix(1)
            mix(1)
            dqk(1)
            scores(3)
            dmix(2)
            mix(2)
            scores(4)
            dmix(3)
            mix(3)
            mix(4)
            a = jnp.concatenate([ot_s[...].T, dec_out(e0, CD)], axis=0).astype(BF16)
            if c == 0:
                wait('wo', 'gm', 'wg', 'wu')

                @pl.when(st == 0)
                def _():
                    wait('wd')
                    for m in (2, 3):
                        kcp[m].start()
                        vcp[m].start()
            x1 = round32(xc_s[c].astype(F32) + nn(a, wo_perm()))
            def put(x, rows):
                @pl.when(st == 0)
                def _():
                    so_s[c] = (x + nt(act_s[...], wd_s[...])).astype(BF16)

                @pl.when(st > 0)
                def _():
                    so_s[c] = (x + nn(act_s[...], wdt_s[...])).astype(BF16)

            mlp(x1, CR, put)
            if c == 0:
                @pl.when(st == 0)
                def _():
                    pl.semaphore_wait(bar, 1)

                @pl.when(st > 0)
                def _():
                    pl.semaphore_wait(bar, 2)
            hop(c).start()

        @pl.when(st == LAST)
        def _():
            kt, vt = project()
            loads()
            put_prompt(kt, vt)
            for k in range(2):
                dec_scores(e0 + CD + k, kp_s[...].reshape(KVW, CL), 2 * DR + k)
            dqk(0)
            dqk(1)
            for k in range(2):
                dec_mix(c, CD + k, vp_s[...].reshape(KVW, CL), off + k * SEG + SEG - 1, 2 * DR + k)
            for q in range(4):
                dmix(q)
            if c == 0:
                wait('wo', 'gm', 'wg', 'wu', 'gf')
                pl.semaphore_wait(bar, 1)
            else:
                ls = [dec_out(k * ES + CD, 8)[:2] for k in range(2)]
                a = jnp.concatenate([dec_out(0, CD), dec_out(ES, CD)] + ls + [jnp.zeros((4, HID), F32)], axis=0).astype(BF16)
                xs = [xc_s[k].astype(F32) for k in range(2)]
                xf = jnp.concatenate([xs[0][CP:], xs[1][CP:]] + last_rows(xs[0]) + last_rows(xs[1]) + [jnp.zeros((4, HID), F32)], axis=0)

                def put(x, rows):
                    x2 = round32(x + nn(act_s[:rows, :], wdt_s[...]))
                    fh = rms(x2, gf_s[...].astype(F32).reshape(1, HID))
                    ri = lax.broadcasted_iota(jnp.int32, (FR, FR), 0)
                    src = jnp.where(ri < ND, (ri % NM) * DR + ri // NM, ri)
                    fh_s[...] = nn(jnp.where(lane_iota((FR, FR)) == src, 1.0, 0.0).astype(BF16), fh).astype(BF16)

                mlp(round32(xf + nn(a, wo_perm())), FR, put)
                ofh = pltpu.make_async_copy(fh_s, fh_o, out_sem.at[6])
                ofh.start()
                ofh.wait()

    for c in range(2):
        pltpu.make_async_copy(kdn_s.at[c], kdn.at[c], out_sem.at[c]).wait()
        pltpu.make_async_copy(vdn_s.at[c], vdn.at[c], out_sem.at[2 + c]).wait()
    pltpu.make_async_copy(kp_s, kpn, out_sem.at[4]).wait()
    pltpu.make_async_copy(vp_s, vpn, out_sem.at[5]).wait()

    @pl.when(st < LAST)
    def _():
        wait('gf')
        for c in range(2):
            hop(c).wait_send()


def head_kernel(fh, tok, fo, fh_s, fr_s, lsem, ssem, rsem):
    st = lax.axis_index('stage')
    lfh = pltpu.make_async_copy(fh, fh_s, lsem)
    bar = pltpu.get_barrier_semaphore()
    relay = LAST - 1

    def send(src, k):
        return pltpu.make_async_remote_copy(src, fr_s, ssem.at[k], rsem, device_id={'stage': k}, device_id_type=MESH)

    def hello(k):
        pl.semaphore_signal(bar, inc=1, device_id={'stage': k}, device_id_type=MESH)

    @pl.when(st == LAST)
    def _():
        lfh.start()

    @pl.when(st != relay)
    def _():
        hello(relay)
        pl.semaphore_wait(bar, 1)

    @pl.when(st == relay)
    def _():
        for k in (0, 1, LAST):
            hello(k)
        pl.semaphore_wait(bar, LAST)

    @pl.when(st == LAST)
    def _():
        lfh.wait()
        send(fh_s, relay).start()
        fo[...] = fh_s[...]
        send(fh_s, relay).wait_send()

    @pl.when(st < LAST)
    def _():
        send(fh_s, 0).wait_recv()

        @pl.when(st == relay)
        def _():
            for k in range(relay):
                send(fr_s, k).start()

        fo[...] = fr_s[...]

        @pl.when(st == relay)
        def _():
            for k in range(relay):
                send(fr_s, k).wait_send()


def tile_start(pos):
    return pl.ds(pl.multiple_of((pos // LN) * LN, LN), LN)


def copy_all(kd, vd, ko, vo, ks, vs, ksem, vsem, edit):
    ins = [(pltpu.make_async_copy(kd.at[m], ks.at[m], ksem.at[m]), pltpu.make_async_copy(vd.at[m], vs.at[m], vsem.at[m])) for m in range(NM)]
    for a, b in ins:
        a.start()
        b.start()
    outs = []
    for m in range(NM):
        for c, scr, out, sem, w in ((ins[m][0], ks, ko, ksem, 0), (ins[m][1], vs, vo, vsem, 1)):
            c.wait()
            if edit is not None:
                edit(m, scr, w)
            o = pltpu.make_async_copy(scr.at[m], out.at[m], sem.at[m])
            o.start()
            outs.append(o)
    for o in outs:
        o.wait()


def pre_kernel(kd, vd, ko, vo, tok, ks, vs, ksem, vsem):
    st = lax.axis_index('stage')

    @pl.when(st >= 2)
    def _():
        copy_all(kd, vd, ko, vo, ks, vs, ksem, vsem, None)


def load_new(srcs, dsts, sem):
    cs = [pltpu.make_async_copy(a, b, sem.at[i]) for i, (a, b) in enumerate(zip(srcs, dsts))]
    for c in cs:
        c.start()
    return cs


def update_tiles(dlen, bk, bv, ko, vo, kpo, vpo, kt, vt, new, cs, ksem, vsem, nsem, extra=None):
    lane = lane_iota((HD, LN))

    def cp(hbm, scr, sem, m, i, out):
        h = hbm.at[m, i, :, :, tile_start(dlen[m, i])]
        v = scr.at[m, i]
        return pltpu.make_async_copy(v, h, sem.at[m]) if out else pltpu.make_async_copy(h, v, sem.at[m])

    cs[4].wait()
    for m in range(NM):
        for i in range(DR):
            cp(bk, kt, ksem, m, i, False).start()
            cp(bv, vt, vsem, m, i, False).start()
    if extra is not None:
        extra[0]()
    for c in cs[:4]:
        c.wait()
    po = [pltpu.make_async_copy(new[2], kpo, nsem.at[2]), pltpu.make_async_copy(new[3], vpo, nsem.at[3])]
    for o in po:
        o.start()
    for m in range(NM):
        for hbm, scr, sem, nw in ((ko, kt, ksem, new[0]), (vo, vt, vsem, new[1])):
            for i in range(DR):
                cp(hbm, scr, sem, m, i, False).wait()
            for i in range(DR):
                pos = dlen[m, i]
                for g in range(NKV):
                    col = nw[m // 2, g * HD:(g + 1) * HD, m % 2 * DR + i:m % 2 * DR + i + 1]
                    scr[m, i, g] = jnp.where(lane == pos % LN, col, scr[m, i, g].astype(F32)).astype(BF16)
            for i in range(DR):
                cp(hbm, scr, sem, m, i, True).start()
    if extra is not None:
        extra[1]()
    for m in range(NM):
        for i in range(DR):
            cp(ko, kt, ksem, m, i, True).wait()
            cp(vo, vt, vsem, m, i, True).wait()
    for o in po:
        o.wait()


def mid_kernel(dlen_h, kd, vd, bk, bv, kdn, vdn, kpn, vpn, ko, vo, kpo, vpo, tok, ks, vs, kt, vt, kn_s, vn_s, kp_s, vp_s, dlen, ksem, vsem, nsem):
    st = lax.axis_index('stage')
    new = (kn_s, vn_s, kp_s, vp_s)

    @pl.when(st < 2)
    def _():
        cs = load_new((kdn, vdn, kpn, vpn, dlen_h), new + (dlen,), nsem)
        for c in cs:
            c.wait()
        po = [pltpu.make_async_copy(kp_s, kpo, nsem.at[2]), pltpu.make_async_copy(vp_s, vpo, nsem.at[3])]
        for o in po:
            o.start()
        lane = lane_iota((HD, LN))

        def edit(m, scr, w):
            for i in range(DR):
                pos = dlen[m, i]
                sl = tile_start(pos)
                for g in range(NKV):
                    col = new[w][m // 2, g * HD:(g + 1) * HD, m % 2 * DR + i:m % 2 * DR + i + 1]
                    scr[m, i, g, :, sl] = jnp.where(lane == pos % LN, col, scr[m, i, g, :, sl].astype(F32)).astype(BF16)

        copy_all(kd, vd, ko, vo, ks, vs, ksem, vsem, edit)
        for o in po:
            o.wait()

    @pl.when(st == 2)
    def _():
        cs = load_new((kdn, vdn, kpn, vpn, dlen_h), new + (dlen,), nsem)
        update_tiles(dlen, bk, bv, ko, vo, kpo, vpo, kt, vt, new, cs, ksem, vsem, nsem)


def post_kernel(dlen_h, kdn, vdn, kpn, vpn, fr, wh, bk, bv, bkp, bvp, ko, vo, kpo, vpo, logits,
                kt, vt, fr_s, wh_s, kn_s, vn_s, kp_s, vp_s, dlen, ksem, vsem, nsem, hsem):
    st = lax.axis_index('stage')
    lf = pltpu.make_async_copy(fr, fr_s, hsem.at[0])
    lw = pltpu.make_async_copy(wh, wh_s, hsem.at[1])

    def load():
        lf.start()
        lw.start()

    def head():
        lf.wait()
        lw.wait()
        lg = nn(fr_s[...], wh_s[...])
        for i in range(DR + 1):
            logits[i] = lg[i * NM:(i + 1) * NM]

    @pl.when(st == LAST)
    def _():
        new = (kn_s, vn_s, kp_s, vp_s)
        cs = load_new((kdn, vdn, kpn, vpn, dlen_h), new + (dlen,), nsem)
        update_tiles(dlen, bk, bv, ko, vo, kpo, vpo, kt, vt, new, cs, ksem, vsem, nsem, (load, head))

    @pl.when(st < LAST)
    def _():
        load()
        head()


ANY = pl.BlockSpec(memory_space=pltpu.HBM)


def solution(mesh):
    part = P('replica')
    layer = P('stage')
    cache = P('stage', 'replica')
    in_specs = (part,) * 4 + (layer,) * 9 + (P(), P()) + (cache,) * 4
    out_specs = (part,) + (cache,) * 4
    inv_freq = np.float32(ROPE_BASE) ** (-np.arange(HALF, dtype=np.float32) * np.float32(2.0 / HD))
    ifr_c = np.broadcast_to(inv_freq[:, None], (HALF, NP)).astype(np.float32)

    def device_fn(x_dec, x_pre, dec_len, pre_len, g_attn, w_q, w_k, w_v, w_o, g_mlp, w_gate, w_up, w_down, g_final, w_head, k_dec, v_dec, k_pre, v_pre):
        kd = jnp.transpose(k_dec[0], (0, 1, 3, 4, 2))
        vd = jnp.transpose(v_dec[0], (0, 1, 3, 4, 2))
        kp = jnp.transpose(k_pre[0], (1, 2, 0))
        vp = jnp.transpose(v_pre[0], (1, 2, 0))
        args = (x_dec.reshape(ND, HID), x_pre.reshape(NP, HID), dec_len, pre_len, g_attn, w_q[0], w_k[0].T, w_v[0].T, w_o[0], g_mlp,
                w_gate[0], w_up[0], w_down[0].T, g_final, kd, vd, kp, vp, jnp.asarray(ifr_c))
        vm = lambda shape, dt: pltpu.VMEM(shape, dt)
        scratch = [
            vm((2, CR, HID), BF16), pltpu.SMEM((NM, DR), jnp.int32), pltpu.SMEM((1,), jnp.int32), vm((1, HID), BF16),
            vm((HID, HID), BF16), vm((HID + 2 * KVW, HID), BF16), vm((HID, HID), BF16), vm((1, HID), BF16),
            vm((HID, FFN), BF16), vm((HID, FFN), BF16), vm((HID, FFN), BF16), vm((FFN, HID), BF16), vm((HID,), BF16),
            vm(kd.shape, BF16), vm(vd.shape, BF16), vm(kp.shape, BF16), vm(vp.shape, BF16), vm((HALF, 2 * LN), F32),
            vm((2, HALF, 2 * LN), F32), vm((2, HALF, 2 * LN), F32), vm((HID, LN), BF16),
            vm((2 * ES * 8, LN), F32), vm((2 * ES * 8, LN), F32), vm((2, 24, LN), F32), vm((2 * ES, KVW), F32),
            vm((2 * ES * 8, LN), F32), vm((2 * ES * 8, LN), F32),
            vm((2, KVW, LN), F32), vm((2, KVW, LN), F32), vm(((2 * DR + 2) * 24, CL), F32), vm((2, CL, 2 * LN), F32), vm((2, CL, 2 * LN), BF16),
            vm((CL, LN), F32), vm((HID, LN), F32), vm((CR, FFN), BF16), vm((2, CR, HID), BF16), vm((FR, HID), BF16),
            pltpu.SemaphoreType.DMA((19,)), pltpu.SemaphoreType.DMA((NM,)), pltpu.SemaphoreType.DMA((NM,)), pltpu.SemaphoreType.DMA((7,)),
            pltpu.SemaphoreType.DMA((2,)), pltpu.SemaphoreType.DMA((2,)),
        ]
        sds = jax.ShapeDtypeStruct
        big = pltpu.CompilerParams(vmem_limit_bytes=62 * 1024 * 1024)
        cshape = sds(kd.shape, BF16)
        pshape = sds(kp.shape, BF16)
        nsems = [pltpu.SemaphoreType.DMA((NM,)), pltpu.SemaphoreType.DMA((NM,))]
        tile = vm((NM, DR, NKV, HD, LN), BF16)
        news = [vm((2, KVW, LN), F32), vm((2, KVW, LN), F32), vm(kp.shape, BF16), vm(vp.shape, BF16), pltpu.SMEM((NM, DR), jnp.int32)]
        vmem = pl.BlockSpec(memory_space=pltpu.VMEM)
        tshape = sds((8, LN), F32)
        bk, bv, tok = pl.pallas_call(
            pre_kernel, out_shape=(cshape, cshape, tshape), in_specs=[ANY, ANY], out_specs=(ANY, ANY, ANY),
            scratch_shapes=[vm(kd.shape, BF16), vm(vd.shape, BF16)] + nsems, name='pre', compiler_params=big)(kd, vd)
        args = args + (tok,)
        kdn, vdn, kpn, vpn, fh = pl.pallas_call(
            pipe_kernel,
            out_shape=(sds((2, KVW, LN), F32), sds((2, KVW, LN), F32), pshape, pshape, sds((ND + 8, HID), BF16)),
            in_specs=[ANY] * len(args),
            out_specs=(ANY,) * 5,
            scratch_shapes=scratch,
            name='pipe',
            compiler_params=pltpu.CompilerParams(collective_id=0, has_side_effects=True, vmem_limit_bytes=62 * 1024 * 1024),
        )(*args)
        bk, bv, bkp, bvp, tok2 = pl.pallas_call(
            mid_kernel, out_shape=(cshape, cshape, pshape, pshape, tshape), in_specs=[ANY] * 9, out_specs=(ANY,) * 5,
            input_output_aliases={3: 0, 4: 1},
            scratch_shapes=[vm(kd.shape, BF16), vm(vd.shape, BF16), tile, tile] + news + nsems + [pltpu.SemaphoreType.DMA((5,))],
            name='mid', compiler_params=big)(dec_len, kd, vd, bk, bv, kdn, vdn, kpn, vpn)
        fr = pl.pallas_call(
            head_kernel, out_shape=sds((FR, HID), BF16), in_specs=[ANY] * 2, out_specs=vmem,
            scratch_shapes=[vm((FR, HID), BF16), vm((FR, HID), BF16),
                            pltpu.SemaphoreType.DMA, pltpu.SemaphoreType.DMA((LAST,)), pltpu.SemaphoreType.DMA],
            name='head', compiler_params=pltpu.CompilerParams(collective_id=1, has_side_effects=True))(fh, tok2)
        ko, vo, kpo, vpo, logits = pl.pallas_call(
            post_kernel, out_shape=(cshape, cshape, pshape, pshape, sds((DR + 1, NM, VOC), F32)), in_specs=[ANY] * 11,
            out_specs=(ANY,) * 4 + (vmem,), input_output_aliases={7: 0, 8: 1, 9: 2, 10: 3},
            scratch_shapes=[tile, tile, vm((FR, HID), BF16), vm((HID, VOC), BF16)] + news + nsems + [pltpu.SemaphoreType.DMA((5,)), pltpu.SemaphoreType.DMA((2,))],
            name='post', compiler_params=big)(dec_len, kdn, vdn, kpn, vpn, fr, w_head, bk, bv, bkp, bvp)
        back = lambda a: jnp.transpose(a, (0, 1, 4, 2, 3))[None]
        backp = lambda a: jnp.transpose(a, (2, 0, 1))[None]
        return jnp.transpose(logits, (1, 0, 2)), back(ko), back(vo), backp(kpo), backp(vpo)

    return jax.shard_map(device_fn, mesh=mesh, in_specs=in_specs, out_specs=out_specs, check_vma=False)
```

```python
import functools

import jax
import jax.numpy as jnp
import numpy as np
from jax import lax
from jax.experimental import pallas as pl
from jax.experimental.pallas import tpu as pltpu
from jax.sharding import PartitionSpec as P

F32 = jnp.float32
BF16 = jnp.bfloat16
MESH = pl.DeviceIdType.MESH
NORM_EPS = 1e-6
ROPE_BASE = 10000.0
NEG = -1e30

HID = 576
NQ = 9
NKV = 3
GRP = 3
HD = 64
HALF = 32
KVW = NKV * HD
FFN = 1536
NM = 4
DR = 8
SEG = 64
CL = 512
VOC = 1024
ND = NM * DR
NP = NM * SEG
LAST = 3
LN = 128
CP = 128
CD = 16
CR = CP + CD
ES = CD + 8
FR = ND + 8


def nt(a, b):
    return lax.dot_general(a, b, (((1,), (1,)), ((), ())), preferred_element_type=F32)


def nn(a, b):
    return jnp.dot(a, b, preferred_element_type=F32)


def rms(x, g):
    inv = lax.rsqrt(jnp.mean(x * x, axis=-1, keepdims=True) + NORM_EPS)
    return (x * inv * g).astype(BF16)


def rope_t(m, cos, sin):
    parts = []
    for j in range(m.shape[0] // HD):
        a = m[j * HD:j * HD + HALF]
        b = m[j * HD + HALF:(j + 1) * HD]
        parts += [a * cos - b * sin, b * cos + a * sin]
    return jnp.concatenate(parts, axis=0)


def lane_iota(shape):
    return lax.broadcasted_iota(jnp.int32, shape, len(shape) - 1)


def pipe_kernel(xd, xp, dlen, plen, ga, wq, wk, wv, wo, gm, wg, wu, wd, gf, kd, vd, kp, vp, ifr, tok,
                kdn, vdn, kpn, vpn, fh_o,
                xc_s, dl_s, pl_s, ga_s, wq_s, w3_s, wo_s, gm_s, wg_s, wu_s, wd_s, wdt_s, gf_s,
                kd_s, vd_s, kp_s, vp_s, ifr_s,
                cos_s, sin_s, qt_s, qa_s, qb_s, self_s, vn_s, oa_s, ob_s,
                kdn_s, vdn_s, sc_s, ps_s, pb_s, bias_s, ot_s, act_s, so_s, fh_s,
                in_sem, kd_sem, vd_sem, out_sem, ssem, rsem):
    st = lax.axis_index('stage')
    order = [(dlen, dl_s), (plen, pl_s), (ga, ga_s), (ifr, ifr_s), (wq, wq_s), (wk, w3_s.at[HID:HID + KVW]), (wv, w3_s.at[HID + KVW:]),
             (kp, kp_s), (vp, vp_s), (wo, wo_s), (gm, gm_s), (wg, wg_s), (wu, wu_s), (wd, wd_s), (gf, gf_s),
             (xp.at[0:CP], xc_s.at[0, 0:CP]), (xd.at[0:CD], xc_s.at[0, CP:CR]), (xp.at[CP:2 * CP], xc_s.at[1, 0:CP]), (xd.at[CD:2 * CD], xc_s.at[1, CP:CR])]
    names = ['dl', 'pl', 'ga', 'ifr', 'wq', 'wk', 'wv', 'kp', 'vp', 'wo', 'gm', 'wg', 'wu', 'wd', 'gf', 'p0', 'd0', 'p1', 'd1']
    cps = {n: pltpu.make_async_copy(a, b, in_sem.at[i]) for i, (n, (a, b)) in enumerate(zip(names, order))}
    kcp = [pltpu.make_async_copy(kd.at[m], kd_s.at[m], kd_sem.at[m]) for m in range(NM)]
    vcp = [pltpu.make_async_copy(vd.at[m], vd_s.at[m], vd_sem.at[m]) for m in range(NM)]

    def start(*ns):
        for n in ns:
            cps[n].start()

    def wait(*ns):
        for n in ns:
            cps[n].wait()

    start('dl', 'pl', 'ifr', 'ga', 'wq', 'wk', 'wv')

    @pl.when(st == 0)
    def _():
        start('p0', 'd0')

    bar = pltpu.get_barrier_semaphore()

    @pl.when(st > 0)
    def _():
        pl.semaphore_signal(bar, inc=1, device_id={'stage': jnp.maximum(st - 1, 0)}, device_id_type=MESH)

    @pl.when(st < LAST)
    def _():
        pl.semaphore_signal(bar, inc=1, device_id={'stage': jnp.minimum(st + 1, LAST)}, device_id_type=MESH)

    wait('dl', 'pl', 'ifr')
    for m in range(2):
        kcp[m].start()
        vcp[m].start()
    start('kp', 'vp')

    p0 = pl_s[0]
    li = lane_iota((1, 2 * LN))
    fr = ifr_s[...]
    for c in range(2):
        pos = p0 + (c * CP) + li
        for k in range(CD):
            pos = jnp.where(li == LN + k, dl_s[2 * c + k // DR, k % DR], pos)
        for k in range(2):
            pos = jnp.where(li == LN + CD + k, p0 + (c * CP + k * SEG + SEG - 1), pos)
        ang = fr * pos.astype(F32)
        cos_s[c] = jnp.cos(ang)
        sin_s[c] = jnp.sin(ang)
    qa_s[...] = jnp.zeros_like(qa_s)
    qb_s[...] = jnp.zeros_like(qb_s)
    ob_s[...] = jnp.zeros_like(ob_s)
    for k in range(2):
        pb_s[k] = jnp.zeros((CL, 2 * LN), BF16)

    wait('ga', 'wq')
    start('wo', 'gm', 'wg', 'wu', 'wd', 'gf')

    @pl.when(st > 0)
    def _():
        for m in (2, 3):
            kcp[m].start()
            vcp[m].start()

    w3_s[:HID, :] = wq_s[...].astype(F32).T.astype(BF16)
    wait('wk', 'wv')

    @pl.when(st > 0)
    def _():
        wait('wd')
        for k in range(0, FFN, LN):
            wdt_s[k:k + LN, :] = wd_s[:, k:k + LN].astype(F32).T.astype(BF16)

    gat = ga_s[...].astype(F32)

    lgrp = lane_iota((8, KVW)) // HD

    def dec_scores(e, kt, slot):
        qb = jnp.concatenate([qa_s[e * 8:e * 8 + 8, :], qb_s[e * 8:e * 8 + 8, :HD]], axis=1)
        lhs = jnp.concatenate([jnp.where(lgrp == g, qb, 0.0) for g in range(NKV)], axis=0).astype(BF16)
        sc_s[slot * 24:slot * 24 + 24, :] = nn(lhs, kt)

    def dec_mix(c, k, vt, pos, slot):
        e = c * ES + k
        selfcol = jnp.sum(jnp.where(lane_iota((24, LN)) == k, self_s[c], 0.0), axis=-1, keepdims=True)
        s = jnp.where(lane_iota((24, CL)) < pos, sc_s[slot * 24:slot * 24 + 24, :], NEG)
        mx = jnp.maximum(jnp.max(s, axis=-1, keepdims=True), selfcol)
        p = jnp.exp(s - mx)
        ps = jnp.exp(selfcol - mx)
        rl = 1.0 / (jnp.sum(p, axis=-1, keepdims=True) + ps)
        o = nt((p * rl).astype(BF16), vt)
        o = o + (ps * rl).astype(BF16).astype(F32) * vn_s[e:e + 1, :]
        acc = jnp.where(lgrp == 0, o[0:8], 0.0)
        for g in range(1, NKV):
            acc = jnp.where(lgrp == g, o[8 * g:8 * g + 8], acc)
        oa_s[e * 8:e * 8 + 8, :] = acc[:, :LN]
        ob_s[e * 8:e * 8 + 8, :HD] = acc[:, LN:]

    def dec_out(e, n):
        return jnp.concatenate([x for r in range(GRP) for x in
                                (oa_s[pl.ds(e * 8 + r, n, stride=8), :], ob_s[pl.ds(e * 8 + r, n, stride=8), :][:, :HD])], axis=1)

    def wo_perm():
        return jnp.concatenate([wo_s[(g * GRP + r) * HD:(g * GRP + r + 1) * HD, :] for r in range(GRP) for g in range(NKV)], axis=0)

    def mlp(x, rows, put):
        h2 = rms(x, gm_s[...].astype(F32))
        step = 512
        for c in range(FFN // step):
            gt = nn(h2, wg_s[:, c * step:(c + 1) * step])
            up = nn(h2, wu_s[:, c * step:(c + 1) * step])
            act_s[:rows, c * step:(c + 1) * step] = (gt * (1.0 / (1.0 + jnp.exp(-gt))) * up).astype(BF16)
        put(x, rows)

    def round32(x):
        return x.astype(BF16).astype(F32)

    def hop(c):
        return pltpu.make_async_remote_copy(so_s.at[c], xc_s.at[c], ssem.at[c], rsem.at[c],
                                            device_id={'stage': jnp.minimum(st + 1, LAST)}, device_id_type=MESH)

    def last_rows(x):
        return [x[k * SEG + SEG - 1:k * SEG + SEG] for k in range(2)]

    for c in range(2):
        lim = CL - CP if c == 0 else CL

        @pl.when(st == 0)
        def _():
            wait('p%d' % c, 'd%d' % c)

        @pl.when(st > 0)
        def _():
            hop(c).wait_recv()

        if c == 0:
            wait('kp', 'vp')
        else:
            for m in (2, 3):
                kcp[m].wait()
                vcp[m].wait()
        off = p0 + c * CP
        e0 = c * ES

        def project():
            x = xc_s[c].astype(F32)
            h = x * lax.rsqrt(jnp.mean(x * x, axis=-1, keepdims=True) + NORM_EPS) * gat
            h = jnp.concatenate([h] + last_rows(h) + [jnp.zeros((2 * LN - CR - 2, HID), F32)], axis=0).astype(BF16)
            half = (HID + 2 * KVW) // 2
            qkv = jnp.concatenate([nt(w3_s[:half, :], h), nt(w3_s[half:, :], h)], axis=0)
            cos, sin = cos_s[c], sin_s[c]
            qt = round32(rope_t(qkv[:HID], cos, sin)) * (HD ** -0.5)
            kt = round32(rope_t(qkv[HID:HID + KVW], cos, sin))
            vt = round32(qkv[HID + KVW:])
            qt_s[...] = qt[:, :LN].astype(BF16)
            qe, ke, ve = qt[:, LN:], kt[:, LN:], vt[:, LN:]
            row = lax.broadcasted_iota(jnp.int32, (24, LN), 0)
            sf = jnp.zeros((24, LN), F32)
            for g in range(NKV):
                for r in range(GRP):
                    j = g * GRP + r
                    v = jnp.sum(qe[j * HD:(j + 1) * HD] * ke[g * HD:(g + 1) * HD], axis=0, keepdims=True)
                    sf = jnp.where(row == 8 * g + r, v, sf)
            self_s[c] = sf
            n = CD + 8
            pad = jnp.zeros((HD, LN), F32)
            for r in range(GRP):
                qr = [qe[(g * GRP + r) * HD:(g * GRP + r + 1) * HD] for g in range(NKV)]
                qa_s[pl.ds(e0 * 8 + r, n, stride=8), :] = jnp.concatenate(qr[:2], axis=0).T[:n]
                qb_s[pl.ds(e0 * 8 + r, n, stride=8), :] = jnp.concatenate([qr[2], pad], axis=0).T[:n]
            vn_s[e0:e0 + n, :LN] = ve[:LN].T[:n]
            vn_s[e0:e0 + n, LN:] = jnp.concatenate([ve[LN:], pad], axis=0).T[:n, :HD]
            kdn_s[c] = ke
            vdn_s[c] = ve
            pltpu.make_async_copy(kdn_s.at[c], kdn.at[c], out_sem.at[c]).start()
            pltpu.make_async_copy(vdn_s.at[c], vdn.at[c], out_sem.at[2 + c]).start()
            return kt, vt

        def put_prompt(kt, vt):
            place = jnp.where(lax.broadcasted_iota(jnp.int32, (CP, CL), 0) + off == lane_iota((CP, CL)), 1.0, 0.0).astype(BF16)
            lp = lane_iota((KVW, CL)) - off
            fresh = (lp >= 0) & (lp < CP)
            kpu = jnp.where(fresh, nn(kt[:, :LN].astype(BF16), place), kp_s[...].reshape(KVW, CL).astype(F32))
            vpu = jnp.where(fresh, nn(vt[:, :LN].astype(BF16), place), vp_s[...].reshape(KVW, CL).astype(F32))
            kp_s[...] = kpu.astype(BF16).reshape(NKV, HD, CL)
            vp_s[...] = vpu.astype(BF16).reshape(NKV, HD, CL)
            if c == 1:
                pltpu.make_async_copy(kp_s, kpn, out_sem.at[4]).start()
                pltpu.make_async_copy(vp_s, vpn, out_sem.at[5]).start()
            return kpu

        def loads():
            if c == 0:
                for m in (0, 1):
                    kcp[m].wait()
                    vcp[m].wait()

                @pl.when(st == 0)
                def _():
                    start('p1', 'd1')
                    for m in (2, 3):
                        kcp[m].start()
                        vcp[m].start()

        def dqk(i):
            for k in range(DR):
                dec_scores(c * ES + i * DR + k, kd_s[2 * c + i, k].reshape(KVW, CL), i * DR + k)

        def dmix(q):
            for k in range(4 * q, 4 * q + 4):
                m, i = 2 * c + k // DR, k % DR
                dec_mix(c, k, vd_s[m, i].reshape(KVW, CL), dl_s[m, i], k)

        @pl.when(st < LAST)
        def _():
            kt, vt = project()
            loads()
            kpu = put_prompt(kt, vt)
            kfull = kpu[:, :lim].T.astype(BF16)
            bias_s[:lim, :] = jnp.where(lax.broadcasted_iota(jnp.int32, (lim, LN), 0) <= lane_iota((lim, LN)) + off, 0.0, NEG)

            def heads(t):
                return [j for j in (2 * t, 2 * t + 1) if j < NQ]

            def scores(t):
                cols = []
                for j in heads(t):
                    g = j // GRP
                    parts = [jnp.zeros((g * HD, LN), BF16)] * (g > 0) + [qt_s[j * HD:(j + 1) * HD, :]]
                    parts += [jnp.zeros(((NKV - 1 - g) * HD, LN), BF16)] * (g < NKV - 1)
                    cols.append(jnp.concatenate(parts, axis=0))
                w = len(cols) * LN
                rhs = jnp.concatenate(cols, axis=1)
                for q in range(0, lim, lim // 2):
                    ps_s[t % 2, q:q + lim // 2, :w] = nn(kfull[q:q + lim // 2], rhs)

            def fold(v, op):
                return op(v.reshape(v.shape[0] // 8, 8, v.shape[1]), axis=0)

            ck = 64

            def masked(sl, q, ln):
                v = ps_s[sl, q:q + ck, ln]
                return v if q + ck <= 64 else v + bias_s[q:q + ck, :]

            def mix(t):
                sl = t % 2
                hs = heads(t)
                for i, j in enumerate(hs):
                    ln = slice(i * LN, (i + 1) * LN)
                    mx = jnp.full((8, LN), NEG, F32)
                    for q in range(0, lim, ck):
                        mx = jnp.maximum(mx, fold(masked(sl, q, ln), jnp.max))
                    mx = jnp.max(mx, axis=0, keepdims=True)
                    sm = jnp.zeros((8, LN), F32)
                    for q in range(0, lim, ck):
                        p = jnp.exp(masked(sl, q, ln) - mx)
                        ps_s[sl, q:q + ck, ln] = p
                        sm = sm + fold(p, jnp.sum)
                    rl = 1.0 / jnp.sum(sm, axis=0, keepdims=True)
                    for q in range(0, lim, ck):
                        pb_s[sl, q:q + ck, ln] = (ps_s[sl, q:q + ck, ln] * rl).astype(BF16)
                g0, g1 = hs[0] // GRP, hs[-1] // GRP
                o = nn(vp_s[...].reshape(KVW, CL)[g0 * HD:(g1 + 1) * HD, :lim], pb_s[sl, :lim, :len(hs) * LN])
                for i, j in enumerate(hs):
                    g, r = j // GRP, j % GRP
                    d = (r * NKV + g) * HD
                    ot_s[d:d + HD, :] = o[(g - g0) * HD:(g - g0 + 1) * HD, i * LN:(i + 1) * LN]

            dqk(0)
            scores(0)
            scores(1)
            dmix(0)
            mix(0)
            scores(2)
            dmix(1)
            mix(1)
            dqk(1)
            scores(3)
            dmix(2)
            mix(2)
            scores(4)
            dmix(3)
            mix(3)
            mix(4)
            a = jnp.concatenate([ot_s[...].T, dec_out(e0, CD)], axis=0).astype(BF16)
            if c == 0:
                wait('wo', 'gm', 'wg', 'wu')

                @pl.when(st == 0)
                def _():
                    wait('wd')
            x1 = round32(xc_s[c].astype(F32) + nn(a, wo_perm()))
            def put(x, rows):
                @pl.when(st == 0)
                def _():
                    so_s[c] = (x + nt(act_s[...], wd_s[...])).astype(BF16)

                @pl.when(st > 0)
                def _():
                    so_s[c] = (x + nn(act_s[...], wdt_s[...])).astype(BF16)

            mlp(x1, CR, put)
            if c == 0:
                @pl.when(st == 0)
                def _():
                    pl.semaphore_wait(bar, 1)

                @pl.when(st > 0)
                def _():
                    pl.semaphore_wait(bar, 2)
            hop(c).start()

        @pl.when(st == LAST)
        def _():
            kt, vt = project()
            loads()
            put_prompt(kt, vt)
            for k in range(2):
                dec_scores(e0 + CD + k, kp_s[...].reshape(KVW, CL), 2 * DR + k)
            dqk(0)
            dqk(1)
            for k in range(2):
                dec_mix(c, CD + k, vp_s[...].reshape(KVW, CL), off + k * SEG + SEG - 1, 2 * DR + k)
            for q in range(4):
                dmix(q)
            if c == 0:
                wait('wo', 'gm', 'wg', 'wu', 'gf')
                pl.semaphore_wait(bar, 1)
            else:
                ls = [dec_out(k * ES + CD, 8)[:2] for k in range(2)]
                a = jnp.concatenate([dec_out(0, CD), dec_out(ES, CD)] + ls + [jnp.zeros((4, HID), F32)], axis=0).astype(BF16)
                xs = [xc_s[k].astype(F32) for k in range(2)]
                xf = jnp.concatenate([xs[0][CP:], xs[1][CP:]] + last_rows(xs[0]) + last_rows(xs[1]) + [jnp.zeros((4, HID), F32)], axis=0)

                def put(x, rows):
                    x2 = round32(x + nn(act_s[:rows, :], wdt_s[...]))
                    fh = rms(x2, gf_s[...].astype(F32).reshape(1, HID))
                    ri = lax.broadcasted_iota(jnp.int32, (FR, FR), 0)
                    src = jnp.where(ri < ND, (ri % NM) * DR + ri // NM, ri)
                    fh_s[...] = nn(jnp.where(lane_iota((FR, FR)) == src, 1.0, 0.0).astype(BF16), fh).astype(BF16)

                mlp(round32(xf + nn(a, wo_perm())), FR, put)
                ofh = pltpu.make_async_copy(fh_s, fh_o, out_sem.at[6])
                ofh.start()
                ofh.wait()

    for c in range(2):
        pltpu.make_async_copy(kdn_s.at[c], kdn.at[c], out_sem.at[c]).wait()
        pltpu.make_async_copy(vdn_s.at[c], vdn.at[c], out_sem.at[2 + c]).wait()
    pltpu.make_async_copy(kp_s, kpn, out_sem.at[4]).wait()
    pltpu.make_async_copy(vp_s, vpn, out_sem.at[5]).wait()

    @pl.when(st < LAST)
    def _():
        wait('gf')
        for c in range(2):
            hop(c).wait_send()


def head_kernel(fh, wh, tok, logits, fh_s, fr_s, wh_s, lsem, ssem, rsem):
    st = lax.axis_index('stage')
    lfh = pltpu.make_async_copy(fh, fh_s, lsem.at[0])
    lwh = pltpu.make_async_copy(wh, wh_s, lsem.at[1])

    @pl.when(st == LAST)
    def _():
        lfh.start()

    lwh.start()
    bar = pltpu.get_barrier_semaphore()

    def send(k):
        return pltpu.make_async_remote_copy(fh_s, fr_s, ssem.at[k], rsem, device_id={'stage': k}, device_id_type=MESH)

    def head(ref):
        lwh.wait()
        lg = nn(ref[...], wh_s[...])
        for i in range(DR + 1):
            logits[i] = lg[i * NM:(i + 1) * NM]

    @pl.when(st < LAST)
    def _():
        pl.semaphore_signal(bar, inc=1, device_id={'stage': LAST}, device_id_type=MESH)

    @pl.when(st == LAST)
    def _():
        for k in range(LAST):
            pl.semaphore_signal(bar, inc=1, device_id={'stage': k}, device_id_type=MESH)
        pl.semaphore_wait(bar, LAST)
        lfh.wait()
        for k in range(LAST):
            send(k).start()
        head(fh_s)
        for k in range(LAST):
            send(k).wait_send()

    @pl.when(st < LAST)
    def _():
        pl.semaphore_wait(bar, 1)
        send(0).wait_recv()
        head(fr_s)


def tile_start(pos):
    return pl.ds(pl.multiple_of((pos // LN) * LN, LN), LN)


def copy_all(kd, vd, ko, vo, ks, vs, ksem, vsem, edit):
    ins = [(pltpu.make_async_copy(kd.at[m], ks.at[m], ksem.at[m]), pltpu.make_async_copy(vd.at[m], vs.at[m], vsem.at[m])) for m in range(NM)]
    for a, b in ins:
        a.start()
        b.start()
    outs = []
    for m in range(NM):
        for c, scr, out, sem, w in ((ins[m][0], ks, ko, ksem, 0), (ins[m][1], vs, vo, vsem, 1)):
            c.wait()
            if edit is not None:
                edit(m, scr, w)
            o = pltpu.make_async_copy(scr.at[m], out.at[m], sem.at[m])
            o.start()
            outs.append(o)
    for o in outs:
        o.wait()


def pre_kernel(kd, vd, ko, vo, tok, ks, vs, ksem, vsem):
    st = lax.axis_index('stage')

    @pl.when(st >= 2)
    def _():
        copy_all(kd, vd, ko, vo, ks, vs, ksem, vsem, None)


def load_new(srcs, dsts, sem):
    cs = [pltpu.make_async_copy(a, b, sem.at[i]) for i, (a, b) in enumerate(zip(srcs, dsts))]
    for c in cs[4:] + cs[:4]:
        c.start()
    return cs


def update_tiles(dlen, bk, bv, ko, vo, kpo, vpo, kt, vt, new, cs, ksem, vsem, nsem, extra=None):
    lane = lane_iota((HD, LN))

    def cp(hbm, scr, sem, m, i, out):
        h = hbm.at[m, i, :, :, tile_start(dlen[m, i])]
        v = scr.at[m, i]
        return pltpu.make_async_copy(v, h, sem.at[m]) if out else pltpu.make_async_copy(h, v, sem.at[m])

    cs[4].wait()
    for m in range(NM):
        for i in range(DR):
            cp(bk, kt, ksem, m, i, False).start()
            cp(bv, vt, vsem, m, i, False).start()
    if extra is not None:
        extra()
    for c in cs[:4]:
        c.wait()
    po = [pltpu.make_async_copy(new[2], kpo, nsem.at[2]), pltpu.make_async_copy(new[3], vpo, nsem.at[3])]
    for o in po:
        o.start()
    for m in range(NM):
        for hbm, scr, sem, nw in ((ko, kt, ksem, new[0]), (vo, vt, vsem, new[1])):
            for i in range(DR):
                cp(hbm, scr, sem, m, i, False).wait()
            for i in range(DR):
                pos = dlen[m, i]
                for g in range(NKV):
                    col = nw[m // 2, g * HD:(g + 1) * HD, m % 2 * DR + i:m % 2 * DR + i + 1]
                    scr[m, i, g] = jnp.where(lane == pos % LN, col, scr[m, i, g].astype(F32)).astype(BF16)
            for i in range(DR):
                cp(hbm, scr, sem, m, i, True).start()
    for m in range(NM):
        for i in range(DR):
            cp(ko, kt, ksem, m, i, True).wait()
            cp(vo, vt, vsem, m, i, True).wait()
    for o in po:
        o.wait()


def mid_kernel(dlen_h, kd, vd, bk, bv, kdn, vdn, kpn, vpn, ko, vo, kpo, vpo, tok, ks, vs, kt, vt, kn_s, vn_s, kp_s, vp_s, dlen, ksem, vsem, nsem):
    st = lax.axis_index('stage')
    new = (kn_s, vn_s, kp_s, vp_s)

    @pl.when(st < 2)
    def _():
        cs = load_new((kdn, vdn, kpn, vpn, dlen_h), new + (dlen,), nsem)
        for c in cs:
            c.wait()
        po = [pltpu.make_async_copy(kp_s, kpo, nsem.at[2]), pltpu.make_async_copy(vp_s, vpo, nsem.at[3])]
        for o in po:
            o.start()
        lane = lane_iota((HD, LN))

        def edit(m, scr, w):
            for i in range(DR):
                pos = dlen[m, i]
                sl = tile_start(pos)
                for g in range(NKV):
                    col = new[w][m // 2, g * HD:(g + 1) * HD, m % 2 * DR + i:m % 2 * DR + i + 1]
                    scr[m, i, g, :, sl] = jnp.where(lane == pos % LN, col, scr[m, i, g, :, sl].astype(F32)).astype(BF16)

        copy_all(kd, vd, ko, vo, ks, vs, ksem, vsem, edit)
        for o in po:
            o.wait()

    @pl.when(st == 2)
    def _():
        cs = load_new((kdn, vdn, kpn, vpn, dlen_h), new + (dlen,), nsem)
        update_tiles(dlen, bk, bv, ko, vo, kpo, vpo, kt, vt, new, cs, ksem, vsem, nsem)


def post_kernel(dlen_h, kdn, vdn, kpn, vpn, lg, bk, bv, bkp, bvp, ko, vo, kpo, vpo, logits,
                kt, vt, lg_s, kn_s, vn_s, kp_s, vp_s, dlen, ksem, vsem, nsem, hsem):
    st = lax.axis_index('stage')
    lf = pltpu.make_async_copy(lg, lg_s, hsem.at[0])
    lo = pltpu.make_async_copy(lg_s, logits, hsem.at[1])

    def turn():
        lf.wait()
        lo.start()

    @pl.when(st == LAST)
    def _():
        new = (kn_s, vn_s, kp_s, vp_s)
        cs = load_new((kdn, vdn, kpn, vpn, dlen_h), new + (dlen,), nsem)
        lf.start()
        update_tiles(dlen, bk, bv, ko, vo, kpo, vpo, kt, vt, new, cs, ksem, vsem, nsem, turn)

    @pl.when(st < LAST)
    def _():
        lf.start()
        turn()

    lo.wait()


ANY = pl.BlockSpec(memory_space=pltpu.HBM)


def solution(mesh):
    part = P('replica')
    layer = P('stage')
    cache = P('stage', 'replica')
    in_specs = (part,) * 4 + (layer,) * 9 + (P(), P()) + (cache,) * 4
    out_specs = (part,) + (cache,) * 4
    inv_freq = np.float32(ROPE_BASE) ** (-np.arange(HALF, dtype=np.float32) * np.float32(2.0 / HD))
    ifr_c = np.broadcast_to(inv_freq[:, None], (HALF, NP)).astype(np.float32)

    def device_fn(x_dec, x_pre, dec_len, pre_len, g_attn, w_q, w_k, w_v, w_o, g_mlp, w_gate, w_up, w_down, g_final, w_head, k_dec, v_dec, k_pre, v_pre):
        kd = jnp.transpose(k_dec[0], (0, 1, 3, 4, 2))
        vd = jnp.transpose(v_dec[0], (0, 1, 3, 4, 2))
        kp = jnp.transpose(k_pre[0], (1, 2, 0))
        vp = jnp.transpose(v_pre[0], (1, 2, 0))
        args = (x_dec.reshape(ND, HID), x_pre.reshape(NP, HID), dec_len, pre_len, g_attn, w_q[0], w_k[0].T, w_v[0].T, w_o[0], g_mlp,
                w_gate[0], w_up[0], w_down[0].T, g_final, kd, vd, kp, vp, jnp.asarray(ifr_c))
        vm = lambda shape, dt: pltpu.VMEM(shape, dt)
        scratch = [
            vm((2, CR, HID), BF16), pltpu.SMEM((NM, DR), jnp.int32), pltpu.SMEM((1,), jnp.int32), vm((1, HID), BF16),
            vm((HID, HID), BF16), vm((HID + 2 * KVW, HID), BF16), vm((HID, HID), BF16), vm((1, HID), BF16),
            vm((HID, FFN), BF16), vm((HID, FFN), BF16), vm((HID, FFN), BF16), vm((FFN, HID), BF16), vm((HID,), BF16),
            vm(kd.shape, BF16), vm(vd.shape, BF16), vm(kp.shape, BF16), vm(vp.shape, BF16), vm((HALF, 2 * LN), F32),
            vm((2, HALF, 2 * LN), F32), vm((2, HALF, 2 * LN), F32), vm((HID, LN), BF16),
            vm((2 * ES * 8, LN), F32), vm((2 * ES * 8, LN), F32), vm((2, 24, LN), F32), vm((2 * ES, KVW), F32),
            vm((2 * ES * 8, LN), F32), vm((2 * ES * 8, LN), F32),
            vm((2, KVW, LN), F32), vm((2, KVW, LN), F32), vm(((2 * DR + 2) * 24, CL), F32), vm((2, CL, 2 * LN), F32), vm((2, CL, 2 * LN), BF16),
            vm((CL, LN), F32), vm((HID, LN), F32), vm((CR, FFN), BF16), vm((2, CR, HID), BF16), vm((FR, HID), BF16),
            pltpu.SemaphoreType.DMA((19,)), pltpu.SemaphoreType.DMA((NM,)), pltpu.SemaphoreType.DMA((NM,)), pltpu.SemaphoreType.DMA((7,)),
            pltpu.SemaphoreType.DMA((2,)), pltpu.SemaphoreType.DMA((2,)),
        ]
        sds = jax.ShapeDtypeStruct
        big = pltpu.CompilerParams(vmem_limit_bytes=62 * 1024 * 1024)
        cshape = sds(kd.shape, BF16)
        pshape = sds(kp.shape, BF16)
        nsems = [pltpu.SemaphoreType.DMA((NM,)), pltpu.SemaphoreType.DMA((NM,))]
        tile = vm((NM, DR, NKV, HD, LN), BF16)
        news = [vm((2, KVW, LN), F32), vm((2, KVW, LN), F32), vm(kp.shape, BF16), vm(vp.shape, BF16), pltpu.SMEM((NM, DR), jnp.int32)]
        vmem = pl.BlockSpec(memory_space=pltpu.VMEM)
        tshape = sds((8, LN), F32)
        bk, bv, tok = pl.pallas_call(
            pre_kernel, out_shape=(cshape, cshape, tshape), in_specs=[ANY, ANY], out_specs=(ANY, ANY, ANY),
            scratch_shapes=[vm(kd.shape, BF16), vm(vd.shape, BF16)] + nsems, name='pre', compiler_params=big)(kd, vd)
        args = args + (tok,)
        kdn, vdn, kpn, vpn, fh = pl.pallas_call(
            pipe_kernel,
            out_shape=(sds((2, KVW, LN), F32), sds((2, KVW, LN), F32), pshape, pshape, sds((ND + 8, HID), BF16)),
            in_specs=[ANY] * len(args),
            out_specs=(ANY,) * 5,
            scratch_shapes=scratch,
            name='pipe',
            compiler_params=pltpu.CompilerParams(collective_id=0, has_side_effects=True, vmem_limit_bytes=62 * 1024 * 1024),
        )(*args)
        bk, bv, bkp, bvp, tok2 = pl.pallas_call(
            mid_kernel, out_shape=(cshape, cshape, pshape, pshape, tshape), in_specs=[ANY] * 9, out_specs=(ANY,) * 5,
            input_output_aliases={3: 0, 4: 1},
            scratch_shapes=[vm(kd.shape, BF16), vm(vd.shape, BF16), tile, tile] + news + nsems + [pltpu.SemaphoreType.DMA((5,))],
            name='mid', compiler_params=big)(dec_len, kd, vd, bk, bv, kdn, vdn, kpn, vpn)
        lgs = sds((DR + 1, NM, VOC), F32)
        lg = pl.pallas_call(
            head_kernel, out_shape=lgs, in_specs=[ANY] * 3, out_specs=vmem,
            scratch_shapes=[vm((FR, HID), BF16), vm((FR, HID), BF16), vm((HID, VOC), BF16),
                            pltpu.SemaphoreType.DMA((2,)), pltpu.SemaphoreType.DMA((LAST,)), pltpu.SemaphoreType.DMA],
            name='head', compiler_params=pltpu.CompilerParams(collective_id=1, has_side_effects=True))(fh, w_head, tok2)
        ko, vo, kpo, vpo, logits = pl.pallas_call(
            post_kernel, out_shape=(cshape, cshape, pshape, pshape, lgs), in_specs=[ANY] * 10,
            out_specs=(ANY,) * 5, input_output_aliases={6: 0, 7: 1, 8: 2, 9: 3},
            scratch_shapes=[tile, tile, vm((DR + 1, NM, VOC), F32)] + news + nsems + [pltpu.SemaphoreType.DMA((5,)), pltpu.SemaphoreType.DMA((2,))],
            name='post', compiler_params=big)(dec_len, kdn, vdn, kpn, vpn, lg, bk, bv, bkp, bvp)
        back = lambda a: jnp.transpose(a, (0, 1, 4, 2, 3))[None]
        backp = lambda a: jnp.transpose(a, (2, 0, 1))[None]
        return jnp.transpose(logits, (1, 0, 2)), back(ko), back(vo), backp(kpo), backp(vpo)

    return jax.shard_map(device_fn, mesh=mesh, in_specs=in_specs, out_specs=out_specs, check_vma=False)
```

```python
import functools

import jax
import jax.numpy as jnp
import numpy as np
from jax import lax
from jax.experimental import pallas as pl
from jax.experimental.pallas import tpu as pltpu
from jax.sharding import PartitionSpec as P

F32 = jnp.float32
BF16 = jnp.bfloat16
MESH = pl.DeviceIdType.MESH
NORM_EPS = 1e-6
ROPE_BASE = 10000.0
NEG = -1e30

HID = 576
NQ = 9
NKV = 3
GRP = 3
HD = 64
HALF = 32
KVW = NKV * HD
FFN = 1536
NM = 4
DR = 8
SEG = 64
CL = 512
VOC = 1024
ND = NM * DR
NP = NM * SEG
LAST = 3
LN = 128
CP = 128
CD = 16
CR = CP + CD
ES = CD + 8
FR = ND + 8
PARTS = (slice(0, 256), slice(256, HID))


def nt(a, b):
    return lax.dot_general(a, b, (((1,), (1,)), ((), ())), preferred_element_type=F32)


def nn(a, b):
    return jnp.dot(a, b, preferred_element_type=F32)


def rms(x, g):
    inv = lax.rsqrt(jnp.mean(x * x, axis=-1, keepdims=True) + NORM_EPS)
    return (x * inv * g).astype(BF16)


def rope_t(m, cos, sin):
    parts = []
    for j in range(m.shape[0] // HD):
        a = m[j * HD:j * HD + HALF]
        b = m[j * HD + HALF:(j + 1) * HD]
        parts += [a * cos - b * sin, b * cos + a * sin]
    return jnp.concatenate(parts, axis=0)


def lane_iota(shape):
    return lax.broadcasted_iota(jnp.int32, shape, len(shape) - 1)


def pipe_kernel(xd, xp, dlen, plen, ga, wq, wk, wv, wo, gm, wg, wu, wd, gf, kd, vd, kp, vp, ifr, tok,
                kdn, vdn, kpn, vpn, fh_o,
                xc_s, dl_s, pl_s, ga_s, wq_s, w3_s, wo_s, gm_s, wg_s, wu_s, wd_s, wdt_s, gf_s,
                kd_s, vd_s, kp_s, vp_s, ifr_s,
                cos_s, sin_s, qt_s, qa_s, qb_s, self_s, vn_s, oa_s, ob_s,
                kdn_s, vdn_s, sc_s, ps_s, pb_s, bias_s, ot_s, act_s, so_s, fh_s,
                in_sem, kd_sem, vd_sem, out_sem, ssem, rsem):
    st = lax.axis_index('stage')
    order = [(dlen, dl_s), (plen, pl_s), (ga, ga_s), (ifr, ifr_s), (wq, wq_s), (wk, w3_s.at[HID:HID + KVW]), (wv, w3_s.at[HID + KVW:]),
             (kp, kp_s), (vp, vp_s), (wo, wo_s), (gm, gm_s), (wg, wg_s), (wu, wu_s), (wd, wd_s), (gf, gf_s),
             (xp.at[0:CP], xc_s.at[0, 0:CP]), (xd.at[0:CD], xc_s.at[0, CP:CR]), (xp.at[CP:2 * CP], xc_s.at[1, 0:CP]), (xd.at[CD:2 * CD], xc_s.at[1, CP:CR])]
    names = ['dl', 'pl', 'ga', 'ifr', 'wq', 'wk', 'wv', 'kp', 'vp', 'wo', 'gm', 'wg', 'wu', 'wd', 'gf', 'p0', 'd0', 'p1', 'd1']
    cps = {n: pltpu.make_async_copy(a, b, in_sem.at[i]) for i, (n, (a, b)) in enumerate(zip(names, order))}
    kcp = [pltpu.make_async_copy(kd.at[m], kd_s.at[m], kd_sem.at[m]) for m in range(NM)]
    vcp = [pltpu.make_async_copy(vd.at[m], vd_s.at[m], vd_sem.at[m]) for m in range(NM)]

    def start(*ns):
        for n in ns:
            cps[n].start()

    def wait(*ns):
        for n in ns:
            cps[n].wait()

    start('dl', 'pl', 'ifr', 'ga', 'wq', 'wk', 'wv')

    @pl.when(st == 0)
    def _():
        start('p0', 'd0')

    bar = pltpu.get_barrier_semaphore()

    @pl.when(st > 0)
    def _():
        pl.semaphore_signal(bar, inc=1, device_id={'stage': jnp.maximum(st - 1, 0)}, device_id_type=MESH)

    @pl.when(st < LAST)
    def _():
        pl.semaphore_signal(bar, inc=1, device_id={'stage': jnp.minimum(st + 1, LAST)}, device_id_type=MESH)

    wait('dl', 'pl', 'ifr')
    p0 = pl_s[0]
    li = lane_iota((1, 2 * LN))
    fr = ifr_s[...]
    for c in range(2):
        pos = p0 + (c * CP) + li
        for k in range(CD):
            pos = jnp.where(li == LN + k, dl_s[2 * c + k // DR, k % DR], pos)
        for k in range(2):
            pos = jnp.where(li == LN + CD + k, p0 + (c * CP + k * SEG + SEG - 1), pos)
        ang = fr * pos.astype(F32)
        cos_s[c] = jnp.cos(ang)
        sin_s[c] = jnp.sin(ang)
    qa_s[...] = jnp.zeros_like(qa_s)
    qb_s[...] = jnp.zeros_like(qb_s)
    ob_s[...] = jnp.zeros_like(ob_s)
    for k in range(2):
        pb_s[k] = jnp.zeros((CL, 2 * LN), BF16)

    start('kp', 'vp')
    for m in range(2):
        kcp[m].start()
        vcp[m].start()
    start('wo', 'gm')
    wait('ga', 'wq')

    @pl.when(st > 0)
    def _():
        start('wg', 'wu', 'wd', 'gf')
        for m in (2, 3):
            kcp[m].start()
            vcp[m].start()

    w3_s[:HID, :] = wq_s[...].astype(F32).T.astype(BF16)
    wait('wk', 'wv')

    @pl.when(st > 0)
    def _():
        wait('wd')
        for k in range(0, FFN, LN):
            wdt_s[k:k + LN, :] = wd_s[:, k:k + LN].astype(F32).T.astype(BF16)

    gat = ga_s[...].astype(F32)

    lgrp = lane_iota((8, KVW)) // HD

    def dec_scores(e, kt, slot):
        qb = jnp.concatenate([qa_s[e * 8:e * 8 + 8, :], qb_s[e * 8:e * 8 + 8, :HD]], axis=1)
        lhs = jnp.concatenate([jnp.where(lgrp == g, qb, 0.0) for g in range(NKV)], axis=0).astype(BF16)
        sc_s[slot * 24:slot * 24 + 24, :] = nn(lhs, kt)

    def dec_mix(c, k, vt, pos, slot):
        e = c * ES + k
        selfcol = jnp.sum(jnp.where(lane_iota((24, LN)) == k, self_s[c], 0.0), axis=-1, keepdims=True)
        s = jnp.where(lane_iota((24, CL)) < pos, sc_s[slot * 24:slot * 24 + 24, :], NEG)
        mx = jnp.maximum(jnp.max(s, axis=-1, keepdims=True), selfcol)
        p = jnp.exp(s - mx)
        ps = jnp.exp(selfcol - mx)
        rl = 1.0 / (jnp.sum(p, axis=-1, keepdims=True) + ps)
        o = nt((p * rl).astype(BF16), vt)
        o = o + (ps * rl).astype(BF16).astype(F32) * vn_s[e:e + 1, :]
        acc = jnp.where(lgrp == 0, o[0:8], 0.0)
        for g in range(1, NKV):
            acc = jnp.where(lgrp == g, o[8 * g:8 * g + 8], acc)
        oa_s[e * 8:e * 8 + 8, :] = acc[:, :LN]
        ob_s[e * 8:e * 8 + 8, :HD] = acc[:, LN:]

    def dec_out(e, n):
        return jnp.concatenate([x for r in range(GRP) for x in
                                (oa_s[pl.ds(e * 8 + r, n, stride=8), :], ob_s[pl.ds(e * 8 + r, n, stride=8), :][:, :HD])], axis=1)

    def wo_perm():
        return jnp.concatenate([wo_s[(g * GRP + r) * HD:(g * GRP + r + 1) * HD, :] for r in range(GRP) for g in range(NKV)], axis=0)

    def mlp(x, rows, put):
        h2 = rms(x, gm_s[...].astype(F32))
        step = 512
        for c in range(FFN // step):
            gt = nn(h2, wg_s[:, c * step:(c + 1) * step])
            up = nn(h2, wu_s[:, c * step:(c + 1) * step])
            act_s[:rows, c * step:(c + 1) * step] = (gt * (1.0 / (1.0 + jnp.exp(-gt))) * up).astype(BF16)
        put(x, rows)

    def round32(x):
        return x.astype(BF16).astype(F32)

    def hop(c, i):
        return pltpu.make_async_remote_copy(so_s.at[c, :, PARTS[i]], xc_s.at[c, :, PARTS[i]], ssem.at[c, i], rsem.at[c, i],
                                            device_id={'stage': jnp.minimum(st + 1, LAST)}, device_id_type=MESH)

    def last_rows(x):
        return [x[k * SEG + SEG - 1:k * SEG + SEG] for k in range(2)]

    for c in range(2):
        lim = CL - CP if c == 0 else CL

        @pl.when(st == 0)
        def _():
            wait('p%d' % c, 'd%d' % c)

        @pl.when(st > 0)
        def _():
            for i in range(len(PARTS)):
                hop(c, i).wait_recv()

        if c == 0:
            wait('kp', 'vp')
        else:
            for m in (2, 3):
                kcp[m].wait()
                vcp[m].wait()
        off = p0 + c * CP
        e0 = c * ES

        def project():
            x = xc_s[c].astype(F32)
            h = x * lax.rsqrt(jnp.mean(x * x, axis=-1, keepdims=True) + NORM_EPS) * gat
            h = jnp.concatenate([h] + last_rows(h) + [jnp.zeros((2 * LN - CR - 2, HID), F32)], axis=0).astype(BF16)
            half = (HID + 2 * KVW) // 2
            qkv = jnp.concatenate([nt(w3_s[:half, :], h), nt(w3_s[half:, :], h)], axis=0)
            cos, sin = cos_s[c], sin_s[c]
            qt = round32(rope_t(qkv[:HID], cos, sin)) * (HD ** -0.5)
            kt = round32(rope_t(qkv[HID:HID + KVW], cos, sin))
            vt = round32(qkv[HID + KVW:])
            qt_s[...] = qt[:, :LN].astype(BF16)
            qe, ke, ve = qt[:, LN:], kt[:, LN:], vt[:, LN:]
            row = lax.broadcasted_iota(jnp.int32, (24, LN), 0)
            sf = jnp.zeros((24, LN), F32)
            for g in range(NKV):
                for r in range(GRP):
                    j = g * GRP + r
                    v = jnp.sum(qe[j * HD:(j + 1) * HD] * ke[g * HD:(g + 1) * HD], axis=0, keepdims=True)
                    sf = jnp.where(row == 8 * g + r, v, sf)
            self_s[c] = sf
            n = CD + 8
            pad = jnp.zeros((HD, LN), F32)
            for r in range(GRP):
                qr = [qe[(g * GRP + r) * HD:(g * GRP + r + 1) * HD] for g in range(NKV)]
                qa_s[pl.ds(e0 * 8 + r, n, stride=8), :] = jnp.concatenate(qr[:2], axis=0).T[:n]
                qb_s[pl.ds(e0 * 8 + r, n, stride=8), :] = jnp.concatenate([qr[2], pad], axis=0).T[:n]
            vn_s[e0:e0 + n, :LN] = ve[:LN].T[:n]
            vn_s[e0:e0 + n, LN:] = jnp.concatenate([ve[LN:], pad], axis=0).T[:n, :HD]
            kdn_s[c] = ke
            vdn_s[c] = ve
            pltpu.make_async_copy(kdn_s.at[c], kdn.at[c], out_sem.at[c]).start()
            pltpu.make_async_copy(vdn_s.at[c], vdn.at[c], out_sem.at[2 + c]).start()
            return kt, vt

        def put_prompt(kt, vt):
            place = jnp.where(lax.broadcasted_iota(jnp.int32, (CP, CL), 0) + off == lane_iota((CP, CL)), 1.0, 0.0).astype(BF16)
            lp = lane_iota((KVW, CL)) - off
            fresh = (lp >= 0) & (lp < CP)
            kpu = jnp.where(fresh, nn(kt[:, :LN].astype(BF16), place), kp_s[...].reshape(KVW, CL).astype(F32))
            vpu = jnp.where(fresh, nn(vt[:, :LN].astype(BF16), place), vp_s[...].reshape(KVW, CL).astype(F32))
            kp_s[...] = kpu.astype(BF16).reshape(NKV, HD, CL)
            vp_s[...] = vpu.astype(BF16).reshape(NKV, HD, CL)
            if c == 1:
                pltpu.make_async_copy(kp_s, kpn, out_sem.at[4]).start()
                pltpu.make_async_copy(vp_s, vpn, out_sem.at[5]).start()
            return kpu

        def loads():
            if c == 0:
                kcp[0].wait()

                @pl.when(st == 0)
                def _():
                    start('wg', 'wu', 'wd', 'gf')

                kcp[1].wait()
                vcp[0].wait()
                vcp[1].wait()

                @pl.when(st == 0)
                def _():
                    start('p1', 'd1')
                    kcp[2].start()
                    vcp[2].start()

                wait('wo', 'gm')

        def dqk(i):
            for k in range(DR):
                dec_scores(c * ES + i * DR + k, kd_s[2 * c + i, k].reshape(KVW, CL), i * DR + k)

        def dmix(q):
            for k in range(4 * q, 4 * q + 4):
                m, i = 2 * c + k // DR, k % DR
                dec_mix(c, k, vd_s[m, i].reshape(KVW, CL), dl_s[m, i], k)

        @pl.when(st < LAST)
        def _():
            kt, vt = project()
            loads()
            kpu = put_prompt(kt, vt)
            kfull = kpu[:, :lim].T.astype(BF16)
            bias_s[:lim, :] = jnp.where(lax.broadcasted_iota(jnp.int32, (lim, LN), 0) <= lane_iota((lim, LN)) + off, 0.0, NEG)

            def heads(t):
                return [j for j in (2 * t, 2 * t + 1) if j < NQ]

            def scores(t):
                cols = []
                for j in heads(t):
                    g = j // GRP
                    parts = [jnp.zeros((g * HD, LN), BF16)] * (g > 0) + [qt_s[j * HD:(j + 1) * HD, :]]
                    parts += [jnp.zeros(((NKV - 1 - g) * HD, LN), BF16)] * (g < NKV - 1)
                    cols.append(jnp.concatenate(parts, axis=0))
                w = len(cols) * LN
                rhs = jnp.concatenate(cols, axis=1)
                for q in range(0, lim, lim // 2):
                    ps_s[t % 2, q:q + lim // 2, :w] = nn(kfull[q:q + lim // 2], rhs)

            def fold(v, op):
                return op(v.reshape(v.shape[0] // 8, 8, v.shape[1]), axis=0)

            ck = 64

            def masked(sl, q, ln):
                v = ps_s[sl, q:q + ck, ln]
                return v if q + ck <= 64 else v + bias_s[q:q + ck, :]

            def mix(t):
                sl = t % 2
                hs = heads(t)
                for i, j in enumerate(hs):
                    ln = slice(i * LN, (i + 1) * LN)
                    mx = jnp.full((8, LN), NEG, F32)
                    for q in range(0, lim, ck):
                        mx = jnp.maximum(mx, fold(masked(sl, q, ln), jnp.max))
                    mx = jnp.max(mx, axis=0, keepdims=True)
                    sm = jnp.zeros((8, LN), F32)
                    for q in range(0, lim, ck):
                        p = jnp.exp(masked(sl, q, ln) - mx)
                        ps_s[sl, q:q + ck, ln] = p
                        sm = sm + fold(p, jnp.sum)
                    rl = 1.0 / jnp.sum(sm, axis=0, keepdims=True)
                    for q in range(0, lim, ck):
                        pb_s[sl, q:q + ck, ln] = (ps_s[sl, q:q + ck, ln] * rl).astype(BF16)
                g0, g1 = hs[0] // GRP, hs[-1] // GRP
                o = nn(vp_s[...].reshape(KVW, CL)[g0 * HD:(g1 + 1) * HD, :lim], pb_s[sl, :lim, :len(hs) * LN])
                for i, j in enumerate(hs):
                    g, r = j // GRP, j % GRP
                    d = (r * NKV + g) * HD
                    ot_s[d:d + HD, :] = o[(g - g0) * HD:(g - g0 + 1) * HD, i * LN:(i + 1) * LN]

            dqk(0)
            scores(0)
            scores(1)
            dmix(0)
            mix(0)
            scores(2)
            dmix(1)
            mix(1)
            dqk(1)
            scores(3)
            dmix(2)
            mix(2)
            scores(4)
            dmix(3)
            mix(3)
            mix(4)
            a = jnp.concatenate([ot_s[...].T, dec_out(e0, CD)], axis=0).astype(BF16)
            x1 = round32(xc_s[c].astype(F32) + nn(a, wo_perm()))
            if c == 0:
                wait('wg', 'wu')

                @pl.when(st == 0)
                def _():
                    wait('wd')
                    kcp[3].start()
                    vcp[3].start()
                    pl.semaphore_wait(bar, 1)

                @pl.when(st > 0)
                def _():
                    pl.semaphore_wait(bar, 2)

            def put(x, rows):
                @pl.when(st == 0)
                def _():
                    for i, w in enumerate(PARTS):
                        so_s[c, :, w] = (x[:, w] + nt(act_s[...], wd_s[w, :])).astype(BF16)
                        hop(c, i).start()

                @pl.when(st > 0)
                def _():
                    for i, w in enumerate(PARTS):
                        so_s[c, :, w] = (x[:, w] + nn(act_s[...], wdt_s[:, w])).astype(BF16)
                        hop(c, i).start()

            mlp(x1, CR, put)

        @pl.when(st == LAST)
        def _():
            kt, vt = project()
            loads()
            put_prompt(kt, vt)
            for k in range(2):
                dec_scores(e0 + CD + k, kp_s[...].reshape(KVW, CL), 2 * DR + k)
            dqk(0)
            dqk(1)
            for k in range(2):
                dec_mix(c, CD + k, vp_s[...].reshape(KVW, CL), off + k * SEG + SEG - 1, 2 * DR + k)
            for q in range(4):
                dmix(q)
            if c == 0:
                wait('wg', 'wu', 'gf')
                pl.semaphore_wait(bar, 1)
            else:
                ls = [dec_out(k * ES + CD, 8)[:2] for k in range(2)]
                a = jnp.concatenate([dec_out(0, CD), dec_out(ES, CD)] + ls + [jnp.zeros((4, HID), F32)], axis=0).astype(BF16)
                xs = [xc_s[k].astype(F32) for k in range(2)]
                xf = jnp.concatenate([xs[0][CP:], xs[1][CP:]] + last_rows(xs[0]) + last_rows(xs[1]) + [jnp.zeros((4, HID), F32)], axis=0)

                def put(x, rows):
                    x2 = round32(x + nn(act_s[:rows, :], wdt_s[...]))
                    fh = rms(x2, gf_s[...].astype(F32).reshape(1, HID))
                    ri = lax.broadcasted_iota(jnp.int32, (FR, FR), 0)
                    src = jnp.where(ri < ND, (ri % NM) * DR + ri // NM, ri)
                    fh_s[...] = nn(jnp.where(lane_iota((FR, FR)) == src, 1.0, 0.0).astype(BF16), fh).astype(BF16)

                mlp(round32(xf + nn(a, wo_perm())), FR, put)
                ofh = pltpu.make_async_copy(fh_s, fh_o, out_sem.at[6])
                ofh.start()
                ofh.wait()

    for c in range(2):
        pltpu.make_async_copy(kdn_s.at[c], kdn.at[c], out_sem.at[c]).wait()
        pltpu.make_async_copy(vdn_s.at[c], vdn.at[c], out_sem.at[2 + c]).wait()
    pltpu.make_async_copy(kp_s, kpn, out_sem.at[4]).wait()
    pltpu.make_async_copy(vp_s, vpn, out_sem.at[5]).wait()

    @pl.when(st < LAST)
    def _():
        wait('gf')
        for c in range(2):
            for i in range(len(PARTS)):
                hop(c, i).wait_send()


def head_kernel(fh, wh, tok, logits, fh_s, fr_s, wh_s, lsem, ssem, rsem):
    st = lax.axis_index('stage')
    lfh = pltpu.make_async_copy(fh, fh_s, lsem.at[0])
    lwh = pltpu.make_async_copy(wh, wh_s, lsem.at[1])

    @pl.when(st == LAST)
    def _():
        lfh.start()

    lwh.start()
    bar = pltpu.get_barrier_semaphore()

    def send(k):
        return pltpu.make_async_remote_copy(fh_s, fr_s, ssem.at[k], rsem, device_id={'stage': k}, device_id_type=MESH)

    def head(ref):
        lwh.wait()
        lg = nn(ref[...], wh_s[...])
        for i in range(DR + 1):
            logits[i] = lg[i * NM:(i + 1) * NM]

    @pl.when(st < LAST)
    def _():
        pl.semaphore_signal(bar, inc=1, device_id={'stage': LAST}, device_id_type=MESH)

    @pl.when(st == LAST)
    def _():
        for k in range(LAST):
            pl.semaphore_signal(bar, inc=1, device_id={'stage': k}, device_id_type=MESH)
        pl.semaphore_wait(bar, LAST)
        lfh.wait()
        for k in range(LAST):
            send(k).start()
        head(fh_s)
        for k in range(LAST):
            send(k).wait_send()

    @pl.when(st < LAST)
    def _():
        pl.semaphore_wait(bar, 1)
        send(0).wait_recv()
        head(fr_s)


def tile_start(pos):
    return pl.ds(pl.multiple_of((pos // LN) * LN, LN), LN)


def copy_all(kd, vd, ko, vo, ks, vs, ksem, vsem, edit):
    ins = [(pltpu.make_async_copy(kd.at[m], ks.at[m], ksem.at[m]), pltpu.make_async_copy(vd.at[m], vs.at[m], vsem.at[m])) for m in range(NM)]
    for a, b in ins:
        a.start()
        b.start()
    outs = []
    for m in range(NM):
        for c, scr, out, sem, w in ((ins[m][0], ks, ko, ksem, 0), (ins[m][1], vs, vo, vsem, 1)):
            c.wait()
            if edit is not None:
                edit(m, scr, w)
            o = pltpu.make_async_copy(scr.at[m], out.at[m], sem.at[m])
            o.start()
            outs.append(o)
    for o in outs:
        o.wait()


def pre_kernel(kd, vd, ko, vo, tok, ks, vs, ksem, vsem):
    st = lax.axis_index('stage')

    @pl.when(st >= 2)
    def _():
        copy_all(kd, vd, ko, vo, ks, vs, ksem, vsem, None)


def load_new(srcs, dsts, sem):
    cs = [pltpu.make_async_copy(a, b, sem.at[i]) for i, (a, b) in enumerate(zip(srcs, dsts))]
    for c in cs[4:] + cs[:4]:
        c.start()
    return cs


def update_tiles(dlen, bk, bv, ko, vo, kpo, vpo, kt, vt, new, cs, ksem, vsem, nsem, extra=None):
    lane = lane_iota((HD, LN))

    def cp(hbm, scr, sem, m, i, out):
        h = hbm.at[m, i, :, :, tile_start(dlen[m, i])]
        v = scr.at[m, i]
        return pltpu.make_async_copy(v, h, sem.at[m]) if out else pltpu.make_async_copy(h, v, sem.at[m])

    cs[4].wait()
    for m in range(NM):
        for i in range(DR):
            cp(bk, kt, ksem, m, i, False).start()
            cp(bv, vt, vsem, m, i, False).start()
    if extra is not None:
        extra()
    for c in cs[:4]:
        c.wait()
    po = [pltpu.make_async_copy(new[2], kpo, nsem.at[2]), pltpu.make_async_copy(new[3], vpo, nsem.at[3])]
    for o in po:
        o.start()
    for m in range(NM):
        for hbm, scr, sem, nw in ((ko, kt, ksem, new[0]), (vo, vt, vsem, new[1])):
            for i in range(DR):
                cp(hbm, scr, sem, m, i, False).wait()
            for i in range(DR):
                pos = dlen[m, i]
                for g in range(NKV):
                    col = nw[m // 2, g * HD:(g + 1) * HD, m % 2 * DR + i:m % 2 * DR + i + 1]
                    scr[m, i, g] = jnp.where(lane == pos % LN, col, scr[m, i, g].astype(F32)).astype(BF16)
            for i in range(DR):
                cp(hbm, scr, sem, m, i, True).start()
    for m in range(NM):
        for i in range(DR):
            cp(ko, kt, ksem, m, i, True).wait()
            cp(vo, vt, vsem, m, i, True).wait()
    for o in po:
        o.wait()


def mid_kernel(dlen_h, kd, vd, bk, bv, kdn, vdn, kpn, vpn, ko, vo, kpo, vpo, tok, ks, vs, kt, vt, kn_s, vn_s, kp_s, vp_s, dlen, ksem, vsem, nsem):
    st = lax.axis_index('stage')
    new = (kn_s, vn_s, kp_s, vp_s)

    @pl.when(st < 2)
    def _():
        cs = load_new((kdn, vdn, kpn, vpn, dlen_h), new + (dlen,), nsem)
        for c in cs:
            c.wait()
        po = [pltpu.make_async_copy(kp_s, kpo, nsem.at[2]), pltpu.make_async_copy(vp_s, vpo, nsem.at[3])]
        for o in po:
            o.start()
        lane = lane_iota((HD, LN))

        def edit(m, scr, w):
            for i in range(DR):
                pos = dlen[m, i]
                sl = tile_start(pos)
                for g in range(NKV):
                    col = new[w][m // 2, g * HD:(g + 1) * HD, m % 2 * DR + i:m % 2 * DR + i + 1]
                    scr[m, i, g, :, sl] = jnp.where(lane == pos % LN, col, scr[m, i, g, :, sl].astype(F32)).astype(BF16)

        copy_all(kd, vd, ko, vo, ks, vs, ksem, vsem, edit)
        for o in po:
            o.wait()

    @pl.when(st == 2)
    def _():
        cs = load_new((kdn, vdn, kpn, vpn, dlen_h), new + (dlen,), nsem)
        update_tiles(dlen, bk, bv, ko, vo, kpo, vpo, kt, vt, new, cs, ksem, vsem, nsem)


def post_kernel(dlen_h, kdn, vdn, kpn, vpn, lg, bk, bv, bkp, bvp, ko, vo, kpo, vpo, logits,
                kt, vt, lg_s, kn_s, vn_s, kp_s, vp_s, dlen, ksem, vsem, nsem, hsem):
    st = lax.axis_index('stage')
    lf = pltpu.make_async_copy(lg, lg_s, hsem.at[0])
    lo = pltpu.make_async_copy(lg_s, logits, hsem.at[1])

    def turn():
        lf.wait()
        lo.start()

    @pl.when(st == LAST)
    def _():
        new = (kn_s, vn_s, kp_s, vp_s)
        cs = load_new((kdn, vdn, kpn, vpn, dlen_h), new + (dlen,), nsem)
        lf.start()
        update_tiles(dlen, bk, bv, ko, vo, kpo, vpo, kt, vt, new, cs, ksem, vsem, nsem, turn)

    @pl.when(st < LAST)
    def _():
        lf.start()
        turn()

    lo.wait()


ANY = pl.BlockSpec(memory_space=pltpu.HBM)


def solution(mesh):
    part = P('replica')
    layer = P('stage')
    cache = P('stage', 'replica')
    in_specs = (part,) * 4 + (layer,) * 9 + (P(), P()) + (cache,) * 4
    out_specs = (part,) + (cache,) * 4
    inv_freq = np.float32(ROPE_BASE) ** (-np.arange(HALF, dtype=np.float32) * np.float32(2.0 / HD))
    ifr_c = np.broadcast_to(inv_freq[:, None], (HALF, NP)).astype(np.float32)

    def device_fn(x_dec, x_pre, dec_len, pre_len, g_attn, w_q, w_k, w_v, w_o, g_mlp, w_gate, w_up, w_down, g_final, w_head, k_dec, v_dec, k_pre, v_pre):
        kd = jnp.transpose(k_dec[0], (0, 1, 3, 4, 2))
        vd = jnp.transpose(v_dec[0], (0, 1, 3, 4, 2))
        kp = jnp.transpose(k_pre[0], (1, 2, 0))
        vp = jnp.transpose(v_pre[0], (1, 2, 0))
        args = (x_dec.reshape(ND, HID), x_pre.reshape(NP, HID), dec_len, pre_len, g_attn, w_q[0], w_k[0].T, w_v[0].T, w_o[0], g_mlp,
                w_gate[0], w_up[0], w_down[0].T, g_final, kd, vd, kp, vp, jnp.asarray(ifr_c))
        vm = lambda shape, dt: pltpu.VMEM(shape, dt)
        scratch = [
            vm((2, CR, HID), BF16), pltpu.SMEM((NM, DR), jnp.int32), pltpu.SMEM((1,), jnp.int32), vm((1, HID), BF16),
            vm((HID, HID), BF16), vm((HID + 2 * KVW, HID), BF16), vm((HID, HID), BF16), vm((1, HID), BF16),
            vm((HID, FFN), BF16), vm((HID, FFN), BF16), vm((HID, FFN), BF16), vm((FFN, HID), BF16), vm((HID,), BF16),
            vm(kd.shape, BF16), vm(vd.shape, BF16), vm(kp.shape, BF16), vm(vp.shape, BF16), vm((HALF, 2 * LN), F32),
            vm((2, HALF, 2 * LN), F32), vm((2, HALF, 2 * LN), F32), vm((HID, LN), BF16),
            vm((2 * ES * 8, LN), F32), vm((2 * ES * 8, LN), F32), vm((2, 24, LN), F32), vm((2 * ES, KVW), F32),
            vm((2 * ES * 8, LN), F32), vm((2 * ES * 8, LN), F32),
            vm((2, KVW, LN), F32), vm((2, KVW, LN), F32), vm(((2 * DR + 2) * 24, CL), F32), vm((2, CL, 2 * LN), F32), vm((2, CL, 2 * LN), BF16),
            vm((CL, LN), F32), vm((HID, LN), F32), vm((CR, FFN), BF16), vm((2, CR, HID), BF16), vm((FR, HID), BF16),
            pltpu.SemaphoreType.DMA((19,)), pltpu.SemaphoreType.DMA((NM,)), pltpu.SemaphoreType.DMA((NM,)), pltpu.SemaphoreType.DMA((7,)),
            pltpu.SemaphoreType.DMA((2, 2)), pltpu.SemaphoreType.DMA((2, 2)),
        ]
        sds = jax.ShapeDtypeStruct
        big = pltpu.CompilerParams(vmem_limit_bytes=62 * 1024 * 1024)
        cshape = sds(kd.shape, BF16)
        pshape = sds(kp.shape, BF16)
        nsems = [pltpu.SemaphoreType.DMA((NM,)), pltpu.SemaphoreType.DMA((NM,))]
        tile = vm((NM, DR, NKV, HD, LN), BF16)
        news = [vm((2, KVW, LN), F32), vm((2, KVW, LN), F32), vm(kp.shape, BF16), vm(vp.shape, BF16), pltpu.SMEM((NM, DR), jnp.int32)]
        vmem = pl.BlockSpec(memory_space=pltpu.VMEM)
        tshape = sds((8, LN), F32)
        bk, bv, tok = pl.pallas_call(
            pre_kernel, out_shape=(cshape, cshape, tshape), in_specs=[ANY, ANY], out_specs=(ANY, ANY, ANY),
            scratch_shapes=[vm(kd.shape, BF16), vm(vd.shape, BF16)] + nsems, name='pre', compiler_params=big)(kd, vd)
        args = args + (tok,)
        kdn, vdn, kpn, vpn, fh = pl.pallas_call(
            pipe_kernel,
            out_shape=(sds((2, KVW, LN), F32), sds((2, KVW, LN), F32), pshape, pshape, sds((ND + 8, HID), BF16)),
            in_specs=[ANY] * len(args),
            out_specs=(ANY,) * 5,
            scratch_shapes=scratch,
            name='pipe',
            compiler_params=pltpu.CompilerParams(collective_id=0, has_side_effects=True, vmem_limit_bytes=62 * 1024 * 1024),
        )(*args)
        bk, bv, bkp, bvp, tok2 = pl.pallas_call(
            mid_kernel, out_shape=(cshape, cshape, pshape, pshape, tshape), in_specs=[ANY] * 9, out_specs=(ANY,) * 5,
            input_output_aliases={3: 0, 4: 1},
            scratch_shapes=[vm(kd.shape, BF16), vm(vd.shape, BF16), tile, tile] + news + nsems + [pltpu.SemaphoreType.DMA((5,))],
            name='mid', compiler_params=big)(dec_len, kd, vd, bk, bv, kdn, vdn, kpn, vpn)
        lgs = sds((DR + 1, NM, VOC), F32)
        lg = pl.pallas_call(
            head_kernel, out_shape=lgs, in_specs=[ANY] * 3, out_specs=vmem,
            scratch_shapes=[vm((FR, HID), BF16), vm((FR, HID), BF16), vm((HID, VOC), BF16),
                            pltpu.SemaphoreType.DMA((2,)), pltpu.SemaphoreType.DMA((LAST,)), pltpu.SemaphoreType.DMA],
            name='head', compiler_params=pltpu.CompilerParams(collective_id=1, has_side_effects=True))(fh, w_head, tok2)
        ko, vo, kpo, vpo, logits = pl.pallas_call(
            post_kernel, out_shape=(cshape, cshape, pshape, pshape, lgs), in_specs=[ANY] * 10,
            out_specs=(ANY,) * 5, input_output_aliases={6: 0, 7: 1, 8: 2, 9: 3},
            scratch_shapes=[tile, tile, vm((DR + 1, NM, VOC), F32)] + news + nsems + [pltpu.SemaphoreType.DMA((5,)), pltpu.SemaphoreType.DMA((2,))],
            name='post', compiler_params=big)(dec_len, kdn, vdn, kpn, vpn, lg, bk, bv, bkp, bvp)
        back = lambda a: jnp.transpose(a, (0, 1, 4, 2, 3))[None]
        backp = lambda a: jnp.transpose(a, (2, 0, 1))[None]
        return jnp.transpose(logits, (1, 0, 2)), back(ko), back(vo), backp(kpo), backp(vpo)

    return jax.shard_map(device_fn, mesh=mesh, in_specs=in_specs, out_specs=out_specs, check_vma=False)
```

```python
import functools

import jax
import jax.numpy as jnp
import numpy as np
from jax import lax
from jax.experimental import pallas as pl
from jax.experimental.pallas import tpu as pltpu
from jax.sharding import PartitionSpec as P

F32 = jnp.float32
BF16 = jnp.bfloat16
MESH = pl.DeviceIdType.MESH
NORM_EPS = 1e-6
ROPE_BASE = 10000.0
NEG = -1e30

HID = 576
NQ = 9
NKV = 3
GRP = 3
HD = 64
HALF = 32
KVW = NKV * HD
FFN = 1536
NM = 4
DR = 8
SEG = 64
CL = 512
VOC = 1024
ND = NM * DR
NP = NM * SEG
LAST = 3
LN = 128
CP = 128
CD = 16
CR = CP + CD
ES = CD + 8
FR = ND + 8


def nt(a, b):
    return lax.dot_general(a, b, (((1,), (1,)), ((), ())), preferred_element_type=F32)


def nn(a, b):
    return jnp.dot(a, b, preferred_element_type=F32)


def rms(x, g):
    inv = lax.rsqrt(jnp.mean(x * x, axis=-1, keepdims=True) + NORM_EPS)
    return (x * inv * g).astype(BF16)


def rope_t(m, cos, sin):
    parts = []
    for j in range(m.shape[0] // HD):
        a = m[j * HD:j * HD + HALF]
        b = m[j * HD + HALF:(j + 1) * HD]
        parts += [a * cos - b * sin, b * cos + a * sin]
    return jnp.concatenate(parts, axis=0)


def lane_iota(shape):
    return lax.broadcasted_iota(jnp.int32, shape, len(shape) - 1)


def pipe_kernel(xd, xp, dlen, plen, ga, wq, wk, wv, wo, gm, wg, wu, wd, gf, kd, vd, kp, vp, ifr, tok,
                kdn, vdn, kpn, vpn, fh_o,
                xc_s, dl_s, pl_s, ga_s, wq_s, w3_s, wo_s, gm_s, wg_s, wu_s, wd_s, wdt_s, gf_s,
                kd_s, vd_s, kp_s, vp_s, ifr_s,
                cos_s, sin_s, qt_s, qa_s, qb_s, self_s, vn_s, oa_s, ob_s,
                kdn_s, vdn_s, sc_s, ps_s, pb_s, bias_s, ot_s, act_s, so_s, fh_s,
                in_sem, kd_sem, vd_sem, out_sem, ssem, rsem):
    st = lax.axis_index('stage')
    order = [(dlen, dl_s), (plen, pl_s), (ga, ga_s), (ifr, ifr_s), (wq, wq_s), (wk, w3_s.at[HID:HID + KVW]), (wv, w3_s.at[HID + KVW:]),
             (kp, kp_s), (vp, vp_s), (wo, wo_s), (gm, gm_s), (wg, wg_s), (wu, wu_s), (wd, wd_s), (gf, gf_s),
             (xp.at[0:CP], xc_s.at[0, 0:CP]), (xd.at[0:CD], xc_s.at[0, CP:CR]), (xp.at[CP:2 * CP], xc_s.at[1, 0:CP]), (xd.at[CD:2 * CD], xc_s.at[1, CP:CR])]
    names = ['dl', 'pl', 'ga', 'ifr', 'wq', 'wk', 'wv', 'kp', 'vp', 'wo', 'gm', 'wg', 'wu', 'wd', 'gf', 'p0', 'd0', 'p1', 'd1']
    cps = {n: pltpu.make_async_copy(a, b, in_sem.at[i]) for i, (n, (a, b)) in enumerate(zip(names, order))}
    kcp = [pltpu.make_async_copy(kd.at[m], kd_s.at[m], kd_sem.at[m]) for m in range(NM)]
    vcp = [pltpu.make_async_copy(vd.at[m], vd_s.at[m], vd_sem.at[m]) for m in range(NM)]

    def start(*ns):
        for n in ns:
            cps[n].start()

    def wait(*ns):
        for n in ns:
            cps[n].wait()

    start('dl', 'pl', 'ifr', 'ga', 'wq', 'wk', 'wv')

    @pl.when(st == 0)
    def _():
        start('p0', 'd0')

    bar = pltpu.get_barrier_semaphore()

    @pl.when(st > 0)
    def _():
        pl.semaphore_signal(bar, inc=1, device_id={'stage': jnp.maximum(st - 1, 0)}, device_id_type=MESH)

    @pl.when(st < LAST)
    def _():
        pl.semaphore_signal(bar, inc=1, device_id={'stage': jnp.minimum(st + 1, LAST)}, device_id_type=MESH)

    wait('dl', 'pl', 'ifr')
    p0 = pl_s[0]
    li = lane_iota((1, 2 * LN))
    fr = ifr_s[...]
    for c in range(2):
        pos = p0 + (c * CP) + li
        for k in range(CD):
            pos = jnp.where(li == LN + k, dl_s[2 * c + k // DR, k % DR], pos)
        for k in range(2):
            pos = jnp.where(li == LN + CD + k, p0 + (c * CP + k * SEG + SEG - 1), pos)
        ang = fr * pos.astype(F32)
        cos_s[c] = jnp.cos(ang)
        sin_s[c] = jnp.sin(ang)
    qa_s[...] = jnp.zeros_like(qa_s)
    qb_s[...] = jnp.zeros_like(qb_s)
    ob_s[...] = jnp.zeros_like(ob_s)
    for k in range(2):
        pb_s[k] = jnp.zeros((CL, 2 * LN), BF16)

    start('kp', 'vp')
    for m in range(2):
        kcp[m].start()
        vcp[m].start()
    start('wo', 'gm')

    @pl.when(st > 0)
    def _():
        start('wg', 'wu', 'wd', 'gf')

    wait('ga', 'wq')
    w3_s[:HID, :] = wq_s[...].astype(F32).T.astype(BF16)
    wait('wk', 'wv')

    @pl.when(st > 0)
    def _():
        wait('wd')
        for k in range(0, FFN, LN):
            wdt_s[k:k + LN, :] = wd_s[:, k:k + LN].astype(F32).T.astype(BF16)

    gat = ga_s[...].astype(F32)

    lgrp = lane_iota((8, KVW)) // HD

    def dec_scores(e, kt, slot):
        qb = jnp.concatenate([qa_s[e * 8:e * 8 + 8, :], qb_s[e * 8:e * 8 + 8, :HD]], axis=1)
        lhs = jnp.concatenate([jnp.where(lgrp == g, qb, 0.0) for g in range(NKV)], axis=0).astype(BF16)
        sc_s[slot * 24:slot * 24 + 24, :] = nn(lhs, kt)

    def dec_mix(c, k, vt, pos, slot):
        e = c * ES + k
        selfcol = jnp.sum(jnp.where(lane_iota((24, LN)) == k, self_s[c], 0.0), axis=-1, keepdims=True)
        s = jnp.where(lane_iota((24, CL)) < pos, sc_s[slot * 24:slot * 24 + 24, :], NEG)
        mx = jnp.maximum(jnp.max(s, axis=-1, keepdims=True), selfcol)
        p = jnp.exp(s - mx)
        ps = jnp.exp(selfcol - mx)
        rl = 1.0 / (jnp.sum(p, axis=-1, keepdims=True) + ps)
        o = nt((p * rl).astype(BF16), vt)
        o = o + (ps * rl).astype(BF16).astype(F32) * vn_s[e:e + 1, :]
        acc = jnp.where(lgrp == 0, o[0:8], 0.0)
        for g in range(1, NKV):
            acc = jnp.where(lgrp == g, o[8 * g:8 * g + 8], acc)
        oa_s[e * 8:e * 8 + 8, :] = acc[:, :LN]
        ob_s[e * 8:e * 8 + 8, :HD] = acc[:, LN:]

    def dec_out(e, n):
        return jnp.concatenate([x for r in range(GRP) for x in
                                (oa_s[pl.ds(e * 8 + r, n, stride=8), :], ob_s[pl.ds(e * 8 + r, n, stride=8), :][:, :HD])], axis=1)

    def wo_perm():
        return jnp.concatenate([wo_s[(g * GRP + r) * HD:(g * GRP + r + 1) * HD, :] for r in range(GRP) for g in range(NKV)], axis=0)

    def mlp(x, rows, put):
        h2 = rms(x, gm_s[...].astype(F32))
        step = 512
        for c in range(FFN // step):
            gt = nn(h2, wg_s[:, c * step:(c + 1) * step])
            up = nn(h2, wu_s[:, c * step:(c + 1) * step])
            act_s[:rows, c * step:(c + 1) * step] = (gt * (1.0 / (1.0 + jnp.exp(-gt))) * up).astype(BF16)
        put(x, rows)

    def round32(x):
        return x.astype(BF16).astype(F32)

    def hop(c):
        return pltpu.make_async_remote_copy(so_s.at[c], xc_s.at[c], ssem.at[c], rsem.at[c],
                                            device_id={'stage': jnp.minimum(st + 1, LAST)}, device_id_type=MESH)

    def last_rows(x):
        return [x[k * SEG + SEG - 1:k * SEG + SEG] for k in range(2)]

    for c in range(2):
        lim = CL - CP if c == 0 else CL

        @pl.when(st == 0)
        def _():
            wait('p%d' % c, 'd%d' % c)

        @pl.when(st > 0)
        def _():
            hop(c).wait_recv()

        if c == 0:
            wait('kp', 'vp')

            @pl.when(st == 0)
            def _():
                start('wg', 'wu', 'wd', 'gf')
        else:
            for m in (2, 3):
                kcp[m].wait()
                vcp[m].wait()
        off = p0 + c * CP
        e0 = c * ES

        def project():
            x = xc_s[c].astype(F32)
            h = x * lax.rsqrt(jnp.mean(x * x, axis=-1, keepdims=True) + NORM_EPS) * gat
            h = jnp.concatenate([h] + last_rows(h) + [jnp.zeros((2 * LN - CR - 2, HID), F32)], axis=0).astype(BF16)
            half = (HID + 2 * KVW) // 2
            qkv = jnp.concatenate([nt(w3_s[:half, :], h), nt(w3_s[half:, :], h)], axis=0)
            cos, sin = cos_s[c], sin_s[c]
            qt = round32(rope_t(qkv[:HID], cos, sin)) * (HD ** -0.5)
            kt = round32(rope_t(qkv[HID:HID + KVW], cos, sin))
            vt = round32(qkv[HID + KVW:])
            qt_s[...] = qt[:, :LN].astype(BF16)
            qe, ke, ve = qt[:, LN:], kt[:, LN:], vt[:, LN:]
            row = lax.broadcasted_iota(jnp.int32, (24, LN), 0)
            sf = jnp.zeros((24, LN), F32)
            for g in range(NKV):
                for r in range(GRP):
                    j = g * GRP + r
                    v = jnp.sum(qe[j * HD:(j + 1) * HD] * ke[g * HD:(g + 1) * HD], axis=0, keepdims=True)
                    sf = jnp.where(row == 8 * g + r, v, sf)
            self_s[c] = sf
            n = CD + 8
            pad = jnp.zeros((HD, LN), F32)
            for r in range(GRP):
                qr = [qe[(g * GRP + r) * HD:(g * GRP + r + 1) * HD] for g in range(NKV)]
                qa_s[pl.ds(e0 * 8 + r, n, stride=8), :] = jnp.concatenate(qr[:2], axis=0).T[:n]
                qb_s[pl.ds(e0 * 8 + r, n, stride=8), :] = jnp.concatenate([qr[2], pad], axis=0).T[:n]
            vn_s[e0:e0 + n, :LN] = ve[:LN].T[:n]
            vn_s[e0:e0 + n, LN:] = jnp.concatenate([ve[LN:], pad], axis=0).T[:n, :HD]
            kdn_s[c] = ke
            vdn_s[c] = ve
            pltpu.make_async_copy(kdn_s.at[c], kdn.at[c], out_sem.at[c]).start()
            pltpu.make_async_copy(vdn_s.at[c], vdn.at[c], out_sem.at[2 + c]).start()
            return kt, vt

        def put_prompt(kt, vt):
            place = jnp.where(lax.broadcasted_iota(jnp.int32, (CP, CL), 0) + off == lane_iota((CP, CL)), 1.0, 0.0).astype(BF16)
            lp = lane_iota((KVW, CL)) - off
            fresh = (lp >= 0) & (lp < CP)
            kpu = jnp.where(fresh, nn(kt[:, :LN].astype(BF16), place), kp_s[...].reshape(KVW, CL).astype(F32))
            vpu = jnp.where(fresh, nn(vt[:, :LN].astype(BF16), place), vp_s[...].reshape(KVW, CL).astype(F32))
            kp_s[...] = kpu.astype(BF16).reshape(NKV, HD, CL)
            vp_s[...] = vpu.astype(BF16).reshape(NKV, HD, CL)
            if c == 1:
                pltpu.make_async_copy(kp_s, kpn, out_sem.at[4]).start()
                pltpu.make_async_copy(vp_s, vpn, out_sem.at[5]).start()
            return kpu

        def loads():
            if c == 0:
                for m in (0, 1):
                    kcp[m].wait()
                    vcp[m].wait()

                @pl.when(st == 0)
                def _():
                    start('p1', 'd1')
                for m in (2, 3):
                    kcp[m].start()
                    vcp[m].start()
                wait('wo', 'gm')

        def dqk(i):
            for k in range(DR):
                dec_scores(c * ES + i * DR + k, kd_s[2 * c + i, k].reshape(KVW, CL), i * DR + k)

        def dmix(q):
            for k in range(4 * q, 4 * q + 4):
                m, i = 2 * c + k // DR, k % DR
                dec_mix(c, k, vd_s[m, i].reshape(KVW, CL), dl_s[m, i], k)

        @pl.when(st < LAST)
        def _():
            kt, vt = project()
            loads()
            kpu = put_prompt(kt, vt)
            kfull = kpu[:, :lim].T.astype(BF16)
            bias_s[:lim, :] = jnp.where(lax.broadcasted_iota(jnp.int32, (lim, LN), 0) <= lane_iota((lim, LN)) + off, 0.0, NEG)

            def heads(t):
                return [j for j in (2 * t, 2 * t + 1) if j < NQ]

            def scores(t):
                cols = []
                for j in heads(t):
                    g = j // GRP
                    parts = [jnp.zeros((g * HD, LN), BF16)] * (g > 0) + [qt_s[j * HD:(j + 1) * HD, :]]
                    parts += [jnp.zeros(((NKV - 1 - g) * HD, LN), BF16)] * (g < NKV - 1)
                    cols.append(jnp.concatenate(parts, axis=0))
                w = len(cols) * LN
                rhs = jnp.concatenate(cols, axis=1)
                for q in range(0, lim, lim // 2):
                    ps_s[t % 2, q:q + lim // 2, :w] = nn(kfull[q:q + lim // 2], rhs)

            def fold(v, op):
                return op(v.reshape(v.shape[0] // 8, 8, v.shape[1]), axis=0)

            ck = 64

            def masked(sl, q, ln):
                v = ps_s[sl, q:q + ck, ln]
                return v if q + ck <= 64 else v + bias_s[q:q + ck, :]

            def mix(t):
                sl = t % 2
                hs = heads(t)
                for i, j in enumerate(hs):
                    ln = slice(i * LN, (i + 1) * LN)
                    mx = jnp.full((8, LN), NEG, F32)
                    for q in range(0, lim, ck):
                        mx = jnp.maximum(mx, fold(masked(sl, q, ln), jnp.max))
                    mx = jnp.max(mx, axis=0, keepdims=True)
                    sm = jnp.zeros((8, LN), F32)
                    for q in range(0, lim, ck):
                        p = jnp.exp(masked(sl, q, ln) - mx)
                        ps_s[sl, q:q + ck, ln] = p
                        sm = sm + fold(p, jnp.sum)
                    rl = 1.0 / jnp.sum(sm, axis=0, keepdims=True)
                    for q in range(0, lim, ck):
                        pb_s[sl, q:q + ck, ln] = (ps_s[sl, q:q + ck, ln] * rl).astype(BF16)
                g0, g1 = hs[0] // GRP, hs[-1] // GRP
                o = nn(vp_s[...].reshape(KVW, CL)[g0 * HD:(g1 + 1) * HD, :lim], pb_s[sl, :lim, :len(hs) * LN])
                for i, j in enumerate(hs):
                    g, r = j // GRP, j % GRP
                    d = (r * NKV + g) * HD
                    ot_s[d:d + HD, :] = o[(g - g0) * HD:(g - g0 + 1) * HD, i * LN:(i + 1) * LN]

            dqk(0)
            scores(0)
            scores(1)
            dmix(0)
            mix(0)
            scores(2)
            dmix(1)
            mix(1)
            dqk(1)
            scores(3)
            dmix(2)
            mix(2)
            scores(4)
            dmix(3)
            mix(3)
            mix(4)
            a = jnp.concatenate([ot_s[...].T, dec_out(e0, CD)], axis=0).astype(BF16)
            x1 = round32(xc_s[c].astype(F32) + nn(a, wo_perm()))
            if c == 0:
                wait('wg', 'wu')

                @pl.when(st == 0)
                def _():
                    wait('wd')

            def put(x, rows):
                @pl.when(st == 0)
                def _():
                    so_s[c] = (x + nt(act_s[...], wd_s[...])).astype(BF16)

                @pl.when(st > 0)
                def _():
                    so_s[c] = (x + nn(act_s[...], wdt_s[...])).astype(BF16)

            mlp(x1, CR, put)
            if c == 0:
                @pl.when(st == 0)
                def _():
                    pl.semaphore_wait(bar, 1)

                @pl.when(st > 0)
                def _():
                    pl.semaphore_wait(bar, 2)
            hop(c).start()

        @pl.when(st == LAST)
        def _():
            kt, vt = project()
            loads()
            put_prompt(kt, vt)
            for k in range(2):
                dec_scores(e0 + CD + k, kp_s[...].reshape(KVW, CL), 2 * DR + k)
            dqk(0)
            dqk(1)
            for k in range(2):
                dec_mix(c, CD + k, vp_s[...].reshape(KVW, CL), off + k * SEG + SEG - 1, 2 * DR + k)
            for q in range(4):
                dmix(q)
            if c == 0:
                wait('wg', 'wu', 'gf')
                pl.semaphore_wait(bar, 1)
            else:
                ls = [dec_out(k * ES + CD, 8)[:2] for k in range(2)]
                a = jnp.concatenate([dec_out(0, CD), dec_out(ES, CD)] + ls + [jnp.zeros((4, HID), F32)], axis=0).astype(BF16)
                xs = [xc_s[k].astype(F32) for k in range(2)]
                xf = jnp.concatenate([xs[0][CP:], xs[1][CP:]] + last_rows(xs[0]) + last_rows(xs[1]) + [jnp.zeros((4, HID), F32)], axis=0)

                def put(x, rows):
                    x2 = round32(x + nn(act_s[:rows, :], wdt_s[...]))
                    fh = rms(x2, gf_s[...].astype(F32).reshape(1, HID))
                    ri = lax.broadcasted_iota(jnp.int32, (FR, FR), 0)
                    src = jnp.where(ri < ND, (ri % NM) * DR + ri // NM, ri)
                    fh_s[...] = nn(jnp.where(lane_iota((FR, FR)) == src, 1.0, 0.0).astype(BF16), fh).astype(BF16)

                mlp(round32(xf + nn(a, wo_perm())), FR, put)
                ofh = pltpu.make_async_copy(fh_s, fh_o, out_sem.at[6])
                ofh.start()
                ofh.wait()

    for c in range(2):
        pltpu.make_async_copy(kdn_s.at[c], kdn.at[c], out_sem.at[c]).wait()
        pltpu.make_async_copy(vdn_s.at[c], vdn.at[c], out_sem.at[2 + c]).wait()
    pltpu.make_async_copy(kp_s, kpn, out_sem.at[4]).wait()
    pltpu.make_async_copy(vp_s, vpn, out_sem.at[5]).wait()

    @pl.when(st < LAST)
    def _():
        wait('gf')
        for c in range(2):
            hop(c).wait_send()


def head_kernel(fh, wh, tok, logits, fh_s, fr_s, wh_s, lsem, ssem, rsem):
    st = lax.axis_index('stage')
    lfh = pltpu.make_async_copy(fh, fh_s, lsem.at[0])
    lwh = pltpu.make_async_copy(wh, wh_s, lsem.at[1])

    @pl.when(st == LAST)
    def _():
        lfh.start()

    lwh.start()
    bar = pltpu.get_barrier_semaphore()

    def send(k):
        return pltpu.make_async_remote_copy(fh_s, fr_s, ssem.at[k], rsem, device_id={'stage': k}, device_id_type=MESH)

    def head(ref):
        lwh.wait()
        lg = nn(ref[...], wh_s[...])
        for i in range(DR + 1):
            logits[i] = lg[i * NM:(i + 1) * NM]

    @pl.when(st < LAST)
    def _():
        pl.semaphore_signal(bar, inc=1, device_id={'stage': LAST}, device_id_type=MESH)

    @pl.when(st == LAST)
    def _():
        for k in range(LAST):
            pl.semaphore_signal(bar, inc=1, device_id={'stage': k}, device_id_type=MESH)
        pl.semaphore_wait(bar, LAST)
        lfh.wait()
        for k in range(LAST):
            send(k).start()
        head(fh_s)
        for k in range(LAST):
            send(k).wait_send()

    @pl.when(st < LAST)
    def _():
        pl.semaphore_wait(bar, 1)
        send(0).wait_recv()
        head(fr_s)


def tile_start(pos):
    return pl.ds(pl.multiple_of((pos // LN) * LN, LN), LN)


def copy_all(kd, vd, ko, vo, ks, vs, ksem, vsem, edit):
    ins = [(pltpu.make_async_copy(kd.at[m], ks.at[m], ksem.at[m]), pltpu.make_async_copy(vd.at[m], vs.at[m], vsem.at[m])) for m in range(NM)]
    for a, b in ins:
        a.start()
        b.start()
    outs = []
    for m in range(NM):
        for c, scr, out, sem, w in ((ins[m][0], ks, ko, ksem, 0), (ins[m][1], vs, vo, vsem, 1)):
            c.wait()
            if edit is not None:
                edit(m, scr, w)
            o = pltpu.make_async_copy(scr.at[m], out.at[m], sem.at[m])
            o.start()
            outs.append(o)
    for o in outs:
        o.wait()


def pre_kernel(kd, vd, ko, vo, tok, ks, vs, ksem, vsem):
    st = lax.axis_index('stage')

    @pl.when(st >= 2)
    def _():
        copy_all(kd, vd, ko, vo, ks, vs, ksem, vsem, None)


def load_new(srcs, dsts, sem):
    cs = [pltpu.make_async_copy(a, b, sem.at[i]) for i, (a, b) in enumerate(zip(srcs, dsts))]
    for c in cs[4:] + cs[:4]:
        c.start()
    return cs


def update_tiles(dlen, bk, bv, ko, vo, kpo, vpo, kt, vt, new, cs, ksem, vsem, nsem, extra=None):
    lane = lane_iota((HD, LN))

    def cp(hbm, scr, sem, m, i, out):
        h = hbm.at[m, i, :, :, tile_start(dlen[m, i])]
        v = scr.at[m, i]
        return pltpu.make_async_copy(v, h, sem.at[m]) if out else pltpu.make_async_copy(h, v, sem.at[m])

    cs[4].wait()
    for m in range(NM):
        for i in range(DR):
            cp(bk, kt, ksem, m, i, False).start()
            cp(bv, vt, vsem, m, i, False).start()
    if extra is not None:
        extra()
    for c in cs[:4]:
        c.wait()
    po = [pltpu.make_async_copy(new[2], kpo, nsem.at[2]), pltpu.make_async_copy(new[3], vpo, nsem.at[3])]
    for o in po:
        o.start()
    for m in range(NM):
        for hbm, scr, sem, nw in ((ko, kt, ksem, new[0]), (vo, vt, vsem, new[1])):
            for i in range(DR):
                cp(hbm, scr, sem, m, i, False).wait()
            for i in range(DR):
                pos = dlen[m, i]
                for g in range(NKV):
                    col = nw[m // 2, g * HD:(g + 1) * HD, m % 2 * DR + i:m % 2 * DR + i + 1]
                    scr[m, i, g] = jnp.where(lane == pos % LN, col, scr[m, i, g].astype(F32)).astype(BF16)
            for i in range(DR):
                cp(hbm, scr, sem, m, i, True).start()
    for m in range(NM):
        for i in range(DR):
            cp(ko, kt, ksem, m, i, True).wait()
            cp(vo, vt, vsem, m, i, True).wait()
    for o in po:
        o.wait()


def mid_kernel(dlen_h, kd, vd, bk, bv, kdn, vdn, kpn, vpn, ko, vo, kpo, vpo, tok, ks, vs, kt, vt, kn_s, vn_s, kp_s, vp_s, dlen, ksem, vsem, nsem):
    st = lax.axis_index('stage')
    new = (kn_s, vn_s, kp_s, vp_s)

    @pl.when(st < 2)
    def _():
        cs = load_new((kdn, vdn, kpn, vpn, dlen_h), new + (dlen,), nsem)
        for c in cs:
            c.wait()
        po = [pltpu.make_async_copy(kp_s, kpo, nsem.at[2]), pltpu.make_async_copy(vp_s, vpo, nsem.at[3])]
        for o in po:
            o.start()
        lane = lane_iota((HD, LN))

        def edit(m, scr, w):
            for i in range(DR):
                pos = dlen[m, i]
                sl = tile_start(pos)
                for g in range(NKV):
                    col = new[w][m // 2, g * HD:(g + 1) * HD, m % 2 * DR + i:m % 2 * DR + i + 1]
                    scr[m, i, g, :, sl] = jnp.where(lane == pos % LN, col, scr[m, i, g, :, sl].astype(F32)).astype(BF16)

        copy_all(kd, vd, ko, vo, ks, vs, ksem, vsem, edit)
        for o in po:
            o.wait()

    @pl.when(st == 2)
    def _():
        cs = load_new((kdn, vdn, kpn, vpn, dlen_h), new + (dlen,), nsem)
        update_tiles(dlen, bk, bv, ko, vo, kpo, vpo, kt, vt, new, cs, ksem, vsem, nsem)


def post_kernel(dlen_h, kdn, vdn, kpn, vpn, lg, bk, bv, bkp, bvp, ko, vo, kpo, vpo, logits,
                kt, vt, lg_s, kn_s, vn_s, kp_s, vp_s, dlen, ksem, vsem, nsem, hsem):
    st = lax.axis_index('stage')
    lf = pltpu.make_async_copy(lg, lg_s, hsem.at[0])
    lo = pltpu.make_async_copy(lg_s, logits, hsem.at[1])

    def turn():
        lf.wait()
        lo.start()

    @pl.when(st == LAST)
    def _():
        new = (kn_s, vn_s, kp_s, vp_s)
        cs = load_new((kdn, vdn, kpn, vpn, dlen_h), new + (dlen,), nsem)
        lf.start()
        update_tiles(dlen, bk, bv, ko, vo, kpo, vpo, kt, vt, new, cs, ksem, vsem, nsem, turn)

    @pl.when(st < LAST)
    def _():
        lf.start()
        turn()

    lo.wait()


ANY = pl.BlockSpec(memory_space=pltpu.HBM)


def solution(mesh):
    part = P('replica')
    layer = P('stage')
    cache = P('stage', 'replica')
    in_specs = (part,) * 4 + (layer,) * 9 + (P(), P()) + (cache,) * 4
    out_specs = (part,) + (cache,) * 4
    inv_freq = np.float32(ROPE_BASE) ** (-np.arange(HALF, dtype=np.float32) * np.float32(2.0 / HD))
    ifr_c = np.broadcast_to(inv_freq[:, None], (HALF, NP)).astype(np.float32)

    def device_fn(x_dec, x_pre, dec_len, pre_len, g_attn, w_q, w_k, w_v, w_o, g_mlp, w_gate, w_up, w_down, g_final, w_head, k_dec, v_dec, k_pre, v_pre):
        kd = jnp.transpose(k_dec[0], (0, 1, 3, 4, 2))
        vd = jnp.transpose(v_dec[0], (0, 1, 3, 4, 2))
        kp = jnp.transpose(k_pre[0], (1, 2, 0))
        vp = jnp.transpose(v_pre[0], (1, 2, 0))
        args = (x_dec.reshape(ND, HID), x_pre.reshape(NP, HID), dec_len, pre_len, g_attn, w_q[0], w_k[0].T, w_v[0].T, w_o[0], g_mlp,
                w_gate[0], w_up[0], w_down[0].T, g_final, kd, vd, kp, vp, jnp.asarray(ifr_c))
        vm = lambda shape, dt: pltpu.VMEM(shape, dt)
        scratch = [
            vm((2, CR, HID), BF16), pltpu.SMEM((NM, DR), jnp.int32), pltpu.SMEM((1,), jnp.int32), vm((1, HID), BF16),
            vm((HID, HID), BF16), vm((HID + 2 * KVW, HID), BF16), vm((HID, HID), BF16), vm((1, HID), BF16),
            vm((HID, FFN), BF16), vm((HID, FFN), BF16), vm((HID, FFN), BF16), vm((FFN, HID), BF16), vm((HID,), BF16),
            vm(kd.shape, BF16), vm(vd.shape, BF16), vm(kp.shape, BF16), vm(vp.shape, BF16), vm((HALF, 2 * LN), F32),
            vm((2, HALF, 2 * LN), F32), vm((2, HALF, 2 * LN), F32), vm((HID, LN), BF16),
            vm((2 * ES * 8, LN), F32), vm((2 * ES * 8, LN), F32), vm((2, 24, LN), F32), vm((2 * ES, KVW), F32),
            vm((2 * ES * 8, LN), F32), vm((2 * ES * 8, LN), F32),
            vm((2, KVW, LN), F32), vm((2, KVW, LN), F32), vm(((2 * DR + 2) * 24, CL), F32), vm((2, CL, 2 * LN), F32), vm((2, CL, 2 * LN), BF16),
            vm((CL, LN), F32), vm((HID, LN), F32), vm((CR, FFN), BF16), vm((2, CR, HID), BF16), vm((FR, HID), BF16),
            pltpu.SemaphoreType.DMA((19,)), pltpu.SemaphoreType.DMA((NM,)), pltpu.SemaphoreType.DMA((NM,)), pltpu.SemaphoreType.DMA((7,)),
            pltpu.SemaphoreType.DMA((2,)), pltpu.SemaphoreType.DMA((2,)),
        ]
        sds = jax.ShapeDtypeStruct
        big = pltpu.CompilerParams(vmem_limit_bytes=62 * 1024 * 1024)
        cshape = sds(kd.shape, BF16)
        pshape = sds(kp.shape, BF16)
        nsems = [pltpu.SemaphoreType.DMA((NM,)), pltpu.SemaphoreType.DMA((NM,))]
        tile = vm((NM, DR, NKV, HD, LN), BF16)
        news = [vm((2, KVW, LN), F32), vm((2, KVW, LN), F32), vm(kp.shape, BF16), vm(vp.shape, BF16), pltpu.SMEM((NM, DR), jnp.int32)]
        vmem = pl.BlockSpec(memory_space=pltpu.VMEM)
        tshape = sds((8, LN), F32)
        bk, bv, tok = pl.pallas_call(
            pre_kernel, out_shape=(cshape, cshape, tshape), in_specs=[ANY, ANY], out_specs=(ANY, ANY, ANY),
            scratch_shapes=[vm(kd.shape, BF16), vm(vd.shape, BF16)] + nsems, name='pre', compiler_params=big)(kd, vd)
        args = args + (tok,)
        kdn, vdn, kpn, vpn, fh = pl.pallas_call(
            pipe_kernel,
            out_shape=(sds((2, KVW, LN), F32), sds((2, KVW, LN), F32), pshape, pshape, sds((ND + 8, HID), BF16)),
            in_specs=[ANY] * len(args),
            out_specs=(ANY,) * 5,
            scratch_shapes=scratch,
            name='pipe',
            compiler_params=pltpu.CompilerParams(collective_id=0, has_side_effects=True, vmem_limit_bytes=62 * 1024 * 1024),
        )(*args)
        bk, bv, bkp, bvp, tok2 = pl.pallas_call(
            mid_kernel, out_shape=(cshape, cshape, pshape, pshape, tshape), in_specs=[ANY] * 9, out_specs=(ANY,) * 5,
            input_output_aliases={3: 0, 4: 1},
            scratch_shapes=[vm(kd.shape, BF16), vm(vd.shape, BF16), tile, tile] + news + nsems + [pltpu.SemaphoreType.DMA((5,))],
            name='mid', compiler_params=big)(dec_len, kd, vd, bk, bv, kdn, vdn, kpn, vpn)
        lgs = sds((DR + 1, NM, VOC), F32)
        lg = pl.pallas_call(
            head_kernel, out_shape=lgs, in_specs=[ANY] * 3, out_specs=vmem,
            scratch_shapes=[vm((FR, HID), BF16), vm((FR, HID), BF16), vm((HID, VOC), BF16),
                            pltpu.SemaphoreType.DMA((2,)), pltpu.SemaphoreType.DMA((LAST,)), pltpu.SemaphoreType.DMA],
            name='head', compiler_params=pltpu.CompilerParams(collective_id=1, has_side_effects=True))(fh, w_head, tok2)
        ko, vo, kpo, vpo, logits = pl.pallas_call(
            post_kernel, out_shape=(cshape, cshape, pshape, pshape, lgs), in_specs=[ANY] * 10,
            out_specs=(ANY,) * 5, input_output_aliases={6: 0, 7: 1, 8: 2, 9: 3},
            scratch_shapes=[tile, tile, vm((DR + 1, NM, VOC), F32)] + news + nsems + [pltpu.SemaphoreType.DMA((5,)), pltpu.SemaphoreType.DMA((2,))],
            name='post', compiler_params=big)(dec_len, kdn, vdn, kpn, vpn, lg, bk, bv, bkp, bvp)
        back = lambda a: jnp.transpose(a, (0, 1, 4, 2, 3))[None]
        backp = lambda a: jnp.transpose(a, (2, 0, 1))[None]
        return jnp.transpose(logits, (1, 0, 2)), back(ko), back(vo), backp(kpo), backp(vpo)

    return jax.shard_map(device_fn, mesh=mesh, in_specs=in_specs, out_specs=out_specs, check_vma=False)
```

```python
import functools

import jax
import jax.numpy as jnp
import numpy as np
from jax import lax
from jax.experimental import pallas as pl
from jax.experimental.pallas import tpu as pltpu
from jax.sharding import PartitionSpec as P

F32 = jnp.float32
BF16 = jnp.bfloat16
MESH = pl.DeviceIdType.MESH
NORM_EPS = 1e-6
ROPE_BASE = 10000.0
NEG = -1e30

HID = 576
NQ = 9
NKV = 3
GRP = 3
HD = 64
HALF = 32
KVW = NKV * HD
FFN = 1536
NM = 4
DR = 8
SEG = 64
CL = 512
VOC = 1024
ND = NM * DR
NP = NM * SEG
LAST = 3
LN = 128
CP = 128
CD = 16
CR = CP + CD
ES = CD + 8
FR = ND + 8


def nt(a, b):
    return lax.dot_general(a, b, (((1,), (1,)), ((), ())), preferred_element_type=F32)


def nn(a, b):
    return jnp.dot(a, b, preferred_element_type=F32)


def rms(x, g):
    inv = lax.rsqrt(jnp.mean(x * x, axis=-1, keepdims=True) + NORM_EPS)
    return (x * inv * g).astype(BF16)


def rope_t(m, cos, sin):
    parts = []
    for j in range(m.shape[0] // HD):
        a = m[j * HD:j * HD + HALF]
        b = m[j * HD + HALF:(j + 1) * HD]
        parts += [a * cos - b * sin, b * cos + a * sin]
    return jnp.concatenate(parts, axis=0)


def lane_iota(shape):
    return lax.broadcasted_iota(jnp.int32, shape, len(shape) - 1)


def pipe_kernel(xd, xp, dlen, plen, ga, wq, wk, wv, wo, gm, wg, wu, wd, gf, kd, vd, kp, vp, ifr, tok,
                kdn, vdn, kpn, vpn, fh_o,
                xc_s, dl_s, pl_s, ga_s, wq_s, w3_s, wo_s, gm_s, wg_s, wu_s, wd_s, wdt_s, gf_s,
                kd_s, vd_s, kp_s, vp_s, ifr_s,
                cos_s, sin_s, qt_s, qa_s, qb_s, self_s, vn_s, oa_s, ob_s,
                kdn_s, vdn_s, sc_s, ps_s, pb_s, bias_s, ot_s, act_s, so_s, fh_s,
                in_sem, kd_sem, vd_sem, out_sem, ssem, rsem):
    st = lax.axis_index('stage')
    order = [(dlen, dl_s), (plen, pl_s), (ga, ga_s), (ifr, ifr_s), (wq, wq_s), (wk, w3_s.at[HID:HID + KVW]), (wv, w3_s.at[HID + KVW:]),
             (kp, kp_s), (vp, vp_s), (wo, wo_s), (gm, gm_s), (wg, wg_s), (wu, wu_s), (wd, wd_s), (gf, gf_s),
             (xp.at[0:CP], xc_s.at[0, 0:CP]), (xd.at[0:CD], xc_s.at[0, CP:CR]), (xp.at[CP:2 * CP], xc_s.at[1, 0:CP]), (xd.at[CD:2 * CD], xc_s.at[1, CP:CR])]
    names = ['dl', 'pl', 'ga', 'ifr', 'wq', 'wk', 'wv', 'kp', 'vp', 'wo', 'gm', 'wg', 'wu', 'wd', 'gf', 'p0', 'd0', 'p1', 'd1']
    cps = {n: pltpu.make_async_copy(a, b, in_sem.at[i]) for i, (n, (a, b)) in enumerate(zip(names, order))}
    kcp = [pltpu.make_async_copy(kd.at[m], kd_s.at[m], kd_sem.at[m]) for m in range(NM)]
    vcp = [pltpu.make_async_copy(vd.at[m], vd_s.at[m], vd_sem.at[m]) for m in range(NM)]

    def start(*ns):
        for n in ns:
            cps[n].start()

    def wait(*ns):
        for n in ns:
            cps[n].wait()

    start('dl', 'pl', 'ifr', 'ga', 'wq', 'wk', 'wv')

    @pl.when(st == 0)
    def _():
        start('p0', 'd0')

    bar = pltpu.get_barrier_semaphore()

    @pl.when(st > 0)
    def _():
        pl.semaphore_signal(bar, inc=1, device_id={'stage': jnp.maximum(st - 1, 0)}, device_id_type=MESH)

    @pl.when(st < LAST)
    def _():
        pl.semaphore_signal(bar, inc=1, device_id={'stage': jnp.minimum(st + 1, LAST)}, device_id_type=MESH)

    wait('dl', 'pl', 'ifr')
    start('kp', 'vp')
    for m in range(2):
        kcp[m].start()
        vcp[m].start()
    p0 = pl_s[0]
    li = lane_iota((1, 2 * LN))
    fr = ifr_s[...]
    for c in range(2):
        pos = p0 + (c * CP) + li
        for k in range(CD):
            pos = jnp.where(li == LN + k, dl_s[2 * c + k // DR, k % DR], pos)
        for k in range(2):
            pos = jnp.where(li == LN + CD + k, p0 + (c * CP + k * SEG + SEG - 1), pos)
        ang = fr * pos.astype(F32)
        cos_s[c] = jnp.cos(ang)
        sin_s[c] = jnp.sin(ang)
    qa_s[...] = jnp.zeros_like(qa_s)
    qb_s[...] = jnp.zeros_like(qb_s)
    ob_s[...] = jnp.zeros_like(ob_s)
    for k in range(2):
        pb_s[k] = jnp.zeros((CL, 2 * LN), BF16)

    start('wo', 'gm')

    @pl.when(st > 0)
    def _():
        start('wg', 'wu', 'wd', 'gf')

    wait('ga', 'wq')
    w3_s[:HID, :] = wq_s[...].astype(F32).T.astype(BF16)
    wait('wk', 'wv')

    @pl.when(st > 0)
    def _():
        wait('wd')
        for k in range(0, FFN, LN):
            wdt_s[k:k + LN, :] = wd_s[:, k:k + LN].astype(F32).T.astype(BF16)

    gat = ga_s[...].astype(F32)

    lgrp = lane_iota((8, KVW)) // HD

    def dec_scores(e, kt, slot):
        qb = jnp.concatenate([qa_s[e * 8:e * 8 + 8, :], qb_s[e * 8:e * 8 + 8, :HD]], axis=1)
        lhs = jnp.concatenate([jnp.where(lgrp == g, qb, 0.0) for g in range(NKV)], axis=0).astype(BF16)
        sc_s[slot * 24:slot * 24 + 24, :] = nn(lhs, kt)

    def dec_mix(c, k, vt, pos, slot):
        e = c * ES + k
        selfcol = jnp.sum(jnp.where(lane_iota((24, LN)) == k, self_s[c], 0.0), axis=-1, keepdims=True)
        s = jnp.where(lane_iota((24, CL)) < pos, sc_s[slot * 24:slot * 24 + 24, :], NEG)
        mx = jnp.maximum(jnp.max(s, axis=-1, keepdims=True), selfcol)
        p = jnp.exp(s - mx)
        ps = jnp.exp(selfcol - mx)
        rl = 1.0 / (jnp.sum(p, axis=-1, keepdims=True) + ps)
        o = nt((p * rl).astype(BF16), vt)
        o = o + (ps * rl).astype(BF16).astype(F32) * vn_s[e:e + 1, :]
        acc = jnp.where(lgrp == 0, o[0:8], 0.0)
        for g in range(1, NKV):
            acc = jnp.where(lgrp == g, o[8 * g:8 * g + 8], acc)
        oa_s[e * 8:e * 8 + 8, :] = acc[:, :LN]
        ob_s[e * 8:e * 8 + 8, :HD] = acc[:, LN:]

    def dec_out(e, n):
        return jnp.concatenate([x for r in range(GRP) for x in
                                (oa_s[pl.ds(e * 8 + r, n, stride=8), :], ob_s[pl.ds(e * 8 + r, n, stride=8), :][:, :HD])], axis=1)

    def wo_perm():
        return jnp.concatenate([wo_s[(g * GRP + r) * HD:(g * GRP + r + 1) * HD, :] for r in range(GRP) for g in range(NKV)], axis=0)

    def mlp(x, rows, put):
        h2 = rms(x, gm_s[...].astype(F32))
        step = 512
        for c in range(FFN // step):
            gt = nn(h2, wg_s[:, c * step:(c + 1) * step])
            up = nn(h2, wu_s[:, c * step:(c + 1) * step])
            act_s[:rows, c * step:(c + 1) * step] = (gt * (1.0 / (1.0 + jnp.exp(-gt))) * up).astype(BF16)
        put(x, rows)

    def round32(x):
        return x.astype(BF16).astype(F32)

    def hop(c):
        return pltpu.make_async_remote_copy(so_s.at[c], xc_s.at[c], ssem.at[c], rsem.at[c],
                                            device_id={'stage': jnp.minimum(st + 1, LAST)}, device_id_type=MESH)

    def last_rows(x):
        return [x[k * SEG + SEG - 1:k * SEG + SEG] for k in range(2)]

    for c in range(2):
        lim = CL - CP if c == 0 else CL

        @pl.when(st == 0)
        def _():
            wait('p%d' % c, 'd%d' % c)

        @pl.when(st > 0)
        def _():
            hop(c).wait_recv()

        if c == 0:
            wait('kp', 'vp')

            @pl.when(st == 0)
            def _():
                start('wg', 'wu', 'wd', 'gf')
        else:
            for m in (2, 3):
                kcp[m].wait()
                vcp[m].wait()
        off = p0 + c * CP
        e0 = c * ES

        def project():
            x = xc_s[c].astype(F32)
            h = x * lax.rsqrt(jnp.mean(x * x, axis=-1, keepdims=True) + NORM_EPS) * gat
            h = jnp.concatenate([h] + last_rows(h) + [jnp.zeros((2 * LN - CR - 2, HID), F32)], axis=0).astype(BF16)
            half = (HID + 2 * KVW) // 2
            qkv = jnp.concatenate([nt(w3_s[:half, :], h), nt(w3_s[half:, :], h)], axis=0)
            cos, sin = cos_s[c], sin_s[c]
            qt = round32(rope_t(qkv[:HID], cos, sin)) * (HD ** -0.5)
            kt = round32(rope_t(qkv[HID:HID + KVW], cos, sin))
            vt = round32(qkv[HID + KVW:])
            qt_s[...] = qt[:, :LN].astype(BF16)
            qe, ke, ve = qt[:, LN:], kt[:, LN:], vt[:, LN:]
            row = lax.broadcasted_iota(jnp.int32, (24, LN), 0)
            sf = jnp.zeros((24, LN), F32)
            for g in range(NKV):
                for r in range(GRP):
                    j = g * GRP + r
                    v = jnp.sum(qe[j * HD:(j + 1) * HD] * ke[g * HD:(g + 1) * HD], axis=0, keepdims=True)
                    sf = jnp.where(row == 8 * g + r, v, sf)
            self_s[c] = sf
            n = CD + 8
            pad = jnp.zeros((HD, LN), F32)
            for r in range(GRP):
                qr = [qe[(g * GRP + r) * HD:(g * GRP + r + 1) * HD] for g in range(NKV)]
                qa_s[pl.ds(e0 * 8 + r, n, stride=8), :] = jnp.concatenate(qr[:2], axis=0).T[:n]
                qb_s[pl.ds(e0 * 8 + r, n, stride=8), :] = jnp.concatenate([qr[2], pad], axis=0).T[:n]
            vn_s[e0:e0 + n, :LN] = ve[:LN].T[:n]
            vn_s[e0:e0 + n, LN:] = jnp.concatenate([ve[LN:], pad], axis=0).T[:n, :HD]
            kdn_s[c] = ke
            vdn_s[c] = ve
            pltpu.make_async_copy(kdn_s.at[c], kdn.at[c], out_sem.at[c]).start()
            pltpu.make_async_copy(vdn_s.at[c], vdn.at[c], out_sem.at[2 + c]).start()
            return kt, vt

        def put_prompt(kt, vt):
            place = jnp.where(lax.broadcasted_iota(jnp.int32, (CP, CL), 0) + off == lane_iota((CP, CL)), 1.0, 0.0).astype(BF16)
            lp = lane_iota((KVW, CL)) - off
            fresh = (lp >= 0) & (lp < CP)
            kpu = jnp.where(fresh, nn(kt[:, :LN].astype(BF16), place), kp_s[...].reshape(KVW, CL).astype(F32))
            vpu = jnp.where(fresh, nn(vt[:, :LN].astype(BF16), place), vp_s[...].reshape(KVW, CL).astype(F32))
            kp_s[...] = kpu.astype(BF16).reshape(NKV, HD, CL)
            vp_s[...] = vpu.astype(BF16).reshape(NKV, HD, CL)
            if c == 1:
                pltpu.make_async_copy(kp_s, kpn, out_sem.at[4]).start()
                pltpu.make_async_copy(vp_s, vpn, out_sem.at[5]).start()
            return kpu

        def loads():
            if c == 0:
                for m in (0, 1):
                    kcp[m].wait()
                    vcp[m].wait()

                @pl.when(st == 0)
                def _():
                    start('p1', 'd1')
                for m in (2, 3):
                    kcp[m].start()
                    vcp[m].start()
                wait('wo', 'gm')

        def dqk(i):
            for k in range(DR):
                dec_scores(c * ES + i * DR + k, kd_s[2 * c + i, k].reshape(KVW, CL), i * DR + k)

        def dmix(q):
            for k in range(4 * q, 4 * q + 4):
                m, i = 2 * c + k // DR, k % DR
                dec_mix(c, k, vd_s[m, i].reshape(KVW, CL), dl_s[m, i], k)

        @pl.when(st < LAST)
        def _():
            kt, vt = project()
            loads()
            kpu = put_prompt(kt, vt)
            kfull = kpu[:, :lim].T.astype(BF16)
            bias_s[:lim, :] = jnp.where(lax.broadcasted_iota(jnp.int32, (lim, LN), 0) <= lane_iota((lim, LN)) + off, 0.0, NEG)

            def heads(t):
                return [j for j in (2 * t, 2 * t + 1) if j < NQ]

            def scores(t):
                cols = []
                for j in heads(t):
                    g = j // GRP
                    parts = [jnp.zeros((g * HD, LN), BF16)] * (g > 0) + [qt_s[j * HD:(j + 1) * HD, :]]
                    parts += [jnp.zeros(((NKV - 1 - g) * HD, LN), BF16)] * (g < NKV - 1)
                    cols.append(jnp.concatenate(parts, axis=0))
                w = len(cols) * LN
                rhs = jnp.concatenate(cols, axis=1)
                for q in range(0, lim, lim // 2):
                    ps_s[t % 2, q:q + lim // 2, :w] = nn(kfull[q:q + lim // 2], rhs)

            def fold(v, op):
                return op(v.reshape(v.shape[0] // 8, 8, v.shape[1]), axis=0)

            ck = 64

            def masked(sl, q, ln):
                v = ps_s[sl, q:q + ck, ln]
                return v if q + ck <= 64 else v + bias_s[q:q + ck, :]

            def mix(t):
                sl = t % 2
                hs = heads(t)
                for i, j in enumerate(hs):
                    ln = slice(i * LN, (i + 1) * LN)
                    mx = jnp.full((8, LN), NEG, F32)
                    for q in range(0, lim, ck):
                        mx = jnp.maximum(mx, fold(masked(sl, q, ln), jnp.max))
                    mx = jnp.max(mx, axis=0, keepdims=True)
                    sm = jnp.zeros((8, LN), F32)
                    for q in range(0, lim, ck):
                        p = jnp.exp(masked(sl, q, ln) - mx)
                        ps_s[sl, q:q + ck, ln] = p
                        sm = sm + fold(p, jnp.sum)
                    rl = 1.0 / jnp.sum(sm, axis=0, keepdims=True)
                    for q in range(0, lim, ck):
                        pb_s[sl, q:q + ck, ln] = (ps_s[sl, q:q + ck, ln] * rl).astype(BF16)
                g0, g1 = hs[0] // GRP, hs[-1] // GRP
                o = nn(vp_s[...].reshape(KVW, CL)[g0 * HD:(g1 + 1) * HD, :lim], pb_s[sl, :lim, :len(hs) * LN])
                for i, j in enumerate(hs):
                    g, r = j // GRP, j % GRP
                    d = (r * NKV + g) * HD
                    ot_s[d:d + HD, :] = o[(g - g0) * HD:(g - g0 + 1) * HD, i * LN:(i + 1) * LN]

            dqk(0)
            scores(0)
            scores(1)
            dmix(0)
            mix(0)
            scores(2)
            dmix(1)
            mix(1)
            dqk(1)
            scores(3)
            dmix(2)
            mix(2)
            scores(4)
            dmix(3)
            mix(3)
            mix(4)
            a = jnp.concatenate([ot_s[...].T, dec_out(e0, CD)], axis=0).astype(BF16)
            x1 = round32(xc_s[c].astype(F32) + nn(a, wo_perm()))
            if c == 0:
                wait('wg', 'wu')

                @pl.when(st == 0)
                def _():
                    wait('wd')

            def put(x, rows):
                @pl.when(st == 0)
                def _():
                    so_s[c] = (x + nt(act_s[...], wd_s[...])).astype(BF16)

                @pl.when(st > 0)
                def _():
                    so_s[c] = (x + nn(act_s[...], wdt_s[...])).astype(BF16)

            mlp(x1, CR, put)
            if c == 0:
                @pl.when(st == 0)
                def _():
                    pl.semaphore_wait(bar, 1)

                @pl.when(st > 0)
                def _():
                    pl.semaphore_wait(bar, 2)
            hop(c).start()

        @pl.when(st == LAST)
        def _():
            kt, vt = project()
            loads()
            put_prompt(kt, vt)
            for k in range(2):
                dec_scores(e0 + CD + k, kp_s[...].reshape(KVW, CL), 2 * DR + k)
            dqk(0)
            dqk(1)
            for k in range(2):
                dec_mix(c, CD + k, vp_s[...].reshape(KVW, CL), off + k * SEG + SEG - 1, 2 * DR + k)
            for q in range(4):
                dmix(q)
            if c == 0:
                wait('wg', 'wu', 'gf')
                pl.semaphore_wait(bar, 1)
            else:
                ls = [dec_out(k * ES + CD, 8)[:2] for k in range(2)]
                a = jnp.concatenate([dec_out(0, CD), dec_out(ES, CD)] + ls + [jnp.zeros((4, HID), F32)], axis=0).astype(BF16)
                xs = [xc_s[k].astype(F32) for k in range(2)]
                xf = jnp.concatenate([xs[0][CP:], xs[1][CP:]] + last_rows(xs[0]) + last_rows(xs[1]) + [jnp.zeros((4, HID), F32)], axis=0)

                def put(x, rows):
                    x2 = round32(x + nn(act_s[:rows, :], wdt_s[...]))
                    fh = rms(x2, gf_s[...].astype(F32).reshape(1, HID))
                    ri = lax.broadcasted_iota(jnp.int32, (FR, FR), 0)
                    src = jnp.where(ri < ND, (ri % NM) * DR + ri // NM, ri)
                    fh_s[...] = nn(jnp.where(lane_iota((FR, FR)) == src, 1.0, 0.0).astype(BF16), fh).astype(BF16)

                mlp(round32(xf + nn(a, wo_perm())), FR, put)
                ofh = pltpu.make_async_copy(fh_s, fh_o, out_sem.at[6])
                ofh.start()
                ofh.wait()

    for c in range(2):
        pltpu.make_async_copy(kdn_s.at[c], kdn.at[c], out_sem.at[c]).wait()
        pltpu.make_async_copy(vdn_s.at[c], vdn.at[c], out_sem.at[2 + c]).wait()
    pltpu.make_async_copy(kp_s, kpn, out_sem.at[4]).wait()
    pltpu.make_async_copy(vp_s, vpn, out_sem.at[5]).wait()

    @pl.when(st < LAST)
    def _():
        wait('gf')
        for c in range(2):
            hop(c).wait_send()


def head_kernel(fh, wh, tok, logits, fh_s, fr_s, wh_s, lsem, ssem, rsem):
    st = lax.axis_index('stage')
    lfh = pltpu.make_async_copy(fh, fh_s, lsem.at[0])
    lwh = pltpu.make_async_copy(wh, wh_s, lsem.at[1])

    @pl.when(st == LAST)
    def _():
        lfh.start()

    lwh.start()
    bar = pltpu.get_barrier_semaphore()

    def send(k):
        return pltpu.make_async_remote_copy(fh_s, fr_s, ssem.at[k], rsem, device_id={'stage': k}, device_id_type=MESH)

    def head(ref):
        lwh.wait()
        lg = nn(ref[...], wh_s[...])
        for i in range(DR + 1):
            logits[i] = lg[i * NM:(i + 1) * NM]

    @pl.when(st < LAST)
    def _():
        pl.semaphore_signal(bar, inc=1, device_id={'stage': LAST}, device_id_type=MESH)

    @pl.when(st == LAST)
    def _():
        for k in range(LAST):
            pl.semaphore_signal(bar, inc=1, device_id={'stage': k}, device_id_type=MESH)
        pl.semaphore_wait(bar, LAST)
        lfh.wait()
        for k in range(LAST):
            send(k).start()
        head(fh_s)
        for k in range(LAST):
            send(k).wait_send()

    @pl.when(st < LAST)
    def _():
        pl.semaphore_wait(bar, 1)
        send(0).wait_recv()
        head(fr_s)


def tile_start(pos):
    return pl.ds(pl.multiple_of((pos // LN) * LN, LN), LN)


def copy_all(kd, vd, ko, vo, ks, vs, ksem, vsem, edit):
    ins = [(pltpu.make_async_copy(kd.at[m], ks.at[m], ksem.at[m]), pltpu.make_async_copy(vd.at[m], vs.at[m], vsem.at[m])) for m in range(NM)]
    for a, b in ins:
        a.start()
        b.start()
    outs = []
    for m in range(NM):
        for c, scr, out, sem, w in ((ins[m][0], ks, ko, ksem, 0), (ins[m][1], vs, vo, vsem, 1)):
            c.wait()
            if edit is not None:
                edit(m, scr, w)
            o = pltpu.make_async_copy(scr.at[m], out.at[m], sem.at[m])
            o.start()
            outs.append(o)
    for o in outs:
        o.wait()


def pre_kernel(kd, vd, ko, vo, tok, ks, vs, ksem, vsem):
    st = lax.axis_index('stage')

    @pl.when(st >= 2)
    def _():
        copy_all(kd, vd, ko, vo, ks, vs, ksem, vsem, None)


def load_new(srcs, dsts, sem):
    cs = [pltpu.make_async_copy(a, b, sem.at[i]) for i, (a, b) in enumerate(zip(srcs, dsts))]
    for c in cs[4:] + cs[:4]:
        c.start()
    return cs


def update_tiles(dlen, bk, bv, ko, vo, kpo, vpo, kt, vt, new, cs, ksem, vsem, nsem, extra=None):
    lane = lane_iota((HD, LN))

    def cp(hbm, scr, sem, m, i, out):
        h = hbm.at[m, i, :, :, tile_start(dlen[m, i])]
        v = scr.at[m, i]
        return pltpu.make_async_copy(v, h, sem.at[m]) if out else pltpu.make_async_copy(h, v, sem.at[m])

    cs[4].wait()
    for m in range(NM):
        for i in range(DR):
            cp(bk, kt, ksem, m, i, False).start()
            cp(bv, vt, vsem, m, i, False).start()
    if extra is not None:
        extra()
    for c in cs[:4]:
        c.wait()
    po = [pltpu.make_async_copy(new[2], kpo, nsem.at[2]), pltpu.make_async_copy(new[3], vpo, nsem.at[3])]
    for o in po:
        o.start()
    for m in range(NM):
        for hbm, scr, sem, nw in ((ko, kt, ksem, new[0]), (vo, vt, vsem, new[1])):
            for i in range(DR):
                cp(hbm, scr, sem, m, i, False).wait()
            for i in range(DR):
                pos = dlen[m, i]
                for g in range(NKV):
                    col = nw[m // 2, g * HD:(g + 1) * HD, m % 2 * DR + i:m % 2 * DR + i + 1]
                    scr[m, i, g] = jnp.where(lane == pos % LN, col, scr[m, i, g].astype(F32)).astype(BF16)
            for i in range(DR):
                cp(hbm, scr, sem, m, i, True).start()
    for m in range(NM):
        for i in range(DR):
            cp(ko, kt, ksem, m, i, True).wait()
            cp(vo, vt, vsem, m, i, True).wait()
    for o in po:
        o.wait()


def mid_kernel(dlen_h, kd, vd, bk, bv, kdn, vdn, kpn, vpn, ko, vo, kpo, vpo, tok, ks, vs, kt, vt, kn_s, vn_s, kp_s, vp_s, dlen, ksem, vsem, nsem):
    st = lax.axis_index('stage')
    new = (kn_s, vn_s, kp_s, vp_s)

    @pl.when(st < 2)
    def _():
        cs = load_new((kdn, vdn, kpn, vpn, dlen_h), new + (dlen,), nsem)
        for c in cs:
            c.wait()
        po = [pltpu.make_async_copy(kp_s, kpo, nsem.at[2]), pltpu.make_async_copy(vp_s, vpo, nsem.at[3])]
        for o in po:
            o.start()
        lane = lane_iota((HD, LN))

        def edit(m, scr, w):
            for i in range(DR):
                pos = dlen[m, i]
                sl = tile_start(pos)
                for g in range(NKV):
                    col = new[w][m // 2, g * HD:(g + 1) * HD, m % 2 * DR + i:m % 2 * DR + i + 1]
                    scr[m, i, g, :, sl] = jnp.where(lane == pos % LN, col, scr[m, i, g, :, sl].astype(F32)).astype(BF16)

        copy_all(kd, vd, ko, vo, ks, vs, ksem, vsem, edit)
        for o in po:
            o.wait()

    @pl.when(st == 2)
    def _():
        cs = load_new((kdn, vdn, kpn, vpn, dlen_h), new + (dlen,), nsem)
        update_tiles(dlen, bk, bv, ko, vo, kpo, vpo, kt, vt, new, cs, ksem, vsem, nsem)


def post_kernel(dlen_h, kdn, vdn, kpn, vpn, lg, bk, bv, bkp, bvp, ko, vo, kpo, vpo, logits,
                kt, vt, lg_s, kn_s, vn_s, kp_s, vp_s, dlen, ksem, vsem, nsem, hsem):
    st = lax.axis_index('stage')
    lf = pltpu.make_async_copy(lg, lg_s, hsem.at[0])
    lo = pltpu.make_async_copy(lg_s, logits, hsem.at[1])

    def turn():
        lf.wait()
        lo.start()

    @pl.when(st == LAST)
    def _():
        new = (kn_s, vn_s, kp_s, vp_s)
        cs = load_new((kdn, vdn, kpn, vpn, dlen_h), new + (dlen,), nsem)
        lf.start()
        update_tiles(dlen, bk, bv, ko, vo, kpo, vpo, kt, vt, new, cs, ksem, vsem, nsem, turn)

    @pl.when(st < LAST)
    def _():
        lf.start()
        turn()

    lo.wait()


ANY = pl.BlockSpec(memory_space=pltpu.HBM)


def solution(mesh):
    part = P('replica')
    layer = P('stage')
    cache = P('stage', 'replica')
    in_specs = (part,) * 4 + (layer,) * 9 + (P(), P()) + (cache,) * 4
    out_specs = (part,) + (cache,) * 4
    inv_freq = np.float32(ROPE_BASE) ** (-np.arange(HALF, dtype=np.float32) * np.float32(2.0 / HD))
    ifr_c = np.broadcast_to(inv_freq[:, None], (HALF, NP)).astype(np.float32)

    def device_fn(x_dec, x_pre, dec_len, pre_len, g_attn, w_q, w_k, w_v, w_o, g_mlp, w_gate, w_up, w_down, g_final, w_head, k_dec, v_dec, k_pre, v_pre):
        kd = jnp.transpose(k_dec[0], (0, 1, 3, 4, 2))
        vd = jnp.transpose(v_dec[0], (0, 1, 3, 4, 2))
        kp = jnp.transpose(k_pre[0], (1, 2, 0))
        vp = jnp.transpose(v_pre[0], (1, 2, 0))
        args = (x_dec.reshape(ND, HID), x_pre.reshape(NP, HID), dec_len, pre_len, g_attn, w_q[0], w_k[0].T, w_v[0].T, w_o[0], g_mlp,
                w_gate[0], w_up[0], w_down[0].T, g_final, kd, vd, kp, vp, jnp.asarray(ifr_c))
        vm = lambda shape, dt: pltpu.VMEM(shape, dt)
        scratch = [
            vm((2, CR, HID), BF16), pltpu.SMEM((NM, DR), jnp.int32), pltpu.SMEM((1,), jnp.int32), vm((1, HID), BF16),
            vm((HID, HID), BF16), vm((HID + 2 * KVW, HID), BF16), vm((HID, HID), BF16), vm((1, HID), BF16),
            vm((HID, FFN), BF16), vm((HID, FFN), BF16), vm((HID, FFN), BF16), vm((FFN, HID), BF16), vm((HID,), BF16),
            vm(kd.shape, BF16), vm(vd.shape, BF16), vm(kp.shape, BF16), vm(vp.shape, BF16), vm((HALF, 2 * LN), F32),
            vm((2, HALF, 2 * LN), F32), vm((2, HALF, 2 * LN), F32), vm((HID, LN), BF16),
            vm((2 * ES * 8, LN), F32), vm((2 * ES * 8, LN), F32), vm((2, 24, LN), F32), vm((2 * ES, KVW), F32),
            vm((2 * ES * 8, LN), F32), vm((2 * ES * 8, LN), F32),
            vm((2, KVW, LN), F32), vm((2, KVW, LN), F32), vm(((2 * DR + 2) * 24, CL), F32), vm((2, CL, 2 * LN), F32), vm((2, CL, 2 * LN), BF16),
            vm((CL, LN), F32), vm((HID, LN), F32), vm((CR, FFN), BF16), vm((2, CR, HID), BF16), vm((FR, HID), BF16),
            pltpu.SemaphoreType.DMA((19,)), pltpu.SemaphoreType.DMA((NM,)), pltpu.SemaphoreType.DMA((NM,)), pltpu.SemaphoreType.DMA((7,)),
            pltpu.SemaphoreType.DMA((2,)), pltpu.SemaphoreType.DMA((2,)),
        ]
        sds = jax.ShapeDtypeStruct
        big = pltpu.CompilerParams(vmem_limit_bytes=62 * 1024 * 1024)
        cshape = sds(kd.shape, BF16)
        pshape = sds(kp.shape, BF16)
        nsems = [pltpu.SemaphoreType.DMA((NM,)), pltpu.SemaphoreType.DMA((NM,))]
        tile = vm((NM, DR, NKV, HD, LN), BF16)
        news = [vm((2, KVW, LN), F32), vm((2, KVW, LN), F32), vm(kp.shape, BF16), vm(vp.shape, BF16), pltpu.SMEM((NM, DR), jnp.int32)]
        vmem = pl.BlockSpec(memory_space=pltpu.VMEM)
        tshape = sds((8, LN), F32)
        bk, bv, tok = pl.pallas_call(
            pre_kernel, out_shape=(cshape, cshape, tshape), in_specs=[ANY, ANY], out_specs=(ANY, ANY, ANY),
            scratch_shapes=[vm(kd.shape, BF16), vm(vd.shape, BF16)] + nsems, name='pre', compiler_params=big)(kd, vd)
        args = args + (tok,)
        kdn, vdn, kpn, vpn, fh = pl.pallas_call(
            pipe_kernel,
            out_shape=(sds((2, KVW, LN), F32), sds((2, KVW, LN), F32), pshape, pshape, sds((ND + 8, HID), BF16)),
            in_specs=[ANY] * len(args),
            out_specs=(ANY,) * 5,
            scratch_shapes=scratch,
            name='pipe',
            compiler_params=pltpu.CompilerParams(collective_id=0, has_side_effects=True, vmem_limit_bytes=62 * 1024 * 1024),
        )(*args)
        bk, bv, bkp, bvp, tok2 = pl.pallas_call(
            mid_kernel, out_shape=(cshape, cshape, pshape, pshape, tshape), in_specs=[ANY] * 9, out_specs=(ANY,) * 5,
            input_output_aliases={3: 0, 4: 1},
            scratch_shapes=[vm(kd.shape, BF16), vm(vd.shape, BF16), tile, tile] + news + nsems + [pltpu.SemaphoreType.DMA((5,))],
            name='mid', compiler_params=big)(dec_len, kd, vd, bk, bv, kdn, vdn, kpn, vpn)
        lgs = sds((DR + 1, NM, VOC), F32)
        lg = pl.pallas_call(
            head_kernel, out_shape=lgs, in_specs=[ANY] * 3, out_specs=vmem,
            scratch_shapes=[vm((FR, HID), BF16), vm((FR, HID), BF16), vm((HID, VOC), BF16),
                            pltpu.SemaphoreType.DMA((2,)), pltpu.SemaphoreType.DMA((LAST,)), pltpu.SemaphoreType.DMA],
            name='head', compiler_params=pltpu.CompilerParams(collective_id=1, has_side_effects=True))(fh, w_head, tok2)
        ko, vo, kpo, vpo, logits = pl.pallas_call(
            post_kernel, out_shape=(cshape, cshape, pshape, pshape, lgs), in_specs=[ANY] * 10,
            out_specs=(ANY,) * 5, input_output_aliases={6: 0, 7: 1, 8: 2, 9: 3},
            scratch_shapes=[tile, tile, vm((DR + 1, NM, VOC), F32)] + news + nsems + [pltpu.SemaphoreType.DMA((5,)), pltpu.SemaphoreType.DMA((2,))],
            name='post', compiler_params=big)(dec_len, kdn, vdn, kpn, vpn, lg, bk, bv, bkp, bvp)
        back = lambda a: jnp.transpose(a, (0, 1, 4, 2, 3))[None]
        backp = lambda a: jnp.transpose(a, (2, 0, 1))[None]
        return jnp.transpose(logits, (1, 0, 2)), back(ko), back(vo), backp(kpo), backp(vpo)

    return jax.shard_map(device_fn, mesh=mesh, in_specs=in_specs, out_specs=out_specs, check_vma=False)
```
